32 devices in a mesh: ctx: 8 (over z, x), fsdp: 4 (over y, core).
Axes of the slice: x: 2, y: 2, z: 4, core: 2. Of those that a mesh axis runs over, the one named last changes fastest.
Arguments:
- inputs: bfloat16 [8, 1024, 1600], P('fsdp', 'ctx'), may hold values from -6 to 6
- cotangent: bfloat16 [8, 1024, 1600], P('fsdp', 'ctx'), may hold values from -6 to 6
- w_query: bfloat16 [1600, 1600], P('fsdp'), may hold values from -0.15625 to 0.15625
- w_key: bfloat16 [1600, 1600], P('fsdp'), may hold values from -0.15625 to 0.15625
- w_value: bfloat16 [1600, 1600], P('fsdp'), may hold values from -0.15625 to 0.15625
- w_out: bfloat16 [1600, 1600], P('fsdp'), may hold values from -1.25 to 1.25
- w_fc: bfloat16 [1600, 6400], P('fsdp'), may hold values from -0.15625 to 0.15625
- w_proj: bfloat16 [6400, 1600], P('fsdp'), may hold values from -0.078125 to 0.078125
- ln1_gain: bfloat16 [1600], P('fsdp'), may hold values from 0.099609375 to 1.8984375
- ln1_bias: bfloat16 [1600], P('fsdp'), may hold values from -3 to 3
- query_bias: bfloat16 [1600], P('fsdp'), may hold values from -3 to 3
- value_bias: bfloat16 [1600], P('fsdp'), may hold values from -3 to 3
- out_bias: bfloat16 [1600], P('fsdp'), may hold values from -3 to 3
- ln2_gain: bfloat16 [1600], P('fsdp'), may hold values from 0.099609375 to 1.8984375
- ln2_bias: bfloat16 [1600], P('fsdp'), may hold values from -3 to 3
- fc_bias: bfloat16 [6400], P('fsdp'), may hold values from -3 to 3
- proj_bias: bfloat16 [1600], P('fsdp'), may hold values from -3 to 3
Outputs:
- outputs: bfloat16 [8, 1024, 1600], P('fsdp', 'ctx')
- input_grad: float32 [8, 1024, 1600], P('fsdp', 'ctx')
- grad_query: float32 [1600, 1600], P('fsdp')
- grad_key: float32 [1600, 1600], P('fsdp')
- grad_value: float32 [1600, 1600], P('fsdp')
- grad_out: float32 [1600, 1600], P('fsdp')
- grad_fc: float32 [1600, 6400], P('fsdp')
- grad_proj: float32 [6400, 1600], P('fsdp')
- grad_ln1_gain: float32 [1600], P('fsdp')
- grad_ln1_bias: float32 [1600], P('fsdp')
- grad_query_bias: float32 [1600], P('fsdp')
- grad_value_bias: float32 [1600], P('fsdp')
- grad_out_bias: float32 [1600], P('fsdp')
- grad_ln2_gain: float32 [1600], P('fsdp')
- grad_ln2_bias: float32 [1600], P('fsdp')
- grad_fc_bias: float32 [6400], P('fsdp')
- grad_proj_bias: float32 [1600], P('fsdp')
The draws below stay inside these ranges and needn't reach their ends.
All inputs are finite; a program needn't handle non-finite values.
Results may differ from the reference program's by a relative error of at most 0.03.
Values may be sent and summed in bfloat16 or wider, within the bound.
A program may use at most 448 MiB of HBM per device.

```python
import jax
import jax.numpy as jnp
from jax import lax

D = 1600
HEADS = 25
HEAD = 64
FF = 6400
LEN = 1024
ROWS = 128
HALF = 64
SEQS = 8
N_CTX = 8


def levels(own_key, shape, split, low, top_value):
    factor_of = 1.0
    for dim, parts in split:
        heights = jax.random.uniform(jax.random.fold_in(jax.random.fold_in(own_key, 6), dim), (parts,), jnp.float32, low / len(split), top_value / len(split))
        factor_of = factor_of * jnp.repeat(jnp.exp(heights), shape[dim] // parts).reshape((-1,) + (1,) * (len(shape) - 1 - dim))
    return factor_of


def bell_draw(stream_key, dims, scale, most, pieces=(), kind=jnp.bfloat16):
    drawn = scale * jax.random.normal(stream_key, dims, jnp.float32)
    if pieces:
        drawn = drawn * levels(stream_key, dims, pieces, -0.22, 0.18)
    return jnp.clip(drawn, -most, most).astype(kind)


def setup_inputs(seed: int = 0) -> dict:
    splits = jax.random.split(jax.random.key(seed), 18)
    inputs = bell_draw(splits[0], (SEQS, LEN, D), 1.0, 6.0, ((0, 4), (1, 8)))
    cotangent = bell_draw(splits[1], (SEQS, LEN, D), 1.0, 6.0, ((0, 4), (1, 8)))
    w_query = bell_draw(splits[2], (D, D), D ** -0.5, 0.15625, ((0, 4),))
    w_key = bell_draw(splits[3], (D, D), D ** -0.5, 0.15625, ((0, 4),))
    w_value = bell_draw(splits[4], (D, D), D ** -0.5, 0.15625, ((0, 4),))
    w_out = bell_draw(splits[5], (D, D), (D // 64) ** -0.5, 1.25, ((0, 4),))
    w_fc = bell_draw(splits[6], (D, FF), D ** -0.5, 0.15625, ((0, 4),))
    w_proj = bell_draw(splits[7], (FF, D), FF ** -0.5, 0.078125, ((0, 4),))
    ln1_gain = jnp.clip(1.0 + 0.18 * jax.random.normal(splits[8], (D,), jnp.float32), 0.099609375, 1.8984375).astype(jnp.bfloat16)
    ln1_bias = bell_draw(splits[9], (D,), 0.5, 3.0, ((0, 4),))
    query_bias = bell_draw(splits[10], (D,), 0.5, 3.0, ((0, 4),))
    value_bias = bell_draw(splits[11], (D,), 0.5, 3.0, ((0, 4),))
    out_bias = bell_draw(splits[12], (D,), 0.5, 3.0, ((0, 4),))
    ln2_gain = jnp.clip(1.0 + 0.18 * jax.random.normal(splits[13], (D,), jnp.float32), 0.099609375, 1.8984375).astype(jnp.bfloat16)
    ln2_bias = bell_draw(splits[14], (D,), 0.5, 3.0, ((0, 4),))
    fc_bias = bell_draw(splits[15], (FF,), 0.5, 3.0, ((0, 4),))
    proj_bias = bell_draw(splits[16], (D,), 0.5, 3.0, ((0, 4),))
    return dict(inputs=inputs, cotangent=cotangent, w_query=w_query, w_key=w_key, w_value=w_value, w_out=w_out, w_fc=w_fc, w_proj=w_proj, ln1_gain=ln1_gain, ln1_bias=ln1_bias, query_bias=query_bias, value_bias=value_bias, out_bias=out_bias, ln2_gain=ln2_gain, ln2_bias=ln2_bias, fc_bias=fc_bias, proj_bias=proj_bias)


@jax.custom_vjp
def low(v):
    return lax.optimization_barrier(v.astype(jnp.bfloat16)).astype(jnp.float32)

@jax.custom_vjp
def low_back(v):
    return v

def low_keep(v):
    return (low(v), None)

def low_pass(kept, grad):
    return (grad,)

def back_keep(v):
    return (v, None)

def back_low(kept, grad):
    return (low(grad),)
low.defvjp(low_keep, low_pass)
low_back.defvjp(back_keep, back_low)
EPS = 1e-05
SCALE = 0.125
NEGATIVE = -1000000000.0
ROOT = 0.7978845608028654
CUBIC = 0.044715
HIGH = lax.Precision.HIGHEST

def positions():
    index = jnp.arange(LEN, dtype=jnp.int32)
    owner = index // ROWS
    inner = index % ROWS
    second = inner // HALF
    blocks = jnp.where(second == 0, owner, 2 * N_CTX - 1 - owner)
    return (blocks * HALF + inner % HALF).astype(jnp.int32)

def layer_norm(values, gain, shift):
    centre = lax.optimization_barrier(jnp.mean(values, axis=-1, keepdims=True))
    centred = values - centre
    spread = lax.optimization_barrier(jnp.mean(centred * centred, axis=-1, keepdims=True))
    return centred * lax.rsqrt(spread + EPS) * gain + shift

def gelu_tanh(values):
    return 0.5 * values * (1.0 + jnp.tanh(ROOT * (values + CUBIC * values * values * values)))

def attend(queries, keys, values, places):
    block = min(512, LEN)
    count = LEN // block
    heads_q = queries.reshape(count, block, HEADS, HEAD)
    heads_k = keys.reshape(LEN, HEADS, HEAD)
    heads_v = values.reshape(LEN, HEADS, HEAD)
    block_places = places.reshape(count, block)

    def one_block(item):
        query_block, query_places = item
        raw = jnp.einsum('qhd,khd->hqk', query_block, heads_k, precision=HIGH) * SCALE
        allowed = places[None, None, :] <= query_places[None, :, None]
        scores = low_back(jnp.where(allowed, raw, NEGATIVE))
        weights = low(jax.nn.softmax(scores, axis=-1))
        return jnp.einsum('hqk,khd->qhd', weights, heads_v, precision=HIGH)
    result = lax.map(jax.checkpoint(one_block), (heads_q, block_places))
    return result.reshape(LEN, D)

def layer(values, places, w_query, w_key, w_value, w_out, w_fc, w_proj, ln1_gain, ln1_bias, query_bias, value_bias, out_bias, ln2_gain, ln2_bias, fc_bias, proj_bias):
    normed_one = low(layer_norm(values, ln1_gain, ln1_bias))
    queries = low(low_back(jnp.dot(normed_one, w_query, precision=HIGH) + query_bias))
    keys = low(low_back(jnp.dot(normed_one, w_key, precision=HIGH)))
    vals = low(low_back(jnp.dot(normed_one, w_value, precision=HIGH) + value_bias))
    attended = low(low_back(attend(queries, keys, vals, places)))
    resid = values + low_back(jnp.dot(attended, w_out, precision=HIGH) + out_bias)
    normed_two = low(layer_norm(resid, ln2_gain, ln2_bias))
    pre_act = low_back(jnp.dot(normed_two, w_fc, precision=HIGH) + fc_bias)
    activated = low(gelu_tanh(pre_act))
    return resid + jnp.dot(activated, w_proj, precision=HIGH) + proj_bias

def reference(inputs, cotangent, w_query, w_key, w_value, w_out, w_fc, w_proj, ln1_gain, ln1_bias, query_bias, value_bias, out_bias, ln2_gain, ln2_bias, fc_bias, proj_bias):
    params = tuple((param.astype(jnp.float32) for param in (w_query, w_key, w_value, w_out, w_fc, w_proj, ln1_gain, ln1_bias, query_bias, value_bias, out_bias, ln2_gain, ln2_bias, fc_bias, proj_bias)))
    places = positions()

    def forward(values, *weights):
        return layer(values, places, *weights)

    def one_sequence(totals, item):
        seq_in, seq_cot = item
        result, pullback = jax.vjp(forward, seq_in.astype(jnp.float32), *params)
        grads = pullback(seq_cot.astype(jnp.float32))
        totals = tuple((left + right for left, right in zip(totals, grads[1:])))
        return (totals, (result.astype(jnp.bfloat16), grads[0]))
    start = tuple((jnp.zeros_like(param) for param in params))
    totals, (outputs, input_grad) = lax.scan(one_sequence, start, (inputs, cotangent))
    return (outputs, input_grad, totals[0], totals[1], totals[2], totals[3], totals[4], totals[5], totals[6], totals[7], totals[8], totals[9], totals[10], totals[11], totals[12], totals[13], totals[14])
```

```python
import functools

import jax
import jax.numpy as jnp
from jax import lax
from jax.experimental import pallas as pl
from jax.experimental.pallas import tpu as pltpu
from jax.sharding import PartitionSpec as P

HEADS = 25
HEAD = 64
EPS = 1e-05
SCALE = 0.125
NEGATIVE = -1000000000.0
ROOT = 0.7978845608028654
CUBIC = 0.044715
LANES = 128
F32 = jnp.float32
BF16 = jnp.bfloat16


def normalize(values):
    centre = jnp.mean(values, axis=-1, keepdims=True)
    centred = values - centre
    spread = jnp.mean(centred * centred, axis=-1, keepdims=True)
    inv_std = lax.rsqrt(spread + EPS)
    return (centred * inv_std, inv_std)


def norm_back(grad_norm, gain, normal, inv_std):
    scaled = grad_norm * gain
    return inv_std * (
        scaled
        - jnp.mean(scaled, axis=-1, keepdims=True)
        - normal * jnp.mean(scaled * normal, axis=-1, keepdims=True)
    )


def gelu_both(values):
    tangent = jnp.tanh(ROOT * (values + CUBIC * values * values * values))
    value = 0.5 * values * (1.0 + tangent)
    slope = 0.5 * (1.0 + tangent) + 0.5 * values * (1.0 - tangent * tangent) * ROOT * (
        1.0 + 3.0 * CUBIC * values * values
    )
    return value, slope


def dot(left, right):
    return jnp.dot(left, right, preferred_element_type=F32)


def dot_nt(left, right):
    return lax.dot_general(left, right, (((1,), (1,)), ((), ())), preferred_element_type=F32)


def dot_tn(left, right):
    return lax.dot_general(left, right, (((0,), (0,)), ((), ())), preferred_element_type=F32)


def lane_half(shape, half):
    lane = lax.broadcasted_iota(jnp.int32, shape, 1)
    return (lane < HEAD) if half == 0 else (lane >= HEAD)


def keep_half(array, half):
    return jnp.where(lane_half(array.shape, half), array, jnp.zeros_like(array))


def causal_tail(scores, first_row, block):
    keys = lax.broadcasted_iota(jnp.int32, scores.shape, 0) + first_row
    queries = lax.broadcasted_iota(jnp.int32, scores.shape, 1)
    return jnp.where(keys <= queries, scores, NEGATIVE)


def attend_kernel(block, heads, q_ref, k_ref, v_ref, o_ref, ot_ref, lse_ref):
    length = q_ref.shape[0]
    pair = pl.program_id(0)
    v_t = jnp.transpose(v_ref[...].astype(F32)).astype(BF16)

    def one_head(half):
        for index in range(length // block):
            rows = slice(index * block, (index + 1) * block)
            count = (index + 1) * block
            query = keep_half(q_ref[rows, :], half) * jnp.asarray(SCALE, BF16)
            scores = dot_nt(k_ref[:count, :], query)
            scores = causal_tail(scores, -index * block, block)
            top = jnp.max(scores, axis=0, keepdims=True)
            weights = jnp.exp(scores - top)
            total = jnp.sum(weights, axis=0, keepdims=True)
            lse_ref[0, half : half + 1, rows] = top + jnp.log(total)
            weights = weights * (1.0 / total)
            ot = dot(v_t[half * HEAD : (half + 1) * HEAD, :count], weights.astype(BF16))
            ot_ref[0, half * HEAD : (half + 1) * HEAD, rows] = ot

    one_head(0)

    @pl.when(2 * pair + 1 < heads)
    def _():
        one_head(1)

    @pl.when(2 * pair + 1 >= heads)
    def _():
        ot_ref[0, HEAD:, :] = jnp.zeros((HEAD, length), F32)
        lse_ref[0, 1:2, :] = jnp.zeros((1, length), F32)

    o_ref[...] = jnp.transpose(ot_ref[0]).astype(BF16)


def attend(queries, keys, values, heads):
    length, width = queries.shape
    pairs = width // LANES
    block = min(256, length)
    column = pl.BlockSpec((length, LANES), lambda p: (0, p))
    return pl.pallas_call(
        functools.partial(attend_kernel, block, heads),
        grid=(pairs,),
        in_specs=[column] * 3,
        out_specs=[
            column,
            pl.BlockSpec((1, LANES, length), lambda p: (p, 0, 0)),
            pl.BlockSpec((1, 2, length), lambda p: (p, 0, 0)),
        ],
        out_shape=[
            jax.ShapeDtypeStruct((length, width), BF16),
            jax.ShapeDtypeStruct((pairs, LANES, length), F32),
            jax.ShapeDtypeStruct((pairs, 2, length), F32),
        ],
        name="attend",
    )(queries, keys, values)


def attend_back_kernel(
    block, heads, q_ref, k_ref, v_ref, do_ref, ot_ref, lse_ref, dq_ref, dk_ref, dv_ref, dk_sum, dv_sum
):
    length = q_ref.shape[0]
    pair = pl.program_id(0)
    k_t = jnp.transpose(k_ref[...].astype(F32)).astype(BF16)
    do_t = jnp.transpose(do_ref[...].astype(F32))
    dk_sum[...] = jnp.zeros_like(dk_sum)
    dv_sum[...] = jnp.zeros_like(dv_sum)
    dq_ref[...] = jnp.zeros_like(dq_ref)

    def one_head(half):
        span = slice(half * HEAD, (half + 1) * HEAD)
        shared = jnp.sum(do_t[span, :] * ot_ref[0, span, :], axis=0, keepdims=True)
        for index in range(length // block):
            rows = slice(index * block, (index + 1) * block)
            count = (index + 1) * block
            query = keep_half(q_ref[rows, :], half) * jnp.asarray(SCALE, BF16)
            grad = keep_half(do_ref[rows, :], half)
            scores = dot_nt(k_ref[:count, :], query)
            scores = causal_tail(scores, -index * block, block)
            probs = jnp.exp(scores - lse_ref[0, half : half + 1, rows])
            grad_probs = dot_nt(v_ref[:count, :], grad)
            grad_scores = (probs * (grad_probs - shared[:, rows])).astype(BF16)
            dv_sum[:count, :] += dot(probs.astype(BF16), grad)
            dk_sum[:count, :] += dot(grad_scores, query)
            dq_t = dot(k_t[span, :count], grad_scores) * SCALE
            pad = jnp.zeros_like(dq_t)
            both = jnp.concatenate([dq_t, pad] if half == 0 else [pad, dq_t], axis=0)
            dq_ref[rows, :] = dq_ref[rows, :] + jnp.transpose(both).astype(BF16)

    one_head(0)

    @pl.when(2 * pair + 1 < heads)
    def _():
        one_head(1)

    dk_ref[...] = dk_sum[...].astype(BF16)
    dv_ref[...] = dv_sum[...].astype(BF16)


def attend_back(queries, keys, values, grad, ot, lse, heads):
    length, width = queries.shape
    pairs = width // LANES
    block = min(256, length)
    column = pl.BlockSpec((length, LANES), lambda p: (0, p))
    return pl.pallas_call(
        functools.partial(attend_back_kernel, block, heads),
        grid=(pairs,),
        in_specs=[column] * 4
        + [
            pl.BlockSpec((1, LANES, length), lambda p: (p, 0, 0)),
            pl.BlockSpec((1, 2, length), lambda p: (p, 0, 0)),
        ],
        out_specs=[column] * 3,
        out_shape=[jax.ShapeDtypeStruct((length, width), BF16)] * 3,
        scratch_shapes=[pltpu.VMEM((length, LANES), F32)] * 2,
        name="attend_back",
    )(queries, keys, values, grad, ot, lse)


def on_device(
    inputs,
    cotangent,
    w_query,
    w_key,
    w_value,
    w_out,
    w_fc,
    w_proj,
    ln1_gain,
    ln1_bias,
    query_bias,
    value_bias,
    out_bias,
    ln2_gain,
    ln2_bias,
    fc_bias,
    proj_bias,
):
    parts = lax.axis_size("fsdp")
    n_ctx = lax.axis_size("ctx")
    me_ctx = lax.axis_index("ctx")
    me_part = lax.axis_index("fsdp")
    seqs, rows, width = inputs.shape
    hidden = w_fc.shape[1]
    quarter = width // parts
    hidden_part = hidden // parts
    own = seqs * rows
    all_seqs = seqs * parts
    tokens = all_seqs * rows
    length = rows * n_ctx
    half_rows = rows // 2
    groups = n_ctx // all_seqs
    heads_part = -(-HEADS // parts)
    live = heads_part * HEAD
    slots = -(-heads_part // (2 * groups)) * 2 * groups
    cols = slots * HEAD
    piece = cols // groups
    heads_here = heads_part if groups == 1 else slots // groups
    near = (live - quarter) * parts

    def gather(array):
        return lax.all_gather(array, "fsdp", axis=0, tiled=True)

    def scatter(array):
        return lax.psum_scatter(array.astype(BF16), "fsdp", scatter_dimension=0, tiled=True)

    def to_slots(array):
        lead = array.shape[:-1]
        array = jnp.pad(array, [(0, 0)] * len(lead) + [(0, parts * live - width)])
        array = array.reshape(*lead, parts, live)
        array = jnp.pad(array, [(0, 0)] * len(lead) + [(0, 0), (0, cols - live)])
        return array.reshape(*lead, parts * cols)

    small = jnp.concatenate(
        [ln1_gain, ln1_bias, query_bias, value_bias, out_bias, ln2_gain, ln2_bias, proj_bias]
    )[None, :]
    small = gather(small).astype(F32).reshape(parts, 8, quarter)
    gain_one, shift_one, bias_query, bias_value, bias_out, gain_two, shift_two, bias_proj = [
        small[:, i].reshape(-1) for i in range(8)
    ]
    bias_query = lax.dynamic_slice_in_dim(to_slots(bias_query), me_part * cols, cols, 0)
    bias_value = lax.dynamic_slice_in_dim(to_slots(bias_value), me_part * cols, cols, 0)
    bias_fc = fc_bias.astype(F32)

    qkv = to_slots(jnp.stack([w_query, w_key, w_value]))
    qkv = lax.all_to_all(qkv, "fsdp", split_axis=2, concat_axis=1, tiled=True)
    fc = lax.all_to_all(w_fc, "fsdp", split_axis=1, concat_axis=0, tiled=True)
    proj = w_proj
    from_right = lax.ppermute(w_out[:near], "fsdp", [(i + 1, i) for i in range(parts - 1)])
    out_w = lax.dynamic_slice_in_dim(
        jnp.concatenate([w_out, from_right]), me_part * (live - quarter), live, 0
    )
    out_w = jnp.pad(out_w, ((0, cols - live), (0, 0)))

    x_full = inputs.astype(F32).reshape(own, width)
    hat_one, inv_one = normalize(x_full)
    normed_one = gather((hat_one * gain_one + shift_one).astype(BF16))
    grad_y = gather(cotangent.reshape(own, width))
    queries = (dot(normed_one, qkv[0]) + bias_query).astype(BF16)
    keys = dot(normed_one, qkv[1]).astype(BF16)
    values = (dot(normed_one, qkv[2]) + bias_value).astype(BF16)

    def to_heads(array):
        array = array.reshape(all_seqs, rows, groups, piece)
        array = jnp.transpose(array, (0, 2, 1, 3)).reshape(n_ctx, rows, piece)
        array = lax.all_to_all(array, "ctx", split_axis=0, concat_axis=0, tiled=True)
        first, second = array[:, :half_rows], array[:, half_rows:]
        return jnp.concatenate([first, second[::-1]]).reshape(length, piece)

    def from_heads(array):
        array = array.reshape(2 * n_ctx, half_rows, piece)
        array = jnp.concatenate([array[:n_ctx], array[n_ctx:][::-1]], axis=1)
        array = lax.all_to_all(array, "ctx", split_axis=0, concat_axis=0, tiled=True)
        array = array.reshape(all_seqs, groups, rows, piece)
        return jnp.transpose(array, (0, 2, 1, 3)).reshape(tokens, cols)

    q_seq, k_seq, v_seq = to_heads(queries), to_heads(keys), to_heads(values)
    o_seq, ot, lse = attend(q_seq, k_seq, v_seq, heads_here)
    attended = from_heads(o_seq)
    resid = x_full + scatter(dot(attended, out_w)).astype(F32) + bias_out

    hat_two, inv_two = normalize(resid)
    normed_two = gather((hat_two * gain_two + shift_two).astype(BF16))
    pre_act = dot(normed_two, fc) + bias_fc
    value, slope = gelu_both(pre_act)
    activated = value.astype(BF16)
    mlp = scatter(dot(activated, proj)).astype(F32)
    outputs = (resid + mlp + bias_proj).astype(BF16).reshape(seqs, rows, width)

    grad_pre = (dot_nt(grad_y, proj) * slope).astype(BF16)
    grad_norm_two = scatter(dot_nt(grad_pre, fc)).astype(F32)
    grad_y_own = cotangent.reshape(own, width).astype(F32)
    grad_gain_two = jnp.sum(grad_norm_two * hat_two, axis=0)
    grad_shift_two = jnp.sum(grad_norm_two, axis=0)
    grad_bias_proj = jnp.sum(grad_y_own, axis=0)
    grad_bias_fc = jnp.sum(grad_pre.astype(F32), axis=0)
    grad_resid = grad_y_own + norm_back(grad_norm_two, gain_two, hat_two, inv_two)
    grad_branch = grad_resid.astype(BF16)
    grad_bias_out = jnp.sum(grad_branch.astype(F32), axis=0)
    grad_branch = gather(grad_branch)
    grad_attended = dot_nt(grad_branch, out_w).astype(BF16)

    dq_seq, dk_seq, dv_seq = attend_back(
        q_seq, k_seq, v_seq, to_heads(grad_attended), ot, lse, heads_here
    )
    grad_qkv = jnp.stack([from_heads(dq_seq), from_heads(dk_seq), from_heads(dv_seq)])
    grad_norm_one = scatter(
        dot_nt(grad_qkv[0], qkv[0]) + dot_nt(grad_qkv[1], qkv[1]) + dot_nt(grad_qkv[2], qkv[2])
    ).astype(F32)
    grad_bias_query = jnp.sum(grad_qkv[0].astype(F32), axis=0)
    grad_bias_value = jnp.sum(grad_qkv[2].astype(F32), axis=0)
    grad_gain_one = jnp.sum(grad_norm_one * hat_one, axis=0)
    grad_shift_one = jnp.sum(grad_norm_one, axis=0)
    input_grad = grad_resid + norm_back(grad_norm_one, gain_one, hat_one, inv_one)
    input_grad = input_grad.reshape(seqs, rows, width)

    per = n_ctx // parts
    slab = width // n_ctx
    proj_part = dot_tn(activated, grad_y).astype(BF16)
    fc_part = dot_tn(normed_two, grad_pre).astype(BF16)
    qkv_part = [dot_tn(normed_one, grad_qkv[i]).astype(BF16) for i in range(3)]
    out_part = dot_tn(attended, grad_branch).astype(BF16)

    def total(array):
        return lax.all_gather(
            lax.psum_scatter(array, "ctx", scatter_dimension=0, tiled=True), "ctx", axis=0, tiled=True
        )

    proj_grad = total(proj_part).astype(F32)
    out_grad = total(out_part)

    def across(array):
        n = array.shape[1]
        array = array.reshape(n_ctx, slab, n)
        array = jnp.roll(array, -per * me_part, axis=0)
        array = lax.psum_scatter(array, "ctx", scatter_dimension=0, tiled=True)
        pairs = [
            (c * parts + f, c * parts + (f + c // per) % parts)
            for c in range(n_ctx)
            for f in range(parts)
        ]
        array = lax.ppermute(array, ("ctx", "fsdp"), pairs)
        array = lax.all_gather(array, "ctx", axis=0, tiled=True)
        array = array.reshape(parts, per, slab, n)
        order = (me_part - jnp.arange(parts)) % parts
        array = jnp.take(array, order, axis=0)
        return jnp.transpose(array, (1, 2, 0, 3)).reshape(quarter, parts, n)

    fc_grad = across(fc_part).reshape(quarter, hidden).astype(F32)
    qkv_grad = [
        across(part)[:, :, :live].reshape(quarter, parts * live)[:, :width].astype(F32)
        for part in qkv_part
    ]
    out_rows = out_grad[:live]
    from_left = lax.ppermute(out_rows[live - near :], "fsdp", [(i, i + 1) for i in range(parts - 1)])
    out_rows = lax.dynamic_slice_in_dim(
        jnp.concatenate([from_left, out_rows]), near - me_part * (live - quarter), quarter, 0
    ).astype(F32)

    def window(vector):
        whole = jnp.zeros((parts * live,), F32)
        return lax.dynamic_update_slice_in_dim(whole, vector[:live], me_part * live, 0)[:width]

    small_grads = jnp.stack(
        [
            grad_gain_one,
            grad_shift_one,
            window(grad_bias_query),
            window(grad_bias_value),
            grad_bias_out,
            grad_gain_two,
            grad_shift_two,
            grad_bias_proj,
        ]
    )
    small_grads = lax.psum(small_grads, ("ctx", "fsdp"))
    small_grads = lax.dynamic_slice_in_dim(small_grads, me_part * quarter, quarter, 1)
    fc_bias_grad = lax.psum(grad_bias_fc, "ctx")
    return (
        outputs,
        input_grad,
        qkv_grad[0],
        qkv_grad[1],
        qkv_grad[2],
        out_rows,
        fc_grad,
        proj_grad,
        small_grads[0],
        small_grads[1],
        small_grads[2],
        small_grads[3],
        small_grads[4],
        small_grads[5],
        small_grads[6],
        fc_bias_grad,
        small_grads[7],
    )


def solution(mesh):
    tokens = P("fsdp", "ctx", None)
    matrix = P("fsdp", None)
    vector = P("fsdp")
    return jax.shard_map(
        on_device,
        mesh=mesh,
        in_specs=(tokens, tokens) + (matrix,) * 6 + (vector,) * 9,
        out_specs=(tokens, tokens) + (matrix,) * 6 + (vector,) * 9,
        check_vma=False,
    )
```

```python
import functools

import jax
import jax.numpy as jnp
from jax import lax
from jax.experimental import pallas as pl
from jax.experimental.pallas import tpu as pltpu
from jax.sharding import PartitionSpec as P

HEADS = 25
HEAD = 64
EPS = 1e-05
SCALE = 0.125
NEGATIVE = -1000000000.0
ROOT = 0.7978845608028654
CUBIC = 0.044715
LANES = 128
F32 = jnp.float32
BF16 = jnp.bfloat16


def normalize(values):
    centre = jnp.mean(values, axis=-1, keepdims=True)
    centred = values - centre
    spread = jnp.mean(centred * centred, axis=-1, keepdims=True)
    inv_std = lax.rsqrt(spread + EPS)
    return (centred * inv_std, inv_std)


def norm_back(grad_norm, gain, normal, inv_std):
    scaled = grad_norm * gain
    return inv_std * (
        scaled
        - jnp.mean(scaled, axis=-1, keepdims=True)
        - normal * jnp.mean(scaled * normal, axis=-1, keepdims=True)
    )


def gelu_both(values):
    tangent = jnp.tanh(ROOT * (values + CUBIC * values * values * values))
    value = 0.5 * values * (1.0 + tangent)
    slope = 0.5 * (1.0 + tangent) + 0.5 * values * (1.0 - tangent * tangent) * ROOT * (
        1.0 + 3.0 * CUBIC * values * values
    )
    return value, slope


def dot(left, right):
    return jnp.dot(left, right, preferred_element_type=F32)


def dot_nt(left, right):
    return lax.dot_general(left, right, (((1,), (1,)), ((), ())), preferred_element_type=F32)


def dot_tn(left, right):
    return lax.dot_general(left, right, (((0,), (0,)), ((), ())), preferred_element_type=F32)


def lane_half(shape, half):
    lane = lax.broadcasted_iota(jnp.int32, shape, 1)
    return (lane < HEAD) if half == 0 else (lane >= HEAD)


def keep_half(array, half):
    return jnp.where(lane_half(array.shape, half), array, jnp.zeros_like(array))


def causal_tail(scores, first_row, block):
    keys = lax.broadcasted_iota(jnp.int32, scores.shape, 0) + first_row
    queries = lax.broadcasted_iota(jnp.int32, scores.shape, 1)
    return jnp.where(keys <= queries, scores, NEGATIVE)


def attend_kernel(block, heads, q_ref, k_ref, v_ref, o_ref, ot_ref, lse_ref):
    length = q_ref.shape[0]
    pair = pl.program_id(0)
    v_t = jnp.transpose(v_ref[...].astype(F32)).astype(BF16)

    def one_head(half):
        for index in range(length // block):
            rows = slice(index * block, (index + 1) * block)
            count = (index + 1) * block
            query = keep_half(q_ref[rows, :], half) * jnp.asarray(SCALE, BF16)
            scores = dot_nt(k_ref[:count, :], query)
            scores = causal_tail(scores, -index * block, block)
            top = jnp.max(scores, axis=0, keepdims=True)
            weights = jnp.exp(scores - top)
            total = jnp.sum(weights, axis=0, keepdims=True)
            lse_ref[0, half : half + 1, rows] = top + jnp.log(total)
            weights = weights * (1.0 / total)
            ot = dot(v_t[half * HEAD : (half + 1) * HEAD, :count], weights.astype(BF16))
            ot_ref[0, half * HEAD : (half + 1) * HEAD, rows] = ot

    one_head(0)

    @pl.when(2 * pair + 1 < heads)
    def _():
        one_head(1)

    @pl.when(2 * pair + 1 >= heads)
    def _():
        ot_ref[0, HEAD:, :] = jnp.zeros((HEAD, length), F32)
        lse_ref[0, 1:2, :] = jnp.zeros((1, length), F32)

    o_ref[...] = jnp.transpose(ot_ref[0]).astype(BF16)


def attend(queries, keys, values, heads):
    length, width = queries.shape
    pairs = width // LANES
    block = min(256, length)
    column = pl.BlockSpec((length, LANES), lambda p: (0, p))
    return pl.pallas_call(
        functools.partial(attend_kernel, block, heads),
        grid=(pairs,),
        in_specs=[column] * 3,
        out_specs=[
            column,
            pl.BlockSpec((1, LANES, length), lambda p: (p, 0, 0)),
            pl.BlockSpec((1, 2, length), lambda p: (p, 0, 0)),
        ],
        out_shape=[
            jax.ShapeDtypeStruct((length, width), BF16),
            jax.ShapeDtypeStruct((pairs, LANES, length), F32),
            jax.ShapeDtypeStruct((pairs, 2, length), F32),
        ],
        name="attend",
    )(queries, keys, values)


def attend_back_kernel(
    block, heads, q_ref, k_ref, v_ref, do_ref, ot_ref, lse_ref, dq_ref, dk_ref, dv_ref, dk_sum, dv_sum
):
    length = q_ref.shape[0]
    pair = pl.program_id(0)
    k_t = jnp.transpose(k_ref[...].astype(F32)).astype(BF16)
    do_t = jnp.transpose(do_ref[...].astype(F32))
    dk_sum[...] = jnp.zeros_like(dk_sum)
    dv_sum[...] = jnp.zeros_like(dv_sum)
    dq_ref[...] = jnp.zeros_like(dq_ref)

    def one_head(half):
        span = slice(half * HEAD, (half + 1) * HEAD)
        shared = jnp.sum(do_t[span, :] * ot_ref[0, span, :], axis=0, keepdims=True)
        for index in range(length // block):
            rows = slice(index * block, (index + 1) * block)
            count = (index + 1) * block
            query = keep_half(q_ref[rows, :], half) * jnp.asarray(SCALE, BF16)
            grad = keep_half(do_ref[rows, :], half)
            scores = dot_nt(k_ref[:count, :], query)
            scores = causal_tail(scores, -index * block, block)
            probs = jnp.exp(scores - lse_ref[0, half : half + 1, rows])
            grad_probs = dot_nt(v_ref[:count, :], grad)
            grad_scores = (probs * (grad_probs - shared[:, rows])).astype(BF16)
            dv_sum[:count, :] += dot(probs.astype(BF16), grad)
            dk_sum[:count, :] += dot(grad_scores, query)
            dq_t = dot(k_t[span, :count], grad_scores) * SCALE
            pad = jnp.zeros_like(dq_t)
            both = jnp.concatenate([dq_t, pad] if half == 0 else [pad, dq_t], axis=0)
            dq_ref[rows, :] = dq_ref[rows, :] + jnp.transpose(both).astype(BF16)

    one_head(0)

    @pl.when(2 * pair + 1 < heads)
    def _():
        one_head(1)

    dk_ref[...] = dk_sum[...].astype(BF16)
    dv_ref[...] = dv_sum[...].astype(BF16)


def attend_back(queries, keys, values, grad, ot, lse, heads):
    length, width = queries.shape
    pairs = width // LANES
    block = min(256, length)
    column = pl.BlockSpec((length, LANES), lambda p: (0, p))
    return pl.pallas_call(
        functools.partial(attend_back_kernel, block, heads),
        grid=(pairs,),
        in_specs=[column] * 4
        + [
            pl.BlockSpec((1, LANES, length), lambda p: (p, 0, 0)),
            pl.BlockSpec((1, 2, length), lambda p: (p, 0, 0)),
        ],
        out_specs=[column] * 3,
        out_shape=[jax.ShapeDtypeStruct((length, width), BF16)] * 3,
        scratch_shapes=[pltpu.VMEM((length, LANES), F32)] * 2,
        name="attend_back",
    )(queries, keys, values, grad, ot, lse)


class Place:
    def __init__(self):
        self.parts = lax.axis_size("fsdp")
        self.n_ctx = lax.axis_size("ctx")
        self.part = lax.axis_index("fsdp")
        self.ctx = lax.axis_index("ctx")
        self.beside = self.part + 1 - 2 * (self.part % 2)
        self.far = (self.part + 2) % self.parts
        self.diagonal = (self.beside + 2) % self.parts

    def at(self, position):
        n = self.n_ctx
        position = (position + 2 * n) % n
        upper = position // (n // 2)
        return (1 - upper) * 2 * position + upper * (2 * (n - 1 - position) + 1)

    @property
    def position(self):
        odd = self.ctx % 2
        return (1 - odd) * (self.ctx // 2) + odd * (self.n_ctx - 1 - self.ctx // 2)


def remote(source, target, send, recv, **where):
    return pltpu.make_async_remote_copy(
        src_ref=source,
        dst_ref=target,
        send_sem=send,
        recv_sem=recv,
        device_id=where,
        device_id_type=pl.DeviceIdType.MESH,
    )


def cut(rows):
    step = 64 if rows % 64 == 0 else rows
    return [slice(start, start + step) for start in range(0, rows, step)]


class Gather:
    reach = ("fsdp",)

    def __init__(self, array):
        self.ins = [array]
        self.parts = lax.axis_size("fsdp")
        self.pieces = cut(array.shape[0])
        self.outs = [jax.ShapeDtypeStruct((self.parts, *array.shape), array.dtype)]
        self.scratch = [pltpu.SemaphoreType.DMA((3, len(self.pieces)))] * 2

    def phases(self, place, ins, outs, scratch):
        (source,), (out,), (send, recv) = ins, outs, scratch
        count = range(len(self.pieces))

        def copy(kind, k, index, target):
            piece = self.pieces[k]
            start = source.at[piece] if kind < 2 else out.at[index, piece]
            return remote(start, out.at[index, piece], send.at[kind, k], recv.at[kind, k], fsdp=target)

        def first():
            for k in count:
                copy(1, k, place.part, place.far).start()
            for k in count:
                copy(0, k, place.part, place.beside).start()
            out[place.part] = source[...]

        def second():
            for k in count:
                copy(1, k, place.far, place.far).wait_recv()
                copy(2, k, place.far, place.beside).start()

        def third():
            for k in count:
                copy(0, k, place.beside, place.beside).wait_recv()
                copy(2, k, place.diagonal, place.beside).wait_recv()
            for k in count:
                copy(0, k, place.part, place.beside).wait_send()
                copy(1, k, place.part, place.far).wait_send()
                copy(2, k, place.far, place.beside).wait_send()

        return [first, second, third]


class Scatter:
    reach = ("fsdp",)

    def __init__(self, array):
        parts, rows, columns = array.shape
        self.ins = [array]
        self.pieces = cut(rows)
        self.outs = [jax.ShapeDtypeStruct((rows, columns), F32)]
        self.scratch = [pltpu.VMEM((rows, columns), array.dtype)] * 3
        self.scratch += [pltpu.SemaphoreType.DMA((3, len(self.pieces)))] * 2

    def phases(self, place, ins, outs, scratch):
        (source,), (out,) = ins, outs
        for_far, for_own, from_far, send, recv = scratch
        count = range(len(self.pieces))

        def copy(kind, k):
            piece = self.pieces[k]
            start, target, where = [
                (source.at[place.diagonal, piece], for_far, place.beside),
                (source.at[place.beside, piece], for_own, place.beside),
                (for_far.at[piece], from_far, place.far),
            ][kind]
            return remote(start, target.at[piece], send.at[kind, k], recv.at[kind, k], fsdp=where)

        def first():
            for k in count:
                copy(0, k).start()
            for k in count:
                copy(1, k).start()

        def second():
            for k in count:
                piece = self.pieces[k]
                copy(0, k).wait_recv()
                total = for_far[piece].astype(F32) + source[place.far, piece].astype(F32)
                for_far[piece] = total.astype(for_far.dtype)
                copy(2, k).start()

        def third():
            for k in count:
                piece = self.pieces[k]
                copy(1, k).wait_recv()
                out[piece] = for_own[piece].astype(F32) + source[place.part, piece].astype(F32)

        def fourth():
            for k in count:
                piece = self.pieces[k]
                copy(2, k).wait_recv()
                out[piece] += from_far[piece].astype(F32)
            for k in count:
                for kind in range(3):
                    copy(kind, k).wait_send()

        return [first, second, third, fourth]


class ToHeads:
    reach = ("ctx",)

    def __init__(self, arrays):
        seqs, _, half, columns = arrays[0].shape
        self.n = lax.axis_size("ctx")
        self.groups = self.n // seqs
        self.piece = columns // self.groups
        self.ins = list(arrays)
        self.outs = [jax.ShapeDtypeStruct((2 * self.n, half, self.piece), a.dtype) for a in arrays]
        self.scratch = [pltpu.SemaphoreType.DMA((len(arrays), 2, self.n))] * 2

    def whole(self, ref, other, half):
        if self.groups == 1:
            return ref.at[other, half]
        column = pl.multiple_of((other % self.groups) * self.piece, LANES)
        return ref.at[other // self.groups, half, :, pl.ds(column, self.piece)]

    def block(self, ref, other, half):
        return ref.at[other if half == 0 else 2 * self.n - 1 - other]

    def source(self, ref, other, half):
        return self.whole(ref, other, half)

    def target(self, ref, other, half):
        return self.block(ref, other, half)

    def phases(self, place, ins, outs, scratch):
        send, recv = scratch
        n, me = self.n, place.ctx
        every = [(i, half) for i in range(len(ins)) for half in range(2)]

        def first():
            def begin(step, _):
                other = (me + step) % n
                for i, half in every:
                    remote(
                        self.source(ins[i], other, half),
                        self.target(outs[i], me, half),
                        send.at[i, half, step],
                        recv.at[i, half, step],
                        ctx=other,
                    ).start()
                return 0

            lax.fori_loop(1, n, begin, 0)
            for i, half in every:
                self.target(outs[i], me, half)[...] = self.source(ins[i], me, half)[...]

        def second():
            def end(step, _):
                other = (me + n - step) % n
                for i, half in every:
                    copy = remote(
                        self.source(ins[i], other, half),
                        self.target(outs[i], other, half),
                        send.at[i, half, step],
                        recv.at[i, half, step],
                        ctx=other,
                    )
                    copy.wait_recv()
                    copy.wait_send()
                return 0

            lax.fori_loop(1, n, end, 0)

        return [first, second]


class FromHeads(ToHeads):
    def __init__(self, arrays, seqs):
        blocks, half, piece = arrays[0].shape
        self.n = blocks // 2
        self.groups = self.n // seqs
        self.piece = piece
        self.ins = list(arrays)
        shape = (seqs, 2, half, piece * self.groups)
        self.outs = [jax.ShapeDtypeStruct(shape, a.dtype) for a in arrays]
        self.scratch = [pltpu.SemaphoreType.DMA((len(arrays), 2, self.n))] * 2

    def source(self, ref, other, half):
        return self.block(ref, other, half)

    def target(self, ref, other, half):
        return self.whole(ref, other, half)


class Swap:
    reach = ("fsdp",)

    def __init__(self, arrays, live, wide):
        self.parts = lax.axis_size("fsdp")
        self.live, self.wide = live, wide
        self.ins = list(arrays)
        rows = arrays[0].shape[0]
        shape = (len(arrays), self.parts, rows, wide)
        self.outs = [jax.ShapeDtypeStruct(shape, arrays[0].dtype)]
        self.scratch = [pltpu.VMEM(shape, arrays[0].dtype)]
        self.scratch += [pltpu.SemaphoreType.DMA((len(arrays), self.parts))] * 2

    def phases(self, place, ins, outs, scratch):
        (out,), (stage, send, recv) = outs, scratch
        parts, live = self.parts, self.live
        every = [(i, step) for step in (2, 3, 1) for i in range(len(ins))]

        def copy(i, step, index):
            other = (place.part + step) % parts
            return remote(
                stage.at[i, other], out.at[i, index], send.at[i, step], recv.at[i, step], fsdp=other
            )

        def first():
            for i, ref in enumerate(ins):
                for part in range(parts):
                    start = part * live
                    stop = min(start + live, ref.shape[1])
                    stage[i, part, :, : stop - start] = ref[:, start:stop]
                    if stop - start < self.wide:
                        shape = (ref.shape[0], self.wide - stop + start)
                        stage[i, part, :, stop - start :] = jnp.zeros(shape, ref.dtype)
            for i, step in every:
                copy(i, step, place.part).start()
            for i in range(len(ins)):
                out[i, place.part] = stage[i, place.part]

        def second():
            for i, step in every:
                copy(i, step, (place.part + parts - step) % parts).wait_recv()
                copy(i, step, place.part).wait_send()

        return [first, second]


class Window:
    reach = ("fsdp",)

    def __init__(self, array, live, wide):
        self.parts = lax.axis_size("fsdp")
        self.quarter, columns = array.shape
        self.live, self.wide = live, wide
        self.near = (live - self.quarter) * self.parts
        self.ins = [array]
        self.outs = [jax.ShapeDtypeStruct((wide, columns), array.dtype)]
        self.scratch = [pltpu.VMEM((self.quarter + self.near, columns), array.dtype)]
        self.scratch += [pltpu.SemaphoreType.DMA] * 2

    def phases(self, place, ins, outs, scratch):
        (source,), (out,), (both, send, recv) = ins, outs, scratch
        left = (place.part + self.parts - 1) % self.parts
        copy = remote(
            source.at[: self.near], both.at[self.quarter :], send, recv, fsdp=left
        )

        def first():
            copy.start()
            both[: self.quarter] = source[...]

        def second():
            copy.wait()
            start = pl.multiple_of(place.part * (self.live - self.quarter), 16)
            rows = both[pl.ds(start, self.live), :]
            index = lax.broadcasted_iota(jnp.int32, rows.shape, 0) + place.part * self.live
            inside = index < self.quarter * self.parts
            out[: self.live] = jnp.where(inside, rows, jnp.zeros_like(rows))
            if self.wide > self.live:
                out[self.live :] = jnp.zeros((self.wide - self.live, rows.shape[1]), rows.dtype)

        return [first, second]


class Total:
    reach = ("ctx",)

    def __init__(self, array):
        self.n = lax.axis_size("ctx")
        self.ins = [array]
        self.outs = [jax.ShapeDtypeStruct(array.shape, F32)]
        self.scratch = [pltpu.VMEM((self.n, *array.shape), array.dtype)]
        self.scratch += [pltpu.SemaphoreType.DMA((self.n,))] * 2

    def phases(self, place, ins, outs, scratch):
        (source,), (out,), (held, send, recv) = ins, outs, scratch
        n, me = self.n, place.ctx

        def copy(step, index):
            return remote(source, held.at[index], send.at[step], recv.at[step], ctx=(me + step) % n)

        def first():
            lax.fori_loop(1, n, lambda step, _: (copy(step, me).start(), 0)[1], 0)
            held[me] = source[...]

        def last():
            def end(step, _):
                copy(step, (me + n - step) % n).wait_recv()
                copy(step, me).wait_send()
                return 0

            lax.fori_loop(1, n, end, 0)
            total = held[0].astype(F32)
            for i in range(1, n):
                total = total + held[i].astype(F32)
            out[...] = total

        return [first, last]


class Ring:
    reach = ("ring", "fsdp")

    def __init__(self, streams):
        self.n = lax.axis_size("ctx")
        self.parts = lax.axis_size("fsdp")
        self.per = self.n // self.parts
        self.streams = []
        self.ins, self.outs, self.scratch = [], [], []
        for array, direction, crossing in streams:
            n, rows, columns = array.shape
            self.ins.append(array)
            self.outs.append(jax.ShapeDtypeStruct(array.shape, array.dtype))
            self.scratch.append(pltpu.VMEM((n - 1, rows, columns), array.dtype))
            middle = (columns // 2 + LANES - 1) // LANES * LANES
            for low, high in ((0, middle), (middle, columns)):
                self.streams.append((len(self.ins) - 1, direction, crossing, slice(low, high)))
        self.scratch += [pltpu.SemaphoreType.DMA((len(self.streams), 2, self.n))] * 2

    def phases(self, place, ins, outs, scratch):
        slots, (send, recv) = scratch[:-2], scratch[-2:]
        n, parts, per, here = self.n, self.parts, self.per, place.position
        shift = place.ctx // per
        owner = (place.part + shift) % parts

        def slab(stream, position):
            index = place.at(position)
            return (index + per * place.part) % n if self.streams[stream][2] else index

        def reducing(stream, step):
            array, direction, _, columns = self.streams[stream]
            if step == 0:
                source = ins[array].at[slab(stream, here - direction), :, columns]
            else:
                source = slots[array].at[step - 1, :, columns]
            return remote(
                source,
                slots[array].at[step, :, columns],
                send.at[stream, 0, step],
                recv.at[stream, 0, step],
                ctx=place.at(here + direction),
            )

        def crossing(stream):
            array, _, _, columns = self.streams[stream]
            return remote(
                slots[array].at[n - 2, :, columns],
                outs[array].at[place.ctx, :, columns],
                send.at[stream, 0, n - 1],
                recv.at[stream, 0, n - 1],
                fsdp=owner,
            )

        def gathering(stream, step, back=0):
            array, direction, _, columns = self.streams[stream]
            index = place.at(here - direction * (step + back))
            return remote(
                outs[array].at[index, :, columns],
                outs[array].at[index, :, columns],
                send.at[stream, 1, step],
                recv.at[stream, 1, step],
                ctx=place.at(here + direction),
            )

        every = range(len(self.streams))

        def begin():
            for stream in every:
                reducing(stream, 0).start()

        def add(stream, step):
            array, direction, _, columns = self.streams[stream]
            reducing(stream, step).wait_recv()
            own = ins[array][slab(stream, here - direction * (step + 2)), :, columns]
            return (slots[array][step, :, columns].astype(F32) + own.astype(F32)).astype(own.dtype)

        def reduce(step):
            for stream in every:
                array, _, _, columns = self.streams[stream]
                slots[array][step - 1, :, columns] = add(stream, step - 1)
                reducing(stream, step).start()

        def turn():
            for stream in every:
                array, _, crosses, columns = self.streams[stream]
                total = add(stream, n - 2)
                if not crosses:
                    outs[array][place.ctx, :, columns] = total
                    gathering(stream, 0).start()
                    continue

                @pl.when(shift == 0)
                def _():
                    outs[array][place.ctx, :, columns] = total

                @pl.when(shift != 0)
                def _():
                    slots[array][n - 2, :, columns] = total
                    crossing(stream).start()

        def launch():
            for stream in every:
                if self.streams[stream][2]:

                    @pl.when(shift != 0)
                    def _():
                        crossing(stream).wait()

                    gathering(stream, 0).start()

        def forward(step):
            for stream in every:
                gathering(stream, step - 1, 1).wait_recv()
                gathering(stream, step).start()

        def end():
            for stream in every:
                gathering(stream, n - 2, 1).wait_recv()
            for stream in every:
                for step in range(n - 1):
                    reducing(stream, step).wait_send()
                    gathering(stream, step).wait_send()

        steps = [begin]
        steps += [functools.partial(reduce, step) for step in range(1, n - 1)]
        steps += [turn, launch]
        steps += [functools.partial(forward, step) for step in range(1, n - 1)]
        return steps + [end]


def exchange_kernel(transfers, *refs):
    refs = list(refs)

    def take(lists):
        taken = []
        for items in lists:
            taken.append(refs[: len(items)])
            del refs[: len(items)]
        return taken

    ins = take([t.ins for t in transfers])
    outs = take([t.outs for t in transfers])
    scratch = take([t.scratch for t in transfers])
    place = Place()
    reach = {name for t in transfers for name in t.reach}
    peers = []
    if "fsdp" in reach:
        peers += [dict(fsdp=(place.part + k) % place.parts) for k in range(1, place.parts)]
    if "ctx" in reach:
        peers += [dict(ctx=(place.ctx + k) % place.n_ctx) for k in range(1, place.n_ctx)]
    if "ring" in reach:
        peers += [dict(ctx=place.at(place.position + k)) for k in (1, -1)]
    barrier = pltpu.get_barrier_semaphore()
    for peer in peers:
        pl.semaphore_signal(barrier, inc=1, device_id=peer, device_id_type=pl.DeviceIdType.MESH)
    pl.semaphore_wait(barrier, len(peers))
    lists = [t.phases(place, *each) for t, *each in zip(transfers, ins, outs, scratch)]
    for index in range(max(map(len, lists))):
        for phases in lists:
            if index < len(phases):
                phases[index]()


def exchange(number, name, *transfers):
    memory = pl.BlockSpec(memory_space=pltpu.VMEM)
    ins = [a for t in transfers for a in t.ins]
    outs = [a for t in transfers for a in t.outs]
    results = pl.pallas_call(
        functools.partial(exchange_kernel, transfers),
        out_shape=outs,
        in_specs=[memory] * len(ins),
        out_specs=[memory] * len(outs),
        scratch_shapes=[s for t in transfers for s in t.scratch],
        compiler_params=pltpu.CompilerParams(collective_id=number, has_side_effects=True),
        name=name,
    )(*ins)
    results = list(results)
    split = []
    for t in transfers:
        split.append(results[: len(t.outs)])
        del results[: len(t.outs)]
    return split


def results_kernel(widths, parts, order_ref, *refs):
    for index, (live, total) in enumerate(widths):
        out = refs[len(widths) * parts + index]
        for part in range(parts):
            stop = min((part + 1) * live, total)
            block = refs[index * parts + part][0, :, : stop - part * live]
            out[:, part * live : stop] = block.astype(F32)


def by_rows(arrays, widths, per, part, parts):
    slabs, rows, _ = arrays[0].shape
    order = (part - jnp.arange(parts, dtype=jnp.int32) + parts) % parts
    if rows % 8:
        outs = []
        for array, (live, total) in zip(arrays, widths):
            array = jnp.take(array.reshape(parts, per, rows, -1), order, axis=0)[..., :live]
            array = jnp.transpose(array, (1, 2, 0, 3)).reshape(per * rows, parts * live)
            outs.append(array[:, :total].astype(F32))
        return outs
    step = 40 if rows % 40 == 0 else rows
    inner = rows // step

    def source(column, array):
        return pl.BlockSpec(
            (1, step, array.shape[2]),
            lambda i, order: (order[column] * per + i // inner, i % inner, 0),
        )

    return pl.pallas_call(
        functools.partial(results_kernel, widths, parts),
        out_shape=[jax.ShapeDtypeStruct((per * rows, total), F32) for _, total in widths],
        grid_spec=pltpu.PrefetchScalarGridSpec(
            num_scalar_prefetch=1,
            grid=(per * inner,),
            in_specs=[source(column, array) for array in arrays for column in range(parts)],
            out_specs=[pl.BlockSpec((step, total), lambda i, order: (i, 0)) for _, total in widths],
        ),
        name="by_rows",
    )(order, *[array for array in arrays for _ in range(parts)])


def on_device(
    inputs,
    cotangent,
    w_query,
    w_key,
    w_value,
    w_out,
    w_fc,
    w_proj,
    ln1_gain,
    ln1_bias,
    query_bias,
    value_bias,
    out_bias,
    ln2_gain,
    ln2_bias,
    fc_bias,
    proj_bias,
):
    parts = lax.axis_size("fsdp")
    n_ctx = lax.axis_size("ctx")
    me_part = lax.axis_index("fsdp")
    seqs, rows, width = inputs.shape
    hidden = w_fc.shape[1]
    quarter = width // parts
    hidden_part = hidden // parts
    own = seqs * rows
    all_seqs = seqs * parts
    tokens = all_seqs * rows
    length = rows * n_ctx
    half_rows = rows // 2
    groups = n_ctx // all_seqs
    heads_part = -(-HEADS // parts)
    live = heads_part * HEAD
    slots = -(-heads_part // (2 * groups)) * 2 * groups
    cols = slots * HEAD
    piece = cols // groups
    heads_here = heads_part if groups == 1 else slots // groups
    near = (live - quarter) * parts
    per = n_ctx // parts
    slab = width // n_ctx

    def to_slots(vector):
        vector = jnp.pad(vector, (0, parts * live - width)).reshape(parts, live)
        return jnp.pad(vector, ((0, 0), (0, cols - live)))[me_part]

    def by_parts(array):
        return array.astype(BF16).reshape(parts, own, width)

    def by_sequences(array):
        return array.reshape(all_seqs, 2, half_rows, cols)

    def by_slabs(array, count):
        return array.astype(BF16).reshape(count, -1, array.shape[1])

    small = jnp.concatenate(
        [ln1_gain, ln1_bias, query_bias, value_bias, out_bias, ln2_gain, ln2_bias, proj_bias]
    )[None, :]
    small = lax.all_gather(small, "fsdp", axis=0, tiled=True).astype(F32).reshape(parts, 8, quarter)
    gain_one, shift_one, bias_query, bias_value, bias_out, gain_two, shift_two, bias_proj = [
        small[:, i].reshape(-1) for i in range(8)
    ]
    bias_query, bias_value = to_slots(bias_query), to_slots(bias_value)
    bias_fc = fc_bias.astype(F32)

    x_full = inputs.astype(F32).reshape(own, width)
    hat_one, inv_one = normalize(x_full)
    (qkv,), (out_w,), (normed_one,) = exchange(
        0,
        "start",
        Swap([w_query, w_key, w_value], live, cols),
        Window(w_out, live, cols),
        Gather((hat_one * gain_one + shift_one).astype(BF16)),
    )
    qkv = qkv.reshape(3, width, cols)
    normed_one = normed_one.reshape(tokens, width)
    queries = (dot(normed_one, qkv[0]) + bias_query).astype(BF16)
    keys = dot(normed_one, qkv[1]).astype(BF16)
    values = (dot(normed_one, qkv[2]) + bias_value).astype(BF16)
    heads, (fc,), (grad_y,) = exchange(
        1,
        "to_heads",
        ToHeads([by_sequences(a) for a in (queries, keys, values)]),
        Swap([w_fc], hidden_part, hidden_part),
        Gather(cotangent.reshape(own, width)),
    )
    fc = fc.reshape(width, hidden_part)
    grad_y = grad_y.reshape(tokens, width)
    proj = w_proj

    q_seq, k_seq, v_seq = [a.reshape(length, piece) for a in heads]
    o_seq, ot, lse = attend(q_seq, k_seq, v_seq, heads_here)

    def blocks(array):
        return array.reshape(2 * n_ctx, half_rows, piece)

    (attended,) = exchange(2, "from_heads", FromHeads([blocks(o_seq)], all_seqs))[0]
    attended = attended.reshape(tokens, cols)
    (branch,) = exchange(3, "branch", Scatter(by_parts(dot(attended, out_w))))[0]
    resid = x_full + branch + bias_out

    hat_two, inv_two = normalize(resid)
    (normed_two,) = exchange(4, "second", Gather((hat_two * gain_two + shift_two).astype(BF16)))[0]
    normed_two = normed_two.reshape(tokens, width)
    pre_act = dot(normed_two, fc) + bias_fc
    value, slope = gelu_both(pre_act)
    activated = value.astype(BF16)
    mlp = by_parts(dot(activated, proj))

    grad_pre = (dot_nt(grad_y, proj) * slope).astype(BF16)
    (grad_norm_two,), (mlp,) = exchange(
        5, "second_back", Scatter(by_parts(dot_nt(grad_pre, fc))), Scatter(mlp)
    )
    outputs = (resid + mlp + bias_proj).astype(BF16).reshape(seqs, rows, width)
    grad_y_own = cotangent.reshape(own, width).astype(F32)
    grad_gain_two = jnp.sum(grad_norm_two * hat_two, axis=0)
    grad_shift_two = jnp.sum(grad_norm_two, axis=0)
    grad_bias_proj = jnp.sum(grad_y_own, axis=0)
    grad_bias_fc = jnp.sum(grad_pre.astype(F32), axis=0)
    grad_resid = grad_y_own + norm_back(grad_norm_two, gain_two, hat_two, inv_two)
    grad_branch = grad_resid.astype(BF16)
    grad_bias_out = jnp.sum(grad_branch.astype(F32), axis=0)
    proj_part = by_slabs(dot_tn(activated, grad_y), n_ctx)
    fc_part = by_slabs(dot_tn(normed_two, grad_pre), n_ctx)
    (proj_grad, fc_grad), (grad_branch,) = exchange(
        6, "wide_grads", Ring([(proj_part, 1, False), (fc_part, -1, True)]), Gather(grad_branch)
    )
    grad_branch = grad_branch.reshape(tokens, width)
    grad_attended = dot_nt(grad_branch, out_w).astype(BF16)

    ((grad_heads,),) = exchange(7, "to_heads_back", ToHeads([by_sequences(grad_attended)]))
    dq_seq, dk_seq, dv_seq = attend_back(
        q_seq, k_seq, v_seq, grad_heads.reshape(length, piece), ot, lse, heads_here
    )
    (grad_qkv,) = exchange(
        8, "from_heads_back", FromHeads([blocks(a) for a in (dq_seq, dk_seq, dv_seq)], all_seqs)
    )
    grad_qkv = [a.reshape(tokens, cols) for a in grad_qkv]
    ((grad_norm_one,),) = exchange(
        9,
        "first_back",
        Scatter(
            by_parts(
                dot_nt(grad_qkv[0], qkv[0]) + dot_nt(grad_qkv[1], qkv[1]) + dot_nt(grad_qkv[2], qkv[2])
            )
        ),
    )
    grad_bias_query = jnp.sum(grad_qkv[0].astype(F32), axis=0)
    grad_bias_value = jnp.sum(grad_qkv[2].astype(F32), axis=0)
    grad_gain_one = jnp.sum(grad_norm_one * hat_one, axis=0)
    grad_shift_one = jnp.sum(grad_norm_one, axis=0)
    input_grad = grad_resid + norm_back(grad_norm_one, gain_one, hat_one, inv_one)
    input_grad = input_grad.reshape(seqs, rows, width)

    def window(vector):
        whole = jnp.zeros((parts * live,), F32)
        return lax.dynamic_update_slice_in_dim(whole, vector[:live], me_part * live, 0)[:width]

    small_grads = jnp.stack(
        [
            grad_gain_one,
            grad_shift_one,
            window(grad_bias_query),
            window(grad_bias_value),
            grad_bias_out,
            grad_gain_two,
            grad_shift_two,
            grad_bias_proj,
        ]
    )
    small_grads = jnp.transpose(small_grads.reshape(8, parts, quarter), (1, 0, 2))
    ((small_grads,),) = exchange(10, "small", Scatter(small_grads))
    small_grads = jnp.concatenate([small_grads, grad_bias_fc.reshape(-1, quarter)])

    q_part, k_part, v_part = [by_slabs(dot_tn(normed_one, a), n_ctx) for a in grad_qkv]
    out_part = by_slabs(dot_tn(attended, grad_branch), n_ctx)
    (out_grad, q_grad, k_grad, v_grad), (small_grads,) = exchange(
        11,
        "narrow_grads",
        Ring([(out_part, 1, False), (q_part, 1, True), (k_part, -1, True), (v_part, -1, True)]),
        Total(small_grads),
    )
    fc_out, q_out, k_out, v_out = by_rows(
        [fc_grad, q_grad, k_grad, v_grad],
        [(hidden_part, hidden)] + [(live, width)] * 3,
        per,
        me_part,
        parts,
    )
    out_rows = out_grad.reshape(cols, width)[:live]
    from_left = lax.ppermute(out_rows[live - near :], "fsdp", [(i, i + 1) for i in range(parts - 1)])
    out_rows = lax.dynamic_slice_in_dim(
        jnp.concatenate([from_left, out_rows]), near - me_part * (live - quarter), quarter, 0
    ).astype(F32)
    return (
        outputs,
        input_grad,
        q_out,
        k_out,
        v_out,
        out_rows,
        fc_out,
        proj_grad.reshape(hidden_part, width).astype(F32),
        small_grads[0],
        small_grads[1],
        small_grads[2],
        small_grads[3],
        small_grads[4],
        small_grads[5],
        small_grads[6],
        small_grads[8:].reshape(-1),
        small_grads[7],
    )


def solution(mesh):
    tokens = P("fsdp", "ctx", None)
    matrix = P("fsdp", None)
    vector = P("fsdp")
    return jax.shard_map(
        on_device,
        mesh=mesh,
        in_specs=(tokens, tokens) + (matrix,) * 6 + (vector,) * 9,
        out_specs=(tokens, tokens) + (matrix,) * 6 + (vector,) * 9,
        check_vma=False,
    )
```

```python
import functools

import jax
import jax.numpy as jnp
from jax import lax
from jax.experimental import pallas as pl
from jax.experimental.pallas import tpu as pltpu
from jax.sharding import PartitionSpec as P

HEADS = 25
HEAD = 64
EPS = 1e-05
SCALE = 0.125
NEGATIVE = -1000000000.0
ROOT = 0.7978845608028654
CUBIC = 0.044715
LANES = 128
F32 = jnp.float32
BF16 = jnp.bfloat16


def normalize(values):
    centre = jnp.mean(values, axis=-1, keepdims=True)
    centred = values - centre
    spread = jnp.mean(centred * centred, axis=-1, keepdims=True)
    inv_std = lax.rsqrt(spread + EPS)
    return (centred * inv_std, inv_std)


def norm_back(grad_norm, gain, normal, inv_std):
    scaled = grad_norm * gain
    return inv_std * (
        scaled
        - jnp.mean(scaled, axis=-1, keepdims=True)
        - normal * jnp.mean(scaled * normal, axis=-1, keepdims=True)
    )


def gelu_both(values):
    tangent = jnp.tanh(ROOT * (values + CUBIC * values * values * values))
    value = 0.5 * values * (1.0 + tangent)
    slope = 0.5 * (1.0 + tangent) + 0.5 * values * (1.0 - tangent * tangent) * ROOT * (
        1.0 + 3.0 * CUBIC * values * values
    )
    return value, slope


def dot(left, right):
    return jnp.dot(left, right, preferred_element_type=F32)


def dot_nt(left, right):
    return lax.dot_general(left, right, (((1,), (1,)), ((), ())), preferred_element_type=F32)


def dot_tn(left, right):
    return lax.dot_general(left, right, (((0,), (0,)), ((), ())), preferred_element_type=F32)


def lane_half(shape, half):
    lane = lax.broadcasted_iota(jnp.int32, shape, 1)
    return (lane < HEAD) if half == 0 else (lane >= HEAD)


def keep_half(array, half):
    return jnp.where(lane_half(array.shape, half), array, jnp.zeros_like(array))


def causal_tail(scores, first_row, block):
    keys = lax.broadcasted_iota(jnp.int32, scores.shape, 0) + first_row
    queries = lax.broadcasted_iota(jnp.int32, scores.shape, 1)
    return jnp.where(keys <= queries, scores, NEGATIVE)


def attend_kernel(block, heads, q_ref, k_ref, v_ref, o_ref, ot_ref, lse_ref):
    length = q_ref.shape[0]
    pair = pl.program_id(0)
    v_t = jnp.transpose(v_ref[...].astype(F32)).astype(BF16)

    def one_head(half):
        for index in range(length // block):
            rows = slice(index * block, (index + 1) * block)
            count = (index + 1) * block
            query = keep_half(q_ref[rows, :], half) * jnp.asarray(SCALE, BF16)
            scores = dot_nt(k_ref[:count, :], query)
            scores = causal_tail(scores, -index * block, block)
            top = jnp.max(scores, axis=0, keepdims=True)
            weights = jnp.exp(scores - top)
            total = jnp.sum(weights, axis=0, keepdims=True)
            lse_ref[0, half : half + 1, rows] = top + jnp.log(total)
            weights = weights * (1.0 / total)
            ot = dot(v_t[half * HEAD : (half + 1) * HEAD, :count], weights.astype(BF16))
            ot_ref[0, half * HEAD : (half + 1) * HEAD, rows] = ot

    one_head(0)

    @pl.when(2 * pair + 1 < heads)
    def _():
        one_head(1)

    @pl.when(2 * pair + 1 >= heads)
    def _():
        ot_ref[0, HEAD:, :] = jnp.zeros((HEAD, length), F32)
        lse_ref[0, 1:2, :] = jnp.zeros((1, length), F32)

    o_ref[...] = jnp.transpose(ot_ref[0]).astype(BF16)


def attend(queries, keys, values, heads):
    length, width = queries.shape
    pairs = width // LANES
    block = min(256, length)
    column = pl.BlockSpec((length, LANES), lambda p: (0, p))
    return pl.pallas_call(
        functools.partial(attend_kernel, block, heads),
        grid=(pairs,),
        in_specs=[column] * 3,
        out_specs=[
            column,
            pl.BlockSpec((1, LANES, length), lambda p: (p, 0, 0)),
            pl.BlockSpec((1, 2, length), lambda p: (p, 0, 0)),
        ],
        out_shape=[
            jax.ShapeDtypeStruct((length, width), BF16),
            jax.ShapeDtypeStruct((pairs, LANES, length), F32),
            jax.ShapeDtypeStruct((pairs, 2, length), F32),
        ],
        name="attend",
    )(queries, keys, values)


def attend_back_kernel(
    block, heads, q_ref, k_ref, v_ref, do_ref, ot_ref, lse_ref, dq_ref, dk_ref, dv_ref, dk_sum, dv_sum
):
    length = q_ref.shape[0]
    pair = pl.program_id(0)
    k_t = jnp.transpose(k_ref[...].astype(F32)).astype(BF16)
    do_t = jnp.transpose(do_ref[...].astype(F32))
    dk_sum[...] = jnp.zeros_like(dk_sum)
    dv_sum[...] = jnp.zeros_like(dv_sum)
    dq_ref[...] = jnp.zeros_like(dq_ref)

    def one_head(half):
        span = slice(half * HEAD, (half + 1) * HEAD)
        shared = jnp.sum(do_t[span, :] * ot_ref[0, span, :], axis=0, keepdims=True)
        for index in range(length // block):
            rows = slice(index * block, (index + 1) * block)
            count = (index + 1) * block
            query = keep_half(q_ref[rows, :], half) * jnp.asarray(SCALE, BF16)
            grad = keep_half(do_ref[rows, :], half)
            scores = dot_nt(k_ref[:count, :], query)
            scores = causal_tail(scores, -index * block, block)
            probs = jnp.exp(scores - lse_ref[0, half : half + 1, rows])
            grad_probs = dot_nt(v_ref[:count, :], grad)
            grad_scores = (probs * (grad_probs - shared[:, rows])).astype(BF16)
            dv_sum[:count, :] += dot(probs.astype(BF16), grad)
            dk_sum[:count, :] += dot(grad_scores, query)
            dq_t = dot(k_t[span, :count], grad_scores) * SCALE
            pad = jnp.zeros_like(dq_t)
            both = jnp.concatenate([dq_t, pad] if half == 0 else [pad, dq_t], axis=0)
            dq_ref[rows, :] = dq_ref[rows, :] + jnp.transpose(both).astype(BF16)

    one_head(0)

    @pl.when(2 * pair + 1 < heads)
    def _():
        one_head(1)

    dk_ref[...] = dk_sum[...].astype(BF16)
    dv_ref[...] = dv_sum[...].astype(BF16)


def attend_back(queries, keys, values, grad, ot, lse, heads):
    length, width = queries.shape
    pairs = width // LANES
    block = min(256, length)
    column = pl.BlockSpec((length, LANES), lambda p: (0, p))
    return pl.pallas_call(
        functools.partial(attend_back_kernel, block, heads),
        grid=(pairs,),
        in_specs=[column] * 4
        + [
            pl.BlockSpec((1, LANES, length), lambda p: (p, 0, 0)),
            pl.BlockSpec((1, 2, length), lambda p: (p, 0, 0)),
        ],
        out_specs=[column] * 3,
        out_shape=[jax.ShapeDtypeStruct((length, width), BF16)] * 3,
        scratch_shapes=[pltpu.VMEM((length, LANES), F32)] * 2,
        name="attend_back",
    )(queries, keys, values, grad, ot, lse)


class Place:
    def __init__(self):
        self.parts = lax.axis_size("fsdp")
        self.n_ctx = lax.axis_size("ctx")
        self.part = lax.axis_index("fsdp")
        self.ctx = lax.axis_index("ctx")
        self.beside = self.part + 1 - 2 * (self.part % 2)
        self.far = (self.part + 2) % self.parts
        self.diagonal = (self.beside + 2) % self.parts

    def at(self, position):
        n = self.n_ctx
        position = (position + 2 * n) % n
        upper = position // (n // 2)
        return (1 - upper) * 2 * position + upper * (2 * (n - 1 - position) + 1)

    @property
    def position(self):
        odd = self.ctx % 2
        return (1 - odd) * (self.ctx // 2) + odd * (self.n_ctx - 1 - self.ctx // 2)


def remote(source, target, send, recv, **where):
    return pltpu.make_async_remote_copy(
        src_ref=source,
        dst_ref=target,
        send_sem=send,
        recv_sem=recv,
        device_id=where,
        device_id_type=pl.DeviceIdType.MESH,
    )


def cut(rows):
    step = 64 if rows % 64 == 0 else rows
    return [slice(start, start + step) for start in range(0, rows, step)]


class Gather:
    reach = ("fsdp",)

    def __init__(self, array):
        self.ins = [array]
        self.parts = lax.axis_size("fsdp")
        self.pieces = cut(array.shape[0])
        self.outs = [jax.ShapeDtypeStruct((self.parts, *array.shape), array.dtype)]
        self.scratch = [pltpu.SemaphoreType.DMA((3, len(self.pieces)))] * 2

    def phases(self, place, ins, outs, scratch):
        (source,), (out,), (send, recv) = ins, outs, scratch
        count = range(len(self.pieces))

        def copy(kind, k, index, target):
            piece = self.pieces[k]
            start = source.at[piece] if kind < 2 else out.at[index, piece]
            return remote(start, out.at[index, piece], send.at[kind, k], recv.at[kind, k], fsdp=target)

        def first():
            for k in count:
                copy(1, k, place.part, place.far).start()
            for k in count:
                copy(0, k, place.part, place.beside).start()
            out[place.part] = source[...]

        def second():
            for k in count:
                copy(1, k, place.far, place.far).wait_recv()
                copy(2, k, place.far, place.beside).start()

        def third():
            for k in count:
                copy(0, k, place.beside, place.beside).wait_recv()
                copy(2, k, place.diagonal, place.beside).wait_recv()
            for k in count:
                copy(0, k, place.part, place.beside).wait_send()
                copy(1, k, place.part, place.far).wait_send()
                copy(2, k, place.far, place.beside).wait_send()

        return [first, second, third]


class Scatter:
    reach = ("fsdp",)

    def __init__(self, array):
        parts, rows, columns = array.shape
        self.ins = [array]
        self.pieces = cut(rows)
        self.outs = [jax.ShapeDtypeStruct((rows, columns), F32)]
        self.scratch = [pltpu.VMEM((rows, columns), array.dtype)] * 3
        self.scratch += [pltpu.SemaphoreType.DMA((3, len(self.pieces)))] * 2

    def phases(self, place, ins, outs, scratch):
        (source,), (out,) = ins, outs
        for_far, for_own, from_far, send, recv = scratch
        count = range(len(self.pieces))

        def copy(kind, k):
            piece = self.pieces[k]
            start, target, where = [
                (source.at[place.diagonal, piece], for_far, place.beside),
                (source.at[place.beside, piece], for_own, place.beside),
                (for_far.at[piece], from_far, place.far),
            ][kind]
            return remote(start, target.at[piece], send.at[kind, k], recv.at[kind, k], fsdp=where)

        def first():
            for k in count:
                copy(0, k).start()
            for k in count:
                copy(1, k).start()

        def second():
            for k in count:
                piece = self.pieces[k]
                copy(0, k).wait_recv()
                total = for_far[piece].astype(F32) + source[place.far, piece].astype(F32)
                for_far[piece] = total.astype(for_far.dtype)
                copy(2, k).start()

        def third():
            for k in count:
                piece = self.pieces[k]
                copy(1, k).wait_recv()
                out[piece] = for_own[piece].astype(F32) + source[place.part, piece].astype(F32)

        def fourth():
            for k in count:
                piece = self.pieces[k]
                copy(2, k).wait_recv()
                out[piece] += from_far[piece].astype(F32)
            for k in count:
                for kind in range(3):
                    copy(kind, k).wait_send()

        return [first, second, third, fourth]


class ToHeads:
    reach = ("ctx",)

    def __init__(self, arrays):
        seqs, _, half, columns = arrays[0].shape
        self.n = lax.axis_size("ctx")
        self.groups = self.n // seqs
        self.piece = columns // self.groups
        self.ins = list(arrays)
        self.outs = [jax.ShapeDtypeStruct((2 * self.n, half, self.piece), a.dtype) for a in arrays]
        self.scratch = [pltpu.SemaphoreType.DMA((len(arrays), 2, self.n))] * 2

    def whole(self, ref, other, half):
        if self.groups == 1:
            return ref.at[other, half]
        column = pl.multiple_of((other % self.groups) * self.piece, LANES)
        return ref.at[other // self.groups, half, :, pl.ds(column, self.piece)]

    def block(self, ref, other, half):
        return ref.at[other if half == 0 else 2 * self.n - 1 - other]

    def source(self, ref, other, half):
        return self.whole(ref, other, half)

    def target(self, ref, other, half):
        return self.block(ref, other, half)

    def phases(self, place, ins, outs, scratch):
        send, recv = scratch
        n, me = self.n, place.ctx
        every = [(i, half) for i in range(len(ins)) for half in range(2)]

        def first():
            def begin(step, _):
                other = (me + step) % n
                for i, half in every:
                    remote(
                        self.source(ins[i], other, half),
                        self.target(outs[i], me, half),
                        send.at[i, half, step],
                        recv.at[i, half, step],
                        ctx=other,
                    ).start()
                return 0

            lax.fori_loop(1, n, begin, 0)
            for i, half in every:
                self.target(outs[i], me, half)[...] = self.source(ins[i], me, half)[...]

        def second():
            def end(step, _):
                other = (me + n - step) % n
                for i, half in every:
                    copy = remote(
                        self.source(ins[i], other, half),
                        self.target(outs[i], other, half),
                        send.at[i, half, step],
                        recv.at[i, half, step],
                        ctx=other,
                    )
                    copy.wait_recv()
                    copy.wait_send()
                return 0

            lax.fori_loop(1, n, end, 0)

        return [first, second]


class FromHeads(ToHeads):
    def __init__(self, arrays, seqs):
        blocks, half, piece = arrays[0].shape
        self.n = blocks // 2
        self.groups = self.n // seqs
        self.piece = piece
        self.ins = list(arrays)
        shape = (seqs, 2, half, piece * self.groups)
        self.outs = [jax.ShapeDtypeStruct(shape, a.dtype) for a in arrays]
        self.scratch = [pltpu.SemaphoreType.DMA((len(arrays), 2, self.n))] * 2

    def source(self, ref, other, half):
        return self.block(ref, other, half)

    def target(self, ref, other, half):
        return self.whole(ref, other, half)


class Swap:
    reach = ("fsdp",)

    def __init__(self, arrays, live, wide):
        self.parts = lax.axis_size("fsdp")
        self.live, self.wide = live, wide
        self.ins = list(arrays)
        rows = arrays[0].shape[0]
        shape = (len(arrays), self.parts, rows, wide)
        self.outs = [jax.ShapeDtypeStruct(shape[1:], arrays[0].dtype)] * len(arrays)
        self.scratch = [pltpu.VMEM(shape, arrays[0].dtype)]
        self.scratch += [pltpu.SemaphoreType.DMA((len(arrays), self.parts))] * 2

    def phases(self, place, ins, outs, scratch):
        stage, send, recv = scratch
        parts, live = self.parts, self.live
        every = [(i, step) for step in (2, 3, 1) for i in range(len(ins))]

        def copy(i, step, index):
            other = (place.part + step) % parts
            return remote(
                stage.at[i, other], outs[i].at[index], send.at[i, step], recv.at[i, step], fsdp=other
            )

        def first():
            for i, ref in enumerate(ins):
                for part in range(parts):
                    start = part * live
                    stop = min(start + live, ref.shape[1])
                    stage[i, part, :, : stop - start] = ref[:, start:stop]
                    if stop - start < self.wide:
                        shape = (ref.shape[0], self.wide - stop + start)
                        stage[i, part, :, stop - start :] = jnp.zeros(shape, ref.dtype)
            for i, step in every:
                copy(i, step, place.part).start()
            for i in range(len(ins)):
                outs[i][place.part] = stage[i, place.part]

        def second():
            for i, step in every:
                copy(i, step, (place.part + parts - step) % parts).wait_recv()
                copy(i, step, place.part).wait_send()

        return [first, second]


class Window:
    reach = ("fsdp",)

    def __init__(self, array, live, wide):
        self.parts = lax.axis_size("fsdp")
        self.quarter, columns = array.shape
        self.live, self.wide = live, wide
        self.near = (live - self.quarter) * self.parts
        self.ins = [array]
        self.outs = [jax.ShapeDtypeStruct((wide, columns), array.dtype)]
        self.scratch = [pltpu.VMEM((self.quarter + self.near, columns), array.dtype)]
        self.scratch += [pltpu.SemaphoreType.DMA] * 2

    def phases(self, place, ins, outs, scratch):
        (source,), (out,), (both, send, recv) = ins, outs, scratch
        left = (place.part + self.parts - 1) % self.parts
        copy = remote(
            source.at[: self.near], both.at[self.quarter :], send, recv, fsdp=left
        )

        def first():
            copy.start()
            both[: self.quarter] = source[...]

        def second():
            copy.wait()
            start = pl.multiple_of(place.part * (self.live - self.quarter), 16)
            rows = both[pl.ds(start, self.live), :]
            index = lax.broadcasted_iota(jnp.int32, rows.shape, 0) + place.part * self.live
            inside = index < self.quarter * self.parts
            out[: self.live] = jnp.where(inside, rows, jnp.zeros_like(rows))
            if self.wide > self.live:
                out[self.live :] = jnp.zeros((self.wide - self.live, rows.shape[1]), rows.dtype)

        return [first, second]


class Total:
    reach = ("ctx",)

    def __init__(self, array):
        self.n = lax.axis_size("ctx")
        self.ins = [array]
        self.outs = [jax.ShapeDtypeStruct(array.shape, F32)]
        self.scratch = [pltpu.VMEM((self.n, *array.shape), array.dtype)]
        self.scratch += [pltpu.SemaphoreType.DMA((self.n,))] * 2

    def phases(self, place, ins, outs, scratch):
        (source,), (out,), (held, send, recv) = ins, outs, scratch
        n, me = self.n, place.ctx

        def copy(step, index):
            return remote(source, held.at[index], send.at[step], recv.at[step], ctx=(me + step) % n)

        def first():
            lax.fori_loop(1, n, lambda step, _: (copy(step, me).start(), 0)[1], 0)
            held[me] = source[...]

        def last():
            def end(step, _):
                copy(step, (me + n - step) % n).wait_recv()
                copy(step, me).wait_send()
                return 0

            lax.fori_loop(1, n, end, 0)
            total = held[0].astype(F32)
            for i in range(1, n):
                total = total + held[i].astype(F32)
            out[...] = total

        return [first, last]


class Ring:
    reach = ("ring", "fsdp")

    def __init__(self, streams):
        self.n = lax.axis_size("ctx")
        self.parts = lax.axis_size("fsdp")
        self.per = self.n // self.parts
        self.streams = []
        self.ins, self.outs, self.scratch = [], [], []
        for array, direction, crossing in streams:
            n, rows, columns = array.shape
            self.ins.append(array)
            self.outs.append(jax.ShapeDtypeStruct(array.shape, array.dtype))
            self.scratch.append(pltpu.VMEM((n - 1, rows, columns), array.dtype))
            middle = (columns // 2 + LANES - 1) // LANES * LANES
            for low, high in ((0, middle), (middle, columns)):
                self.streams.append((len(self.ins) - 1, direction, crossing, slice(low, high)))
        self.scratch += [pltpu.SemaphoreType.DMA((len(self.streams), 2, self.n))] * 2

    def phases(self, place, ins, outs, scratch):
        slots, (send, recv) = scratch[:-2], scratch[-2:]
        n, parts, per, here = self.n, self.parts, self.per, place.position
        shift = place.ctx // per
        owner = (place.part + shift) % parts

        def slab(stream, position):
            index = place.at(position)
            return (index + per * place.part) % n if self.streams[stream][2] else index

        def reducing(stream, step):
            array, direction, _, columns = self.streams[stream]
            if step == 0:
                source = ins[array].at[slab(stream, here - direction), :, columns]
            else:
                source = slots[array].at[step - 1, :, columns]
            return remote(
                source,
                slots[array].at[step, :, columns],
                send.at[stream, 0, step],
                recv.at[stream, 0, step],
                ctx=place.at(here + direction),
            )

        def crossing(stream):
            array, _, _, columns = self.streams[stream]
            return remote(
                slots[array].at[n - 2, :, columns],
                outs[array].at[place.ctx, :, columns],
                send.at[stream, 0, n - 1],
                recv.at[stream, 0, n - 1],
                fsdp=owner,
            )

        def gathering(stream, step, back=0):
            array, direction, _, columns = self.streams[stream]
            index = place.at(here - direction * (step + back))
            return remote(
                outs[array].at[index, :, columns],
                outs[array].at[index, :, columns],
                send.at[stream, 1, step],
                recv.at[stream, 1, step],
                ctx=place.at(here + direction),
            )

        every = range(len(self.streams))

        def begin():
            for stream in every:
                reducing(stream, 0).start()

        def add(stream, step):
            array, direction, _, columns = self.streams[stream]
            reducing(stream, step).wait_recv()
            own = ins[array][slab(stream, here - direction * (step + 2)), :, columns]
            return (slots[array][step, :, columns].astype(F32) + own.astype(F32)).astype(own.dtype)

        def reduce(step):
            for stream in every:
                array, _, _, columns = self.streams[stream]
                slots[array][step - 1, :, columns] = add(stream, step - 1)
                reducing(stream, step).start()

        def turn():
            for stream in every:
                array, _, crosses, columns = self.streams[stream]
                total = add(stream, n - 2)
                if not crosses:
                    outs[array][place.ctx, :, columns] = total
                    gathering(stream, 0).start()
                    continue

                @pl.when(shift == 0)
                def _():
                    outs[array][place.ctx, :, columns] = total

                @pl.when(shift != 0)
                def _():
                    slots[array][n - 2, :, columns] = total
                    crossing(stream).start()

        def launch():
            for stream in every:
                if self.streams[stream][2]:

                    @pl.when(shift != 0)
                    def _():
                        crossing(stream).wait()

                    gathering(stream, 0).start()

        def forward(step):
            for stream in every:
                gathering(stream, step - 1, 1).wait_recv()
                gathering(stream, step).start()

        def end():
            for stream in every:
                gathering(stream, n - 2, 1).wait_recv()
            for stream in every:
                for step in range(n - 1):
                    reducing(stream, step).wait_send()
                    gathering(stream, step).wait_send()

        steps = [begin]
        steps += [functools.partial(reduce, step) for step in range(1, n - 1)]
        steps += [turn, launch]
        steps += [functools.partial(forward, step) for step in range(1, n - 1)]
        return steps + [end]


def exchange_kernel(transfers, *refs):
    refs = list(refs)

    def take(lists):
        taken = []
        for items in lists:
            taken.append(refs[: len(items)])
            del refs[: len(items)]
        return taken

    ins = take([t.ins for t in transfers])
    outs = take([t.outs for t in transfers])
    scratch = take([t.scratch for t in transfers])
    place = Place()
    reach = {name for t in transfers for name in t.reach}
    peers = []
    if "fsdp" in reach:
        peers += [dict(fsdp=(place.part + k) % place.parts) for k in range(1, place.parts)]
    if "ctx" in reach:
        peers += [dict(ctx=(place.ctx + k) % place.n_ctx) for k in range(1, place.n_ctx)]
    if "ring" in reach:
        peers += [dict(ctx=place.at(place.position + k)) for k in (1, -1)]
    barrier = pltpu.get_barrier_semaphore()
    for peer in peers:
        pl.semaphore_signal(barrier, inc=1, device_id=peer, device_id_type=pl.DeviceIdType.MESH)
    pl.semaphore_wait(barrier, len(peers))
    lists = [t.phases(place, *each) for t, *each in zip(transfers, ins, outs, scratch)]
    for index in range(max(map(len, lists))):
        for phases in lists:
            if index < len(phases):
                phases[index]()


def exchange(number, name, *transfers):
    memory = pl.BlockSpec(memory_space=pltpu.VMEM)
    ins = [a for t in transfers for a in t.ins]
    outs = [a for t in transfers for a in t.outs]
    results = pl.pallas_call(
        functools.partial(exchange_kernel, transfers),
        out_shape=outs,
        in_specs=[memory] * len(ins),
        out_specs=[memory] * len(outs),
        scratch_shapes=[s for t in transfers for s in t.scratch],
        compiler_params=pltpu.CompilerParams(collective_id=number, has_side_effects=True),
        name=name,
    )(*ins)
    results = list(results)
    split = []
    for t in transfers:
        split.append(results[: len(t.outs)])
        del results[: len(t.outs)]
    return split


def like(shape, dtype):
    return jax.ShapeDtypeStruct(shape, dtype)


def share(transfer, place, refs, ins, outs):
    count = len(transfer.scratch)
    taken = refs[:count]
    del refs[:count]
    return transfer.phases(place, ins, outs, taken)


def quarter_rows(place_index, own):
    return pl.ds(pl.multiple_of(place_index * own, own), own)


def scattered(place, partial, part, scatter_phases):
    first, second, third, fourth = scatter_phases

    def fill(index):
        part[index] = partial(index).astype(part.dtype)

    def begin():
        fill(place.diagonal)
        fill(place.beside)
        first()

    def middle():
        fill(place.far)
        second()

    def later():
        fill(place.part)
        third()

    return [begin, middle, later, fourth]


class Middle:
    reach = ("fsdp", "ctx")

    def __init__(self, blocks, seqs, out_w, x_full, vectors):
        own, width = x_full.shape
        parts = lax.axis_size("fsdp")
        self.own, self.parts = own, parts
        self.heads = FromHeads([blocks], seqs)
        self.scatter = Scatter(like((parts, own, width), BF16))
        self.gather = Gather(like((own, width), BF16))
        self.ins = [blocks, out_w, x_full, vectors]
        self.outs = [
            self.heads.outs[0],
            like((own, width), F32),
            like((own, width), F32),
            like((own, 1), F32),
            self.gather.outs[0],
        ]
        self.scratch = [
            pltpu.VMEM((parts, own, width), BF16),
            pltpu.VMEM((own, width), F32),
            pltpu.VMEM((own, width), BF16),
        ]
        for transfer in (self.heads, self.scatter, self.gather):
            self.scratch += transfer.scratch

    def phases(self, place, ins, outs, scratch):
        blocks, out_w, x_full, vectors = ins
        attended, resid, hat, inv, normed_all = outs
        part, branch, normed, *rest = scratch
        heads = share(self.heads, place, rest, [blocks], [attended])
        scatter = share(self.scatter, place, rest, [part], [branch])
        gather = share(self.gather, place, rest, [normed], [normed_all])
        seqs, _, half, cols = attended.shape
        group = seqs // self.parts

        def partial(index):
            rows = attended[pl.ds(index * group, group)].reshape(self.own, cols)
            return dot(rows, out_w[...])

        def norm():
            total = x_full[...] + branch[...] + vectors[0:1]
            resid[...] = total
            hat[...], inv[...] = normalize(total)
            normed[...] = (hat[...] * vectors[1:2] + vectors[2:3]).astype(BF16)

        return heads + scattered(place, partial, part, scatter) + [norm] + gather


class SecondBack:
    reach = ("fsdp",)

    def __init__(self, grad_pre, fc, hat, inv, gain, grad_y, out_w):
        own, width = hat.shape
        parts = lax.axis_size("fsdp")
        self.own, self.parts = own, parts
        self.scatter = Scatter(like((parts, own, width), BF16))
        self.gather = Gather(like((own, width), BF16))
        self.ins = [grad_pre, fc, hat, inv, gain, grad_y, out_w]
        self.outs = [
            like((own, width), F32),
            self.gather.outs[0],
            like((parts * own, out_w.shape[0]), BF16),
            like((4, width), F32),
        ]
        self.scratch = [
            pltpu.VMEM((parts, own, width), BF16),
            pltpu.VMEM((own, width), F32),
            pltpu.VMEM((own, width), BF16),
        ]
        for transfer in (self.scatter, self.gather):
            self.scratch += transfer.scratch

    def phases(self, place, ins, outs, scratch):
        grad_pre, fc, hat, inv, gain, grad_y, out_w = ins
        resid, branch_all, attended, sums = outs
        part, norm_grad, branch, *rest = scratch
        scatter = share(self.scatter, place, rest, [part], [norm_grad])
        gather = share(self.gather, place, rest, [branch], [branch_all])
        own = self.own

        def partial(index):
            return dot_nt(grad_pre[quarter_rows(index, own), :], fc[...])

        def norm():
            given = grad_y[...].astype(F32)
            total = given + norm_back(norm_grad[...], gain[...], hat[...], inv[...])
            resid[...] = total
            branch[...] = total.astype(BF16)
            sums[0:1] = jnp.sum(norm_grad[...] * hat[...], axis=0, keepdims=True)
            sums[1:2] = jnp.sum(norm_grad[...], axis=0, keepdims=True)
            sums[2:3] = jnp.sum(branch[...].astype(F32), axis=0, keepdims=True)
            sums[3:4] = jnp.sum(given, axis=0, keepdims=True)

        def project():
            for index in range(self.parts):
                rows = dot_nt(branch_all[index], out_w[...])
                attended[index * own : (index + 1) * own] = rows.astype(BF16)

        return scattered(place, partial, part, scatter) + [norm] + gather + [project]


class FirstBack:
    reach = ("fsdp", "ctx")

    def __init__(self, grads, weights, hat, inv, gain, resid, rest, bias_fc):
        own, width = hat.shape
        parts = lax.axis_size("fsdp")
        self.own, self.parts, self.count = own, parts, len(grads)
        quarter = width // parts
        lines = rest.shape[0] + 2
        self.scatter = Scatter(like((parts, own, width), BF16))
        self.small = Scatter(like((parts, lines, quarter), F32))
        self.total = Total(like((lines + bias_fc.shape[0], quarter), F32))
        self.ins = [*grads, *weights, hat, inv, gain, resid, rest, bias_fc]
        self.outs = [like((own, width), F32), self.total.outs[0]]
        self.scratch = [
            pltpu.VMEM((parts, own, width), BF16),
            pltpu.VMEM((own, width), F32),
            pltpu.VMEM((lines, width), F32),
            pltpu.VMEM((parts, lines, quarter), F32),
            pltpu.VMEM((lines, quarter), F32),
            pltpu.VMEM((lines + bias_fc.shape[0], quarter), F32),
        ]
        for transfer in (self.scatter, self.small, self.total):
            self.scratch += transfer.scratch

    def phases(self, place, ins, outs, scratch):
        grads, weights = ins[: self.count], ins[self.count : 2 * self.count]
        hat, inv, gain, resid, others, bias_fc = ins[2 * self.count :]
        input_grad, totals = outs
        part, norm_grad, lines, small, small_sum, packed, *rest = scratch
        scatter = share(self.scatter, place, rest, [part], [norm_grad])
        small_scatter = share(self.small, place, rest, [small], [small_sum])
        total = share(self.total, place, rest, [packed], [totals])
        quarter = small.shape[2]
        count = lines.shape[0]

        def partial(index):
            rows = quarter_rows(index, self.own)
            return sum(dot_nt(grad[rows, :], weight[...]) for grad, weight in zip(grads, weights))

        def norm():
            input_grad[...] = resid[...] + norm_back(norm_grad[...], gain[...], hat[...], inv[...])
            lines[0:1] = jnp.sum(norm_grad[...] * hat[...], axis=0, keepdims=True)
            lines[1:2] = jnp.sum(norm_grad[...], axis=0, keepdims=True)
            lines[2:] = others[...]
            for index in range(self.parts):
                small[index] = lines[:, index * quarter : (index + 1) * quarter]

        def pack():
            packed[:count] = small_sum[...]
            packed[count:] = bias_fc[...]
            total[0]()

        phases = scattered(place, partial, part, scatter) + [norm] + small_scatter
        return phases + [pack, total[1]]


def results_kernel(widths, parts, order_ref, *refs):
    for index, (live, total) in enumerate(widths):
        out = refs[len(widths) * parts + index]
        for part in range(parts):
            stop = min((part + 1) * live, total)
            block = refs[index * parts + part][0, :, : stop - part * live]
            out[:, part * live : stop] = block.astype(F32)


def by_rows(arrays, widths, per, part, parts):
    slabs, rows, _ = arrays[0].shape
    order = (part - jnp.arange(parts, dtype=jnp.int32) + parts) % parts
    if rows % 8:
        outs = []
        for array, (live, total) in zip(arrays, widths):
            array = jnp.take(array.reshape(parts, per, rows, -1), order, axis=0)[..., :live]
            array = jnp.transpose(array, (1, 2, 0, 3)).reshape(per * rows, parts * live)
            outs.append(array[:, :total].astype(F32))
        return outs
    step = 40 if rows % 40 == 0 else rows
    inner = rows // step

    def source(column, array):
        return pl.BlockSpec(
            (1, step, array.shape[2]),
            lambda i, order: (order[column] * per + i // inner, i % inner, 0),
        )

    return pl.pallas_call(
        functools.partial(results_kernel, widths, parts),
        out_shape=[jax.ShapeDtypeStruct((per * rows, total), F32) for _, total in widths],
        grid_spec=pltpu.PrefetchScalarGridSpec(
            num_scalar_prefetch=1,
            grid=(per * inner,),
            in_specs=[source(column, array) for array in arrays for column in range(parts)],
            out_specs=[pl.BlockSpec((step, total), lambda i, order: (i, 0)) for _, total in widths],
        ),
        name="by_rows",
    )(order, *[array for array in arrays for _ in range(parts)])


def on_device(
    inputs,
    cotangent,
    w_query,
    w_key,
    w_value,
    w_out,
    w_fc,
    w_proj,
    ln1_gain,
    ln1_bias,
    query_bias,
    value_bias,
    out_bias,
    ln2_gain,
    ln2_bias,
    fc_bias,
    proj_bias,
):
    parts = lax.axis_size("fsdp")
    n_ctx = lax.axis_size("ctx")
    me_part = lax.axis_index("fsdp")
    seqs, rows, width = inputs.shape
    hidden = w_fc.shape[1]
    quarter = width // parts
    hidden_part = hidden // parts
    own = seqs * rows
    all_seqs = seqs * parts
    tokens = all_seqs * rows
    length = rows * n_ctx
    half_rows = rows // 2
    groups = n_ctx // all_seqs
    heads_part = -(-HEADS // parts)
    live = heads_part * HEAD
    slots = -(-heads_part // (2 * groups)) * 2 * groups
    cols = slots * HEAD
    piece = cols // groups
    heads_here = heads_part if groups == 1 else slots // groups
    near = (live - quarter) * parts
    per = n_ctx // parts
    slab = width // n_ctx

    def to_slots(vector):
        vector = jnp.pad(vector, (0, parts * live - width)).reshape(parts, live)
        return jnp.pad(vector, ((0, 0), (0, cols - live)))[me_part]

    def by_parts(array):
        return array.astype(BF16).reshape(parts, own, width)

    def by_sequences(array):
        return array.reshape(all_seqs, 2, half_rows, cols)

    def by_slabs(array, count):
        return array.astype(BF16).reshape(count, -1, array.shape[1])

    small = jnp.concatenate(
        [ln1_gain, ln1_bias, query_bias, value_bias, out_bias, ln2_gain, ln2_bias, proj_bias]
    )[None, :]
    small = lax.all_gather(small, "fsdp", axis=0, tiled=True).astype(F32).reshape(parts, 8, quarter)
    gain_one, shift_one, bias_query, bias_value, bias_out, gain_two, shift_two, bias_proj = [
        small[:, i].reshape(-1) for i in range(8)
    ]
    bias_query, bias_value = to_slots(bias_query), to_slots(bias_value)
    bias_fc = fc_bias.astype(F32)

    x_full = inputs.astype(F32).reshape(own, width)
    hat_one, inv_one = normalize(x_full)
    qkv, (out_w,), (normed_one,) = exchange(
        0,
        "start",
        Swap([w_query, w_key, w_value], live, cols),
        Window(w_out, live, cols),
        Gather((hat_one * gain_one + shift_one).astype(BF16)),
    )
    qkv = [weight.reshape(width, cols) for weight in qkv]
    normed_one = normed_one.reshape(tokens, width)
    queries = (dot(normed_one, qkv[0]) + bias_query).astype(BF16)
    keys = dot(normed_one, qkv[1]).astype(BF16)
    values = (dot(normed_one, qkv[2]) + bias_value).astype(BF16)
    heads, (fc,) = exchange(
        1,
        "to_heads",
        ToHeads([by_sequences(a) for a in (queries, keys, values)]),
        Swap([w_fc], hidden_part, hidden_part),
    )
    fc = fc.reshape(width, hidden_part)
    proj = w_proj

    q_seq, k_seq, v_seq = [a.reshape(length, piece) for a in heads]
    o_seq, ot, lse = attend(q_seq, k_seq, v_seq, heads_here)

    def blocks(array):
        return array.reshape(2 * n_ctx, half_rows, piece)

    (attended, resid, hat_two, inv_two, normed_two), (grad_y,) = exchange(
        2,
        "middle",
        Middle(blocks(o_seq), all_seqs, out_w, x_full, jnp.stack([bias_out, gain_two, shift_two])),
        Gather(cotangent.reshape(own, width)),
    )
    attended = attended.reshape(tokens, cols)
    normed_two = normed_two.reshape(tokens, width)
    grad_y = grad_y.reshape(tokens, width)

    pre_act = dot(normed_two, fc) + bias_fc
    value, slope = gelu_both(pre_act)
    activated = value.astype(BF16)
    mlp = by_parts(dot(activated, proj))

    grad_pre = (dot_nt(grad_y, proj) * slope).astype(BF16)
    grad_bias_fc = jnp.sum(grad_pre.astype(F32), axis=0)
    proj_part = by_slabs(dot_tn(activated, grad_y), n_ctx)
    fc_part = by_slabs(dot_tn(normed_two, grad_pre), n_ctx)
    (proj_grad, fc_grad), (grad_resid, grad_branch, grad_attended, sums_two) = exchange(
        3,
        "wide_grads",
        Ring([(proj_part, 1, False), (fc_part, -1, True)]),
        SecondBack(
            grad_pre, fc, hat_two, inv_two, gain_two[None], cotangent.reshape(own, width), out_w
        ),
    )
    grad_branch = grad_branch.reshape(tokens, width)

    ((grad_heads,),) = exchange(4, "to_heads_back", ToHeads([by_sequences(grad_attended)]))
    dq_seq, dk_seq, dv_seq = attend_back(
        q_seq, k_seq, v_seq, grad_heads.reshape(length, piece), ot, lse, heads_here
    )
    (grad_qkv,) = exchange(
        5, "from_heads_back", FromHeads([blocks(a) for a in (dq_seq, dk_seq, dv_seq)], all_seqs)
    )
    grad_qkv = [a.reshape(tokens, cols) for a in grad_qkv]
    grad_bias_query = jnp.sum(grad_qkv[0].astype(F32), axis=0)
    grad_bias_value = jnp.sum(grad_qkv[2].astype(F32), axis=0)

    def window(vector):
        whole = jnp.zeros((parts * live,), F32)
        return lax.dynamic_update_slice_in_dim(whole, vector[:live], me_part * live, 0)[:width]

    small_grads = jnp.concatenate(
        [window(grad_bias_query)[None], window(grad_bias_value)[None], sums_two]
    )

    q_part, k_part, v_part = [by_slabs(dot_tn(normed_one, a), n_ctx) for a in grad_qkv]
    out_part = by_slabs(dot_tn(attended, grad_branch), n_ctx)
    (out_grad, q_grad, k_grad, v_grad), (input_grad, small_grads), (mlp,) = exchange(
        6,
        "narrow_grads",
        Ring([(out_part, 1, False), (q_part, 1, True), (k_part, -1, True), (v_part, -1, True)]),
        FirstBack(
            grad_qkv,
            qkv,
            hat_one,
            inv_one,
            gain_one[None],
            grad_resid,
            small_grads,
            grad_bias_fc.reshape(-1, quarter),
        ),
        Scatter(mlp),
    )
    outputs = (resid + mlp + bias_proj).astype(BF16).reshape(seqs, rows, width)
    input_grad = input_grad.reshape(seqs, rows, width)
    fc_out, q_out, k_out, v_out = by_rows(
        [fc_grad, q_grad, k_grad, v_grad],
        [(hidden_part, hidden)] + [(live, width)] * 3,
        per,
        me_part,
        parts,
    )
    out_rows = out_grad.reshape(cols, width)[:live]
    from_left = lax.ppermute(out_rows[live - near :], "fsdp", [(i, i + 1) for i in range(parts - 1)])
    out_rows = lax.dynamic_slice_in_dim(
        jnp.concatenate([from_left, out_rows]), near - me_part * (live - quarter), quarter, 0
    ).astype(F32)
    return (
        outputs,
        input_grad,
        q_out,
        k_out,
        v_out,
        out_rows,
        fc_out,
        proj_grad.reshape(hidden_part, width).astype(F32),
        small_grads[0],
        small_grads[1],
        small_grads[2],
        small_grads[3],
        small_grads[6],
        small_grads[4],
        small_grads[5],
        small_grads[8:].reshape(-1),
        small_grads[7],
    )


def solution(mesh):
    tokens = P("fsdp", "ctx", None)
    matrix = P("fsdp", None)
    vector = P("fsdp")
    return jax.shard_map(
        on_device,
        mesh=mesh,
        in_specs=(tokens, tokens) + (matrix,) * 6 + (vector,) * 9,
        out_specs=(tokens, tokens) + (matrix,) * 6 + (vector,) * 9,
        check_vma=False,
    )
```

```python
import functools

import jax
import jax.numpy as jnp
from jax import lax
from jax.experimental import pallas as pl
from jax.experimental.pallas import tpu as pltpu
from jax.sharding import PartitionSpec as P

HEADS = 25
HEAD = 64
EPS = 1e-05
SCALE = 0.125
NEGATIVE = -1000000000.0
ROOT = 0.7978845608028654
CUBIC = 0.044715
LANES = 128
F32 = jnp.float32
BF16 = jnp.bfloat16


def normalize(values):
    centre = jnp.mean(values, axis=-1, keepdims=True)
    centred = values - centre
    spread = jnp.mean(centred * centred, axis=-1, keepdims=True)
    inv_std = lax.rsqrt(spread + EPS)
    return (centred * inv_std, inv_std)


def norm_back(grad_norm, gain, normal, inv_std):
    scaled = grad_norm * gain
    return inv_std * (
        scaled
        - jnp.mean(scaled, axis=-1, keepdims=True)
        - normal * jnp.mean(scaled * normal, axis=-1, keepdims=True)
    )


def gelu_both(values):
    tangent = jnp.tanh(ROOT * (values + CUBIC * values * values * values))
    value = 0.5 * values * (1.0 + tangent)
    slope = 0.5 * (1.0 + tangent) + 0.5 * values * (1.0 - tangent * tangent) * ROOT * (
        1.0 + 3.0 * CUBIC * values * values
    )
    return value, slope


def dot(left, right):
    return jnp.dot(left, right, preferred_element_type=F32)


def dot_nt(left, right):
    return lax.dot_general(left, right, (((1,), (1,)), ((), ())), preferred_element_type=F32)


def dot_tn(left, right):
    return lax.dot_general(left, right, (((0,), (0,)), ((), ())), preferred_element_type=F32)


def lane_half(shape, half):
    lane = lax.broadcasted_iota(jnp.int32, shape, 1)
    return (lane < HEAD) if half == 0 else (lane >= HEAD)


def keep_half(array, half):
    return jnp.where(lane_half(array.shape, half), array, jnp.zeros_like(array))


def causal_tail(scores, first_row, block):
    keys = lax.broadcasted_iota(jnp.int32, scores.shape, 0) + first_row
    queries = lax.broadcasted_iota(jnp.int32, scores.shape, 1)
    return jnp.where(keys <= queries, scores, NEGATIVE)


def attend_kernel(block, heads, q_ref, k_ref, v_ref, o_ref, ot_ref, lse_ref):
    length = q_ref.shape[0]
    pair = pl.program_id(0)
    v_t = jnp.transpose(v_ref[...].astype(F32)).astype(BF16)

    def one_head(half):
        for index in range(length // block):
            rows = slice(index * block, (index + 1) * block)
            count = (index + 1) * block
            query = keep_half(q_ref[rows, :], half) * jnp.asarray(SCALE, BF16)
            scores = dot_nt(k_ref[:count, :], query)
            scores = causal_tail(scores, -index * block, block)
            top = jnp.max(scores, axis=0, keepdims=True)
            weights = jnp.exp(scores - top)
            total = jnp.sum(weights, axis=0, keepdims=True)
            lse_ref[0, half : half + 1, rows] = top + jnp.log(total)
            weights = weights * (1.0 / total)
            ot = dot(v_t[half * HEAD : (half + 1) * HEAD, :count], weights.astype(BF16))
            ot_ref[0, half * HEAD : (half + 1) * HEAD, rows] = ot

    one_head(0)

    @pl.when(2 * pair + 1 < heads)
    def _():
        one_head(1)

    @pl.when(2 * pair + 1 >= heads)
    def _():
        ot_ref[0, HEAD:, :] = jnp.zeros((HEAD, length), F32)
        lse_ref[0, 1:2, :] = jnp.zeros((1, length), F32)

    o_ref[...] = jnp.transpose(ot_ref[0]).astype(BF16)


def attend(queries, keys, values, heads):
    length, width = queries.shape
    pairs = width // LANES
    block = min(256, length)
    column = pl.BlockSpec((length, LANES), lambda p: (0, p))
    return pl.pallas_call(
        functools.partial(attend_kernel, block, heads),
        grid=(pairs,),
        in_specs=[column] * 3,
        out_specs=[
            column,
            pl.BlockSpec((1, LANES, length), lambda p: (p, 0, 0)),
            pl.BlockSpec((1, 2, length), lambda p: (p, 0, 0)),
        ],
        out_shape=[
            jax.ShapeDtypeStruct((length, width), BF16),
            jax.ShapeDtypeStruct((pairs, LANES, length), F32),
            jax.ShapeDtypeStruct((pairs, 2, length), F32),
        ],
        name="attend",
    )(queries, keys, values)


def attend_back_kernel(
    block, heads, q_ref, k_ref, v_ref, do_ref, ot_ref, lse_ref, dq_ref, dk_ref, dv_ref, dk_sum, dv_sum
):
    length = q_ref.shape[0]
    pair = pl.program_id(0)
    k_t = jnp.transpose(k_ref[...].astype(F32)).astype(BF16)
    do_t = jnp.transpose(do_ref[...].astype(F32))
    dk_sum[...] = jnp.zeros_like(dk_sum)
    dv_sum[...] = jnp.zeros_like(dv_sum)
    dq_ref[...] = jnp.zeros_like(dq_ref)

    def one_head(half):
        span = slice(half * HEAD, (half + 1) * HEAD)
        shared = jnp.sum(do_t[span, :] * ot_ref[0, span, :], axis=0, keepdims=True)
        for index in range(length // block):
            rows = slice(index * block, (index + 1) * block)
            count = (index + 1) * block
            query = keep_half(q_ref[rows, :], half) * jnp.asarray(SCALE, BF16)
            grad = keep_half(do_ref[rows, :], half)
            scores = dot_nt(k_ref[:count, :], query)
            scores = causal_tail(scores, -index * block, block)
            probs = jnp.exp(scores - lse_ref[0, half : half + 1, rows])
            grad_probs = dot_nt(v_ref[:count, :], grad)
            grad_scores = (probs * (grad_probs - shared[:, rows])).astype(BF16)
            dv_sum[:count, :] += dot(probs.astype(BF16), grad)
            dk_sum[:count, :] += dot(grad_scores, query)
            dq_t = dot(k_t[span, :count], grad_scores) * SCALE
            pad = jnp.zeros_like(dq_t)
            both = jnp.concatenate([dq_t, pad] if half == 0 else [pad, dq_t], axis=0)
            dq_ref[rows, :] = dq_ref[rows, :] + jnp.transpose(both).astype(BF16)

    one_head(0)

    @pl.when(2 * pair + 1 < heads)
    def _():
        one_head(1)

    dk_ref[...] = dk_sum[...].astype(BF16)
    dv_ref[...] = dv_sum[...].astype(BF16)


def attend_back(queries, keys, values, grad, ot, lse, heads):
    length, width = queries.shape
    pairs = width // LANES
    block = min(256, length)
    column = pl.BlockSpec((length, LANES), lambda p: (0, p))
    return pl.pallas_call(
        functools.partial(attend_back_kernel, block, heads),
        grid=(pairs,),
        in_specs=[column] * 4
        + [
            pl.BlockSpec((1, LANES, length), lambda p: (p, 0, 0)),
            pl.BlockSpec((1, 2, length), lambda p: (p, 0, 0)),
        ],
        out_specs=[column] * 3,
        out_shape=[jax.ShapeDtypeStruct((length, width), BF16)] * 3,
        scratch_shapes=[pltpu.VMEM((length, LANES), F32)] * 2,
        name="attend_back",
    )(queries, keys, values, grad, ot, lse)


class Place:
    def __init__(self):
        self.parts = lax.axis_size("fsdp")
        self.n_ctx = lax.axis_size("ctx")
        self.part = lax.axis_index("fsdp")
        self.ctx = lax.axis_index("ctx")
        self.beside = self.part + 1 - 2 * (self.part % 2)
        self.far = (self.part + 2) % self.parts
        self.diagonal = (self.beside + 2) % self.parts

    def at(self, position):
        n = self.n_ctx
        position = (position + 2 * n) % n
        upper = position // (n // 2)
        return (1 - upper) * 2 * position + upper * (2 * (n - 1 - position) + 1)

    @property
    def position(self):
        odd = self.ctx % 2
        return (1 - odd) * (self.ctx // 2) + odd * (self.n_ctx - 1 - self.ctx // 2)


def like(shape, dtype):
    return jax.ShapeDtypeStruct(shape, dtype)


def remote(source, target, send, recv, **where):
    return pltpu.make_async_remote_copy(
        src_ref=source,
        dst_ref=target,
        send_sem=send,
        recv_sem=recv,
        device_id=where,
        device_id_type=pl.DeviceIdType.MESH,
    )


def cut(rows):
    step = 64 if rows % 64 == 0 else rows
    return [slice(start, start + step) for start in range(0, rows, step)]


class Gather:
    reach = ("fsdp",)

    def __init__(self, array):
        self.ins = [array]
        self.parts = lax.axis_size("fsdp")
        self.pieces = cut(array.shape[0])
        self.outs = [jax.ShapeDtypeStruct((self.parts, *array.shape), array.dtype)]
        self.scratch = [pltpu.SemaphoreType.DMA((3, len(self.pieces)))] * 2

    def phases(self, place, ins, outs, scratch):
        (source,), (out,), (send, recv) = ins, outs, scratch
        count = range(len(self.pieces))

        def copy(kind, k, index, target):
            piece = self.pieces[k]
            start = source.at[piece] if kind < 2 else out.at[index, piece]
            return remote(start, out.at[index, piece], send.at[kind, k], recv.at[kind, k], fsdp=target)

        def first():
            for k in count:
                copy(1, k, place.part, place.far).start()
            for k in count:
                copy(0, k, place.part, place.beside).start()
            out[place.part] = source[...]

        def second():
            for k in count:
                copy(1, k, place.far, place.far).wait_recv()
                copy(2, k, place.far, place.beside).start()

        def third():
            for k in count:
                copy(0, k, place.beside, place.beside).wait_recv()
                copy(2, k, place.diagonal, place.beside).wait_recv()
            for k in count:
                copy(0, k, place.part, place.beside).wait_send()
                copy(1, k, place.part, place.far).wait_send()
                copy(2, k, place.far, place.beside).wait_send()

        return [first, second, third]


class Scatter:
    reach = ("fsdp",)

    def __init__(self, array):
        parts, rows, columns = array.shape
        self.ins = [array]
        self.pieces = cut(rows)
        self.outs = [jax.ShapeDtypeStruct((rows, columns), F32)]
        self.scratch = [pltpu.VMEM((rows, columns), array.dtype)] * 3
        self.scratch += [pltpu.SemaphoreType.DMA((3, len(self.pieces)))] * 2

    def phases(self, place, ins, outs, scratch):
        (source,), (out,) = ins, outs
        for_far, for_own, from_far, send, recv = scratch
        count = range(len(self.pieces))

        def copy(kind, k):
            piece = self.pieces[k]
            start, target, where = [
                (source.at[place.diagonal, piece], for_far, place.beside),
                (source.at[place.beside, piece], for_own, place.beside),
                (for_far.at[piece], from_far, place.far),
            ][kind]
            return remote(start, target.at[piece], send.at[kind, k], recv.at[kind, k], fsdp=where)

        def first():
            for k in count:
                copy(0, k).start()
            for k in count:
                copy(1, k).start()

        def second():
            for k in count:
                piece = self.pieces[k]
                copy(0, k).wait_recv()
                total = for_far[piece].astype(F32) + source[place.far, piece].astype(F32)
                for_far[piece] = total.astype(for_far.dtype)
                copy(2, k).start()

        def third():
            for k in count:
                piece = self.pieces[k]
                copy(1, k).wait_recv()
                out[piece] = for_own[piece].astype(F32) + source[place.part, piece].astype(F32)

        def fourth():
            for k in count:
                piece = self.pieces[k]
                copy(2, k).wait_recv()
                out[piece] += from_far[piece].astype(F32)
            for k in count:
                for kind in range(3):
                    copy(kind, k).wait_send()

        return [first, second, third, fourth]


class ToHeads:
    reach = ("ctx",)

    def __init__(self, arrays):
        seqs, _, half, columns = arrays[0].shape
        self.n = lax.axis_size("ctx")
        self.groups = self.n // seqs
        self.piece = columns // self.groups
        self.ins = list(arrays)
        self.outs = [jax.ShapeDtypeStruct((2 * self.n, half, self.piece), a.dtype) for a in arrays]
        self.scratch = [pltpu.SemaphoreType.DMA((len(arrays), 2, self.n))] * 2

    def whole(self, ref, other, half):
        if self.groups == 1:
            return ref.at[other, half]
        column = pl.multiple_of((other % self.groups) * self.piece, LANES)
        return ref.at[other // self.groups, half, :, pl.ds(column, self.piece)]

    def block(self, ref, other, half):
        return ref.at[other if half == 0 else 2 * self.n - 1 - other]

    def source(self, ref, other, half):
        return self.whole(ref, other, half)

    def target(self, ref, other, half):
        return self.block(ref, other, half)

    def phases(self, place, ins, outs, scratch):
        send, recv = scratch
        n, me = self.n, place.ctx
        every = [(i, half) for i in range(len(ins)) for half in range(2)]

        def begin(i):
            def start(step, _):
                other = (me + step) % n
                for half in range(2):
                    remote(
                        self.source(ins[i], other, half),
                        self.target(outs[i], me, half),
                        send.at[i, half, step],
                        recv.at[i, half, step],
                        ctx=other,
                    ).start()
                return 0

            lax.fori_loop(1, n, start, 0)
            for half in range(2):
                self.target(outs[i], me, half)[...] = self.source(ins[i], me, half)[...]

        def first():
            for i in range(len(ins)):
                begin(i)

        self.begin = begin

        def second():
            def end(step, _):
                other = (me + n - step) % n
                for i, half in every:
                    copy = remote(
                        self.source(ins[i], other, half),
                        self.target(outs[i], other, half),
                        send.at[i, half, step],
                        recv.at[i, half, step],
                        ctx=other,
                    )
                    copy.wait_recv()
                    copy.wait_send()
                return 0

            lax.fori_loop(1, n, end, 0)

        return [first, second]


class FromHeads(ToHeads):
    def __init__(self, arrays, seqs):
        blocks, half, piece = arrays[0].shape
        self.n = blocks // 2
        self.groups = self.n // seqs
        self.piece = piece
        self.ins = list(arrays)
        shape = (seqs, 2, half, piece * self.groups)
        self.outs = [jax.ShapeDtypeStruct(shape, a.dtype) for a in arrays]
        self.scratch = [pltpu.SemaphoreType.DMA((len(arrays), 2, self.n))] * 2

    def source(self, ref, other, half):
        return self.block(ref, other, half)

    def target(self, ref, other, half):
        return self.whole(ref, other, half)


class Swap:
    reach = ("fsdp",)

    def __init__(self, arrays, live, wide):
        self.parts = lax.axis_size("fsdp")
        self.live, self.wide = live, wide
        self.ins = list(arrays)
        rows = arrays[0].shape[0]
        shape = (len(arrays), self.parts, rows, wide)
        self.outs = [jax.ShapeDtypeStruct(shape[1:], arrays[0].dtype)] * len(arrays)
        self.scratch = [pltpu.VMEM(shape, arrays[0].dtype)]
        self.scratch += [pltpu.SemaphoreType.DMA((len(arrays), self.parts))] * 2

    def phases(self, place, ins, outs, scratch):
        stage, send, recv = scratch
        parts, live = self.parts, self.live
        every = [(i, step) for step in (2, 3, 1) for i in range(len(ins))]

        def copy(i, step, index):
            other = (place.part + step) % parts
            return remote(
                stage.at[i, other], outs[i].at[index], send.at[i, step], recv.at[i, step], fsdp=other
            )

        def first():
            for i, ref in enumerate(ins):
                for part in range(parts):
                    start = part * live
                    stop = min(start + live, ref.shape[1])
                    stage[i, part, :, : stop - start] = ref[:, start:stop]
                    if stop - start < self.wide:
                        shape = (ref.shape[0], self.wide - stop + start)
                        stage[i, part, :, stop - start :] = jnp.zeros(shape, ref.dtype)
            for i, step in every:
                copy(i, step, place.part).start()
            for i in range(len(ins)):
                outs[i][place.part] = stage[i, place.part]

        def second():
            for i, step in every:
                copy(i, step, (place.part + parts - step) % parts).wait_recv()
                copy(i, step, place.part).wait_send()

        return [first, second]


class Window:
    reach = ("fsdp",)

    def __init__(self, array, live, wide):
        self.parts = lax.axis_size("fsdp")
        self.quarter, columns = array.shape
        self.live, self.wide = live, wide
        self.near = (live - self.quarter) * self.parts
        self.ins = [array]
        self.outs = [jax.ShapeDtypeStruct((wide, columns), array.dtype)]
        self.scratch = [pltpu.VMEM((self.quarter + self.near, columns), array.dtype)]
        self.scratch += [pltpu.SemaphoreType.DMA] * 2

    def phases(self, place, ins, outs, scratch):
        (source,), (out,), (both, send, recv) = ins, outs, scratch
        left = (place.part + self.parts - 1) % self.parts
        copy = remote(
            source.at[: self.near], both.at[self.quarter :], send, recv, fsdp=left
        )

        def first():
            copy.start()
            both[: self.quarter] = source[...]

        def second():
            copy.wait()
            start = pl.multiple_of(place.part * (self.live - self.quarter), 16)
            rows = both[pl.ds(start, self.live), :]
            index = lax.broadcasted_iota(jnp.int32, rows.shape, 0) + place.part * self.live
            inside = index < self.quarter * self.parts
            out[: self.live] = jnp.where(inside, rows, jnp.zeros_like(rows))
            if self.wide > self.live:
                out[self.live :] = jnp.zeros((self.wide - self.live, rows.shape[1]), rows.dtype)

        return [first, second]


class Total:
    reach = ("ctx",)

    def __init__(self, array):
        self.n = lax.axis_size("ctx")
        self.ins = [array]
        self.outs = [jax.ShapeDtypeStruct(array.shape, F32)]
        self.scratch = [pltpu.VMEM((self.n, *array.shape), array.dtype)]
        self.scratch += [pltpu.SemaphoreType.DMA((self.n,))] * 2

    def phases(self, place, ins, outs, scratch):
        (source,), (out,), (held, send, recv) = ins, outs, scratch
        n, me = self.n, place.ctx

        def copy(step, index):
            return remote(source, held.at[index], send.at[step], recv.at[step], ctx=(me + step) % n)

        def first():
            lax.fori_loop(1, n, lambda step, _: (copy(step, me).start(), 0)[1], 0)
            held[me] = source[...]

        def last():
            def end(step, _):
                copy(step, (me + n - step) % n).wait_recv()
                copy(step, me).wait_send()
                return 0

            lax.fori_loop(1, n, end, 0)
            total = held[0].astype(F32)
            for i in range(1, n):
                total = total + held[i].astype(F32)
            out[...] = total

        return [first, last]


class Ring:
    reach = ("ring", "fsdp")

    def __init__(self, products):
        self.n = n = lax.axis_size("ctx")
        self.parts = lax.axis_size("fsdp")
        self.per = n // self.parts
        self.products, self.streams, lefts = [], [], []
        self.ins, self.outs, slots, local, turned = [], [], [], [], []
        ways = [direction for _, _, direction, _ in products]
        for left, right, direction, crossing in products:
            rows, columns = left.shape[1] // n, right.shape[1]
            known = [k for k, other in enumerate(lefts) if other is left]
            if not known:
                lefts.append(left)
                turned.append(pltpu.VMEM((n, rows, left.shape[0]), left.dtype))
            index = len(self.products)
            self.products.append((known[0] if known else len(lefts) - 1, direction, crossing))
            self.ins.append(right)
            self.outs.append(like((n, rows, columns), BF16))
            slots.append(pltpu.VMEM((n - 1, rows, columns), BF16))
            local.append(pltpu.VMEM((2, rows, columns), BF16))
            middle = columns
            if ways.count(direction) == 1:
                middle = (columns // 2 + LANES - 1) // LANES * LANES
            self.streams.append((index, slice(0, middle)))
            if middle < columns:
                self.streams.append((index, slice(middle, columns)))
        self.counts = (len(lefts), len(products))
        self.ins = lefts + self.ins
        self.spaces = [pl.ANY] * len(self.outs)
        self.scratch = turned + slots + local
        self.scratch += [pltpu.SemaphoreType.DMA((len(self.streams), 2, n))] * 2

    def phases(self, place, ins, outs, scratch):
        n_left, n_product = self.counts
        lefts, rights = ins[:n_left], ins[n_left:]
        turned, scratch = scratch[:n_left], scratch[n_left:]
        slots, scratch = scratch[:n_product], scratch[n_product:]
        local, (send, recv) = scratch[:n_product], scratch[n_product:]
        n, parts, per, here = self.n, self.parts, self.per, place.position
        shift = place.ctx // per
        owner = (place.part + shift) % parts

        def make(step):
            for index, (left, direction, crosses) in enumerate(self.products):
                slab = place.at(here - direction * (step + 1))
                if crosses:
                    slab = (slab + per * place.part) % n
                local[index][step % 2] = dot(turned[left][slab], rights[index][...]).astype(BF16)

        def way(stream):
            return self.products[self.streams[stream][0]][1]

        def crosses(stream):
            return self.products[self.streams[stream][0]][2]

        def reducing(stream, step):
            index, columns = self.streams[stream]
            source = local[index].at[0] if step == 0 else slots[index].at[step - 1]
            return remote(
                source.at[:, columns],
                slots[index].at[step, :, columns],
                send.at[stream, 0, step],
                recv.at[stream, 0, step],
                ctx=place.at(here + way(stream)),
            )

        def last(stream):
            index, columns = self.streams[stream]
            return slots[index].at[n - 2, :, columns]

        def mine(stream):
            index, columns = self.streams[stream]
            return outs[index].at[place.ctx, :, columns]

        def crossing(stream):
            return remote(
                last(stream),
                mine(stream),
                send.at[stream, 0, n - 1],
                recv.at[stream, 0, n - 1],
                fsdp=owner,
            )

        def keeping(stream):
            return pltpu.make_async_copy(last(stream), mine(stream), send.at[stream, 0, n - 1])

        def gathering(stream, step, back=0):
            index, columns = self.streams[stream]
            slab = place.at(here - way(stream) * (step + back))
            block = outs[index].at[slab, :, columns]
            source = block
            if step == 0 and back == 0 and not crosses(stream):
                source = last(stream)
            return remote(
                source,
                block,
                send.at[stream, 1, step],
                recv.at[stream, 1, step],
                ctx=place.at(here + way(stream)),
            )

        every = range(len(self.streams))

        def begin():
            for left, target in zip(lefts, turned):
                rows = target.shape[1]
                for k in range(n):
                    target[k] = jnp.transpose(left[:, k * rows : (k + 1) * rows])
            make(0)
            for stream in every:
                reducing(stream, 0).start()
            make(1)

        def add(stream, step):
            index, columns = self.streams[stream]
            reducing(stream, step).wait_recv()
            total = slots[index][step, :, columns].astype(F32)
            total = total + local[index][(step + 1) % 2, :, columns].astype(F32)
            slots[index][step, :, columns] = total.astype(BF16)

        def reduce(step):
            for stream in every:
                add(stream, step - 1)
                reducing(stream, step).start()
            if step == 1:
                for stream in every:
                    reducing(stream, 0).wait_send()
            make(step + 1)

        def turn():
            for stream in every:
                add(stream, n - 2)
                if not crosses(stream):
                    gathering(stream, 0).start()
                    keeping(stream).start()
                    continue

                @pl.when(shift == 0)
                def _():
                    keeping(stream).start()

                @pl.when(shift != 0)
                def _():
                    crossing(stream).start()

        def launch():
            for stream in every:
                if crosses(stream):

                    @pl.when(shift == 0)
                    def _():
                        keeping(stream).wait()

                    @pl.when(shift != 0)
                    def _():
                        crossing(stream).wait()

                    gathering(stream, 0).start()

        def forward(step):
            for stream in every:
                gathering(stream, step - 1, 1).wait_recv()
                gathering(stream, step).start()

        def end():
            for stream in every:
                gathering(stream, n - 2, 1).wait_recv()
            for stream in every:
                if not crosses(stream):
                    keeping(stream).wait()
                for step in range(n - 1):
                    if step:
                        reducing(stream, step).wait_send()
                    gathering(stream, step).wait_send()

        steps = [begin]
        steps += [functools.partial(reduce, step) for step in range(1, n - 1)]
        steps += [turn, launch]
        steps += [functools.partial(forward, step) for step in range(1, n - 1)]
        return steps + [end]


def exchange_kernel(transfers, places, *refs):
    refs = list(refs)
    inputs = refs[: max(places) + 1]
    refs = [inputs[index] for index in places] + refs[len(inputs) :]

    def take(lists):
        taken = []
        for items in lists:
            taken.append(refs[: len(items)])
            del refs[: len(items)]
        return taken

    ins = take([t.ins for t in transfers])
    outs = take([t.outs for t in transfers])
    scratch = take([t.scratch for t in transfers])
    place = Place()
    reach = {name for t in transfers for name in t.reach}
    peers = []
    if "fsdp" in reach:
        peers += [dict(fsdp=(place.part + k) % place.parts) for k in range(1, place.parts)]
    if "ctx" in reach:
        peers += [dict(ctx=(place.ctx + k) % place.n_ctx) for k in range(1, place.n_ctx)]
    if "ring" in reach:
        peers += [dict(ctx=place.at(place.position + k)) for k in (1, -1)]
    barrier = pltpu.get_barrier_semaphore()
    for peer in peers:
        pl.semaphore_signal(barrier, inc=1, device_id=peer, device_id_type=pl.DeviceIdType.MESH)
    pl.semaphore_wait(barrier, len(peers))
    lists = [t.phases(place, *each) for t, *each in zip(transfers, ins, outs, scratch)]
    for index in range(max(map(len, lists))):
        for phases in lists:
            if index < len(phases):
                phases[index]()


def exchange(number, name, *transfers):
    memory = pl.BlockSpec(memory_space=pltpu.VMEM)
    ins, places = [], []
    for array in [a for t in transfers for a in t.ins]:
        known = [k for k, other in enumerate(ins) if other is array]
        places.append(known[0] if known else len(ins))
        if not known:
            ins.append(array)
    outs = [a for t in transfers for a in t.outs]
    spaces = []
    for t in transfers:
        spaces += getattr(t, "spaces", [pltpu.VMEM] * len(t.outs))
    results = pl.pallas_call(
        functools.partial(exchange_kernel, transfers, places),
        out_shape=outs,
        in_specs=[memory] * len(ins),
        out_specs=[pl.BlockSpec(memory_space=space) for space in spaces],
        scratch_shapes=[s for t in transfers for s in t.scratch],
        compiler_params=pltpu.CompilerParams(collective_id=number, has_side_effects=True),
        name=name,
    )(*ins)
    results = list(results)
    split = []
    for t in transfers:
        split.append(results[: len(t.outs)])
        del results[: len(t.outs)]
    return split


def share(transfer, place, refs, ins, outs):
    count = len(transfer.scratch)
    taken = refs[:count]
    del refs[:count]
    return transfer.phases(place, ins, outs, taken)


def quarter_rows(place_index, own):
    return pl.ds(pl.multiple_of(place_index * own, own), own)


def scattered(place, partial, part, scatter_phases):
    first, second, third, fourth = scatter_phases

    def fill(index):
        part[index] = partial(index).astype(part.dtype)

    def begin():
        fill(place.diagonal)
        fill(place.beside)
        first()

    def middle():
        fill(place.far)
        second()

    def later():
        fill(place.part)
        third()

    return [begin, middle, later, fourth]


class Middle:
    reach = ("fsdp", "ctx")

    def __init__(self, blocks, seqs, out_w, x_full, vectors):
        own, width = x_full.shape
        parts = lax.axis_size("fsdp")
        self.own, self.parts = own, parts
        self.heads = FromHeads([blocks], seqs)
        self.scatter = Scatter(like((parts, own, width), BF16))
        self.gather = Gather(like((own, width), BF16))
        self.ins = [blocks, out_w, x_full, vectors]
        self.outs = [
            self.heads.outs[0],
            like((own, width), F32),
            like((own, width), F32),
            like((own, 1), F32),
            self.gather.outs[0],
        ]
        self.scratch = [
            pltpu.VMEM((parts, own, width), BF16),
            pltpu.VMEM((own, width), F32),
            pltpu.VMEM((own, width), BF16),
        ]
        for transfer in (self.heads, self.scatter, self.gather):
            self.scratch += transfer.scratch

    def phases(self, place, ins, outs, scratch):
        blocks, out_w, x_full, vectors = ins
        attended, resid, hat, inv, normed_all = outs
        part, branch, normed, *rest = scratch
        heads = share(self.heads, place, rest, [blocks], [attended])
        scatter = share(self.scatter, place, rest, [part], [branch])
        gather = share(self.gather, place, rest, [normed], [normed_all])
        seqs, _, half, cols = attended.shape
        group = seqs // self.parts

        def partial(index):
            rows = attended[pl.ds(index * group, group)].reshape(self.own, cols)
            return dot(rows, out_w[...])

        def norm():
            total = x_full[...] + branch[...] + vectors[0:1]
            resid[...] = total
            hat[...], inv[...] = normalize(total)
            normed[...] = (hat[...] * vectors[1:2] + vectors[2:3]).astype(BF16)

        return heads + scattered(place, partial, part, scatter) + [norm] + gather


class Product:
    reach = ("fsdp",)

    def __init__(self, left, right, own):
        parts, width = lax.axis_size("fsdp"), right.shape[1]
        self.own = own
        self.scatter = Scatter(like((parts, own, width), BF16))
        self.ins = [left, right]
        self.outs = [like((own, width), F32)]
        self.scratch = [pltpu.VMEM((parts, own, width), BF16), *self.scatter.scratch]

    def phases(self, place, ins, outs, scratch):
        left, right = ins
        part, *rest = scratch
        scatter = share(self.scatter, place, rest, [part], outs)

        def partial(index):
            return dot(left[quarter_rows(index, self.own), :], right[...])

        return scattered(place, partial, part, scatter)


class SecondBack:
    reach = ("fsdp",)

    def __init__(self, grad_pre, fc, hat, inv, gain, grad_y, out_w):
        own, width = hat.shape
        parts = lax.axis_size("fsdp")
        self.own, self.parts = own, parts
        self.scatter = Scatter(like((parts, own, width), BF16))
        self.gather = Gather(like((own, width), BF16))
        self.ins = [grad_pre, fc, hat, inv, gain, grad_y, out_w]
        self.outs = [
            like((own, width), F32),
            self.gather.outs[0],
            like((parts * own, out_w.shape[0]), BF16),
            like((4, width), F32),
        ]
        self.scratch = [
            pltpu.VMEM((parts, own, width), BF16),
            pltpu.VMEM((own, width), F32),
            pltpu.VMEM((own, width), BF16),
        ]
        for transfer in (self.scatter, self.gather):
            self.scratch += transfer.scratch

    def phases(self, place, ins, outs, scratch):
        grad_pre, fc, hat, inv, gain, grad_y, out_w = ins
        resid, branch_all, attended, sums = outs
        part, norm_grad, branch, *rest = scratch
        scatter = share(self.scatter, place, rest, [part], [norm_grad])
        gather = share(self.gather, place, rest, [branch], [branch_all])
        own = self.own

        def partial(index):
            return dot_nt(grad_pre[quarter_rows(index, own), :], fc[...])

        def norm():
            given = grad_y[...].astype(F32)
            total = given + norm_back(norm_grad[...], gain[...], hat[...], inv[...])
            resid[...] = total
            branch[...] = total.astype(BF16)
            sums[0:1] = jnp.sum(norm_grad[...] * hat[...], axis=0, keepdims=True)
            sums[1:2] = jnp.sum(norm_grad[...], axis=0, keepdims=True)
            sums[2:3] = jnp.sum(branch[...].astype(F32), axis=0, keepdims=True)
            sums[3:4] = jnp.sum(given, axis=0, keepdims=True)

        def project():
            for index in range(self.parts):
                rows = dot_nt(branch_all[index], out_w[...])
                attended[index * own : (index + 1) * own] = rows.astype(BF16)

        return scattered(place, partial, part, scatter) + [norm] + gather + [project]


class FirstBack:
    reach = ("fsdp", "ctx")

    def __init__(self, grads, weights, hat, inv, gain, resid, rest, bias_fc):
        own, width = hat.shape
        parts = lax.axis_size("fsdp")
        self.own, self.parts, self.count = own, parts, len(grads)
        quarter = width // parts
        lines = rest.shape[0] + 2
        self.scatter = Scatter(like((parts, own, width), BF16))
        self.small = Scatter(like((parts, lines, quarter), F32))
        self.total = Total(like((lines + bias_fc.shape[0], quarter), F32))
        self.ins = [*grads, *weights, hat, inv, gain, resid, rest, bias_fc]
        self.outs = [like((own, width), F32), self.total.outs[0]]
        self.scratch = [
            pltpu.VMEM((parts, own, width), BF16),
            pltpu.VMEM((own, width), F32),
            pltpu.VMEM((lines, width), F32),
            pltpu.VMEM((parts, lines, quarter), F32),
            pltpu.VMEM((lines, quarter), F32),
            pltpu.VMEM((lines + bias_fc.shape[0], quarter), F32),
        ]
        for transfer in (self.scatter, self.small, self.total):
            self.scratch += transfer.scratch

    def phases(self, place, ins, outs, scratch):
        grads, weights = ins[: self.count], ins[self.count : 2 * self.count]
        hat, inv, gain, resid, others, bias_fc = ins[2 * self.count :]
        input_grad, totals = outs
        part, norm_grad, lines, small, small_sum, packed, *rest = scratch
        scatter = share(self.scatter, place, rest, [part], [norm_grad])
        small_scatter = share(self.small, place, rest, [small], [small_sum])
        total = share(self.total, place, rest, [packed], [totals])
        quarter = small.shape[2]
        count = lines.shape[0]

        def partial(index):
            rows = quarter_rows(index, self.own)
            return sum(dot_nt(grad[rows, :], weight[...]) for grad, weight in zip(grads, weights))

        def norm():
            input_grad[...] = resid[...] + norm_back(norm_grad[...], gain[...], hat[...], inv[...])
            lines[0:1] = jnp.sum(norm_grad[...] * hat[...], axis=0, keepdims=True)
            lines[1:2] = jnp.sum(norm_grad[...], axis=0, keepdims=True)
            lines[2:] = others[...]
            for index in range(self.parts):
                small[index] = lines[:, index * quarter : (index + 1) * quarter]

        def pack():
            packed[:count] = small_sum[...]
            packed[count:] = bias_fc[...]
            total[0]()

        phases = scattered(place, partial, part, scatter) + [norm] + small_scatter
        return phases + [pack, total[1]]


class Later:
    def __init__(self, transfer, *steps):
        self.transfer, self.steps = transfer, steps
        self.reach = transfer.reach
        self.ins, self.outs, self.scratch = transfer.ins, transfer.outs, transfer.scratch

    def phases(self, place, ins, outs, scratch):
        phases = [lambda: None] * (self.steps[-1] + 1)
        for step, phase in zip(self.steps, self.transfer.phases(place, ins, outs, scratch)):
            phases[step] = phase
        return phases


class Spread:
    reach = ("fsdp", "ring")

    def __init__(self, arrays, live, wide):
        self.n = lax.axis_size("ctx")
        self.parts = lax.axis_size("fsdp")
        self.live, self.wide = live, wide
        self.across = wide // LANES
        self.down = self.n // self.across
        self.rows = arrays[0].shape[0] // self.down
        self.ins = list(arrays)
        shape = (self.parts, self.down, self.rows, wide)
        self.outs = [like(shape, a.dtype) for a in arrays]
        self.scratch = [pltpu.VMEM(shape, a.dtype) for a in arrays]
        self.scratch += [pltpu.SemaphoreType.DMA((len(arrays), self.parts + self.n))] * 2

    @staticmethod
    def fits(rows, wide):
        across = wide // LANES
        n = lax.axis_size("ctx")
        return n % across == 0 and rows % (n // across) == 0 and rows // (n // across) % 8 == 0

    def phases(self, place, ins, outs, scratch):
        stages, (send, recv) = scratch[:-2], scratch[-2:]
        n, parts, here = self.n, self.parts, place.position
        every = range(len(ins))

        def of(ctx):
            column = pl.multiple_of(ctx % self.across * LANES, LANES)
            return (ctx // self.across, slice(None), pl.ds(column, LANES))

        def piece(i, step, index):
            other = (place.part + step) % parts
            mine = of(place.ctx)
            return remote(
                stages[i].at[(other, *mine)],
                outs[i].at[(index, *mine)],
                send.at[i, step],
                recv.at[i, step],
                fsdp=other,
            )

        def passing(i, step, back=0):
            direction = 1 - 2 * (i % 2)
            block = outs[i].at[(slice(None), *of(place.at(here - direction * (step + back))))]
            return remote(
                block,
                block,
                send.at[i, parts + step],
                recv.at[i, parts + step],
                ctx=place.at(here + direction),
            )

        def first():
            for i in every:
                for part in range(parts):
                    start = part * self.live
                    stop = min(start + self.live, ins[i].shape[1])
                    for half in range(self.down):
                        rows = slice(half * self.rows, (half + 1) * self.rows)
                        block = ins[i][rows, start:stop]
                        stages[i][part, half, :, : stop - start] = block
                        if stop - start < self.wide:
                            zeros = jnp.zeros((self.rows, self.wide - stop + start), block.dtype)
                            stages[i][part, half, :, stop - start :] = zeros
                for step in (2, 3, 1):
                    piece(i, step, place.part).start()
                mine = of(place.ctx)
                outs[i][(place.part, *mine)] = stages[i][(place.part, *mine)]

        def turn():
            for i in every:
                for step in (1, 2, 3):
                    piece(i, step, (place.part + parts - step) % parts).wait_recv()
                passing(i, 0).start()

        def forward(step):
            for i in every:
                passing(i, step - 1, 1).wait_recv()
                passing(i, step).start()

        def end():
            for i in every:
                passing(i, n - 2, 1).wait_recv()
            for i in every:
                for step in (1, 2, 3):
                    piece(i, step, place.part).wait_send()
                for step in range(n - 1):
                    passing(i, step).wait_send()

        return [first, turn] + [functools.partial(forward, s) for s in range(1, n - 1)] + [end]


class First:
    reach = ("fsdp", "ctx", "ring")

    def __init__(self, inputs, vectors, weights, live, cols, seqs):
        own, width = inputs.shape
        self.parts = parts = lax.axis_size("fsdp")
        self.n = lax.axis_size("ctx")
        self.own, self.live, self.count = own, live, len(vectors)
        quarter = width // parts
        self.spread = Spread(weights[1:], live, cols) if Spread.fits(quarter, cols) else None
        self.swap = Swap(weights[:1] if self.spread else weights, live, cols)
        self.small = Gather(like((len(vectors), quarter), BF16))
        self.gather = Gather(like((own, width), BF16))
        token = like((seqs, 2, own // (seqs // parts) // 2, cols), BF16)
        self.heads = ToHeads([token] * 3)
        self.ins = [inputs, *vectors, *weights]
        self.outs = [
            *[like((width, cols), BF16)] * 3,
            like((own, width), F32),
            like((own, 1), F32),
            self.gather.outs[0],
            like((len(vectors), width), F32),
            *self.heads.outs,
        ]
        self.scratch = [
            pltpu.VMEM((len(vectors), quarter), BF16),
            pltpu.VMEM((parts, len(vectors), quarter), BF16),
            pltpu.VMEM((own, width), BF16),
            pltpu.VMEM((2, cols), F32),
        ]
        self.scratch += [pltpu.VMEM(token.shape, BF16)] * 3
        self.moved = [*self.swap.outs, *(self.spread.outs if self.spread else [])]
        self.scratch += [pltpu.VMEM(out.shape, BF16) for out in self.moved]
        for transfer in (self.swap, self.small, self.gather, self.heads):
            self.scratch += transfer.scratch
        if self.spread:
            self.scratch += self.spread.scratch

    def phases(self, place, ins, outs, scratch):
        inputs, vectors, weights = ins[0], ins[1 : 1 + self.count], ins[1 + self.count :]
        qkv, (hat, inv, normed_all, full), heads_out = outs[:3], outs[3:7], outs[7:]
        small_own, small_all, normed, bias, *rest = scratch
        tokens, rest = rest[:3], rest[3:]
        moved, rest = rest[:3], rest[3:]
        swapped = moved[: len(self.swap.outs)]
        swap = share(self.swap, place, rest, weights[: len(swapped)], swapped)
        small = share(self.small, place, rest, [small_own], [small_all])
        gather = share(self.gather, place, rest, [normed], [normed_all])
        heads = share(self.heads, place, rest, tokens, heads_out)
        begin_heads = self.heads.begin
        spread = []
        if self.spread:
            spread = share(self.spread, place, rest, weights[1:], moved[1:])
        parts, live, own = self.parts, self.live, self.own
        quarter = small_own.shape[1]
        group = tokens[0].shape[0] // parts

        def begin():
            for index, vector in enumerate(vectors):
                small_own[index : index + 1] = vector[...]
            small[0]()
            if spread:
                spread[0]()
            swap[0]()
            hat[...], inv[...] = normalize(inputs[...].astype(F32))

        def norm():
            small[1]()
            small[2]()
            for part in range(parts):
                full[:, part * quarter : (part + 1) * quarter] = small_all[part].astype(F32)
            normed[...] = (hat[...] * full[0:1] + full[1:2]).astype(BF16)
            gather[0]()
            bias[...] = jnp.zeros_like(bias)
            for part in range(parts):

                @pl.when(place.part == part)
                def _():
                    stop = min(live, full.shape[1] - part * live)
                    bias[:, :stop] = full[2:4, part * live : part * live + stop]

        def arrive():
            gather[1]()
            gather[2]()
            swap[1]()

        def unpack(i):
            source, target = moved[i], qkv[i]
            if len(source.shape) == 3:
                rows = source.shape[1]
                for part in range(parts):
                    target[part * rows : (part + 1) * rows] = source[part]
                return
            _, down, rows, _ = source.shape
            for part in range(parts):
                for half in range(down):
                    start = (part * down + half) * rows
                    target[start : start + rows] = source[part, half]

        def project(i):
            unpack(i)
            for part in range(parts):
                rows = dot(normed_all[part], qkv[i][...])
                if i != 1:
                    rows = rows + bias[i // 2 : i // 2 + 1]
                shape = (group, *tokens[i].shape[1:])
                tokens[i][part * group : (part + 1) * group] = rows.astype(BF16).reshape(shape)
            begin_heads(i)

        phases = [begin, norm] + spread[1:] + [arrive]
        self.ready = len(phases)
        return phases + [functools.partial(project, i) for i in range(3)] + [heads[1]]


def results_kernel(widths, parts, order_ref, *refs):
    for index, (live, total) in enumerate(widths):
        out = refs[len(widths) * parts + index]
        for part in range(parts):
            stop = min((part + 1) * live, total)
            block = refs[index * parts + part][0, :, : stop - part * live]
            out[:, part * live : stop] = block.astype(F32)


def by_rows(arrays, widths, per, part, parts):
    slabs, rows, _ = arrays[0].shape
    order = (part - jnp.arange(parts, dtype=jnp.int32) + parts) % parts
    if rows % 8:
        outs = []
        for array, (live, total) in zip(arrays, widths):
            array = jnp.take(array.reshape(parts, per, rows, -1), order, axis=0)[..., :live]
            array = jnp.transpose(array, (1, 2, 0, 3)).reshape(per * rows, parts * live)
            outs.append(array[:, :total].astype(F32))
        return outs
    step = 40 if rows % 40 == 0 else rows
    inner = rows // step

    def source(column, array):
        return pl.BlockSpec(
            (1, step, array.shape[2]),
            lambda i, order: (order[column] * per + i // inner, i % inner, 0),
        )

    return pl.pallas_call(
        functools.partial(results_kernel, widths, parts),
        out_shape=[jax.ShapeDtypeStruct((per * rows, total), F32) for _, total in widths],
        grid_spec=pltpu.PrefetchScalarGridSpec(
            num_scalar_prefetch=1,
            grid=(per * inner,),
            in_specs=[source(column, array) for array in arrays for column in range(parts)],
            out_specs=[pl.BlockSpec((step, total), lambda i, order: (i, 0)) for _, total in widths],
        ),
        name="by_rows",
    )(order, *[array for array in arrays for _ in range(parts)])


def on_device(
    inputs,
    cotangent,
    w_query,
    w_key,
    w_value,
    w_out,
    w_fc,
    w_proj,
    ln1_gain,
    ln1_bias,
    query_bias,
    value_bias,
    out_bias,
    ln2_gain,
    ln2_bias,
    fc_bias,
    proj_bias,
):
    parts = lax.axis_size("fsdp")
    n_ctx = lax.axis_size("ctx")
    me_part = lax.axis_index("fsdp")
    seqs, rows, width = inputs.shape
    hidden = w_fc.shape[1]
    quarter = width // parts
    hidden_part = hidden // parts
    own = seqs * rows
    all_seqs = seqs * parts
    tokens = all_seqs * rows
    length = rows * n_ctx
    half_rows = rows // 2
    groups = n_ctx // all_seqs
    heads_part = -(-HEADS // parts)
    live = heads_part * HEAD
    slots = -(-heads_part // (2 * groups)) * 2 * groups
    cols = slots * HEAD
    piece = cols // groups
    heads_here = heads_part if groups == 1 else slots // groups
    near = (live - quarter) * parts
    per = n_ctx // parts
    slab = width // n_ctx

    def by_sequences(array):
        return array.reshape(all_seqs, 2, half_rows, cols)

    x_full = inputs.astype(F32).reshape(own, width)
    vectors = [ln1_gain, ln1_bias, query_bias, value_bias, out_bias, ln2_gain, ln2_bias, proj_bias]
    first = First(
        inputs.reshape(own, width),
        [vector[None] for vector in vectors],
        [w_query, w_key, w_value],
        live,
        cols,
        all_seqs,
    )
    steps = 3 + (n_ctx if first.spread else 0)
    (*qkv, hat_one, inv_one, normed_one, full, q_heads, k_heads, v_heads), (fc,), (out_w,) = exchange(
        0,
        "first",
        first,
        Later(Swap([w_fc], hidden_part, hidden_part), steps, steps + 3),
        Later(Window(w_out, live, cols), steps, steps + 3),
    )
    gain_one, gain_two, bias_proj = full[0], full[5], full[7]
    bias_fc = fc_bias.astype(F32)
    normed_one = normed_one.reshape(tokens, width)
    fc = fc.reshape(width, hidden_part)
    proj = w_proj
    heads = [q_heads, k_heads, v_heads]

    q_seq, k_seq, v_seq = [a.reshape(length, piece) for a in heads]
    o_seq, ot, lse = attend(q_seq, k_seq, v_seq, heads_here)

    def blocks(array):
        return array.reshape(2 * n_ctx, half_rows, piece)

    (attended, resid, hat_two, inv_two, normed_two), (grad_y,) = exchange(
        2,
        "middle",
        Middle(blocks(o_seq), all_seqs, out_w, x_full, full[4:7]),
        Gather(cotangent.reshape(own, width)),
    )
    attended = attended.reshape(tokens, cols)
    normed_two = normed_two.reshape(tokens, width)
    grad_y = grad_y.reshape(tokens, width)

    pre_act = dot(normed_two, fc) + bias_fc
    value, slope = gelu_both(pre_act)
    activated = value.astype(BF16)

    grad_pre = (dot_nt(grad_y, proj) * slope).astype(BF16)
    grad_bias_fc = jnp.sum(grad_pre.astype(F32), axis=0)
    (proj_grad, fc_grad), (grad_resid, grad_branch, grad_attended, sums_two) = exchange(
        3,
        "wide_grads",
        Ring([(activated, grad_y, 1, False), (normed_two, grad_pre, -1, True)]),
        SecondBack(
            grad_pre, fc, hat_two, inv_two, gain_two[None], cotangent.reshape(own, width), out_w
        ),
    )
    grad_branch = grad_branch.reshape(tokens, width)

    ((grad_heads,),) = exchange(4, "to_heads_back", ToHeads([by_sequences(grad_attended)]))
    dq_seq, dk_seq, dv_seq = attend_back(
        q_seq, k_seq, v_seq, grad_heads.reshape(length, piece), ot, lse, heads_here
    )
    grad_qkv, (mlp,) = exchange(
        5,
        "from_heads_back",
        Later(FromHeads([blocks(a) for a in (dq_seq, dk_seq, dv_seq)], all_seqs), 0, 4),
        Product(activated, proj, own),
    )
    outputs = (resid + mlp + bias_proj).astype(BF16).reshape(seqs, rows, width)
    grad_qkv = [a.reshape(tokens, cols) for a in grad_qkv]
    grad_bias_query = jnp.sum(grad_qkv[0].astype(F32), axis=0)
    grad_bias_value = jnp.sum(grad_qkv[2].astype(F32), axis=0)

    def window(vector):
        whole = jnp.zeros((parts * live,), F32)
        return lax.dynamic_update_slice_in_dim(whole, vector[:live], me_part * live, 0)[:width]

    small_grads = jnp.concatenate(
        [window(grad_bias_query)[None], window(grad_bias_value)[None], sums_two]
    )

    (out_grad, q_grad, k_grad, v_grad), (input_grad, small_grads) = exchange(
        6,
        "narrow_grads",
        Ring(
            [
                (attended, grad_branch, 1, False),
                (normed_one, grad_qkv[0], 1, True),
                (normed_one, grad_qkv[1], -1, True),
                (normed_one, grad_qkv[2], -1, True),
            ]
        ),
        FirstBack(
            grad_qkv,
            qkv,
            hat_one,
            inv_one,
            gain_one[None],
            grad_resid,
            small_grads,
            grad_bias_fc.reshape(-1, quarter),
        ),
    )
    input_grad = input_grad.reshape(seqs, rows, width)
    fc_out, q_out, k_out, v_out = by_rows(
        [fc_grad, q_grad, k_grad, v_grad],
        [(hidden_part, hidden)] + [(live, width)] * 3,
        per,
        me_part,
        parts,
    )
    out_rows = out_grad.reshape(cols, width)[:live]
    from_left = lax.ppermute(out_rows[live - near :], "fsdp", [(i, i + 1) for i in range(parts - 1)])
    out_rows = lax.dynamic_slice_in_dim(
        jnp.concatenate([from_left, out_rows]), near - me_part * (live - quarter), quarter, 0
    ).astype(F32)
    return (
        outputs,
        input_grad,
        q_out,
        k_out,
        v_out,
        out_rows,
        fc_out,
        proj_grad.reshape(hidden_part, width).astype(F32),
        small_grads[0],
        small_grads[1],
        small_grads[2],
        small_grads[3],
        small_grads[6],
        small_grads[4],
        small_grads[5],
        small_grads[8:].reshape(-1),
        small_grads[7],
    )


def solution(mesh):
    tokens = P("fsdp", "ctx", None)
    matrix = P("fsdp", None)
    vector = P("fsdp")
    return jax.shard_map(
        on_device,
        mesh=mesh,
        in_specs=(tokens, tokens) + (matrix,) * 6 + (vector,) * 9,
        out_specs=(tokens, tokens) + (matrix,) * 6 + (vector,) * 9,
        check_vma=False,
    )
```

```python
import functools

import jax
import jax.numpy as jnp
from jax import lax
from jax.experimental import pallas as pl
from jax.experimental.pallas import tpu as pltpu
from jax.sharding import PartitionSpec as P

HEADS = 25
HEAD = 64
EPS = 1e-05
SCALE = 0.125
NEGATIVE = -1000000000.0
ROOT = 0.7978845608028654
CUBIC = 0.044715
LANES = 128
F32 = jnp.float32
BF16 = jnp.bfloat16


def normalize(values):
    centre = jnp.mean(values, axis=-1, keepdims=True)
    centred = values - centre
    spread = jnp.mean(centred * centred, axis=-1, keepdims=True)
    inv_std = lax.rsqrt(spread + EPS)
    return (centred * inv_std, inv_std)


def norm_back(grad_norm, gain, normal, inv_std):
    scaled = grad_norm * gain
    return inv_std * (
        scaled
        - jnp.mean(scaled, axis=-1, keepdims=True)
        - normal * jnp.mean(scaled * normal, axis=-1, keepdims=True)
    )


def gelu_both(values):
    tangent = jnp.tanh(ROOT * (values + CUBIC * values * values * values))
    value = 0.5 * values * (1.0 + tangent)
    slope = 0.5 * (1.0 + tangent) + 0.5 * values * (1.0 - tangent * tangent) * ROOT * (
        1.0 + 3.0 * CUBIC * values * values
    )
    return value, slope


def dot(left, right):
    return jnp.dot(left, right, preferred_element_type=F32)


def dot_nt(left, right):
    return lax.dot_general(left, right, (((1,), (1,)), ((), ())), preferred_element_type=F32)


def dot_tn(left, right):
    return lax.dot_general(left, right, (((0,), (0,)), ((), ())), preferred_element_type=F32)


def lane_half(shape, half):
    lane = lax.broadcasted_iota(jnp.int32, shape, 1)
    return (lane < HEAD) if half == 0 else (lane >= HEAD)


def keep_half(array, half):
    return jnp.where(lane_half(array.shape, half), array, jnp.zeros_like(array))


def causal_tail(scores, first_row, block):
    keys = lax.broadcasted_iota(jnp.int32, scores.shape, 0) + first_row
    queries = lax.broadcasted_iota(jnp.int32, scores.shape, 1)
    return jnp.where(keys <= queries, scores, NEGATIVE)


def attend_kernel(block, heads, q_ref, k_ref, v_ref, o_ref, ot_ref, lse_ref):
    length = q_ref.shape[0]
    pair = pl.program_id(0)
    v_t = jnp.transpose(v_ref[...].astype(F32)).astype(BF16)

    def one_head(half):
        for index in range(length // block):
            rows = slice(index * block, (index + 1) * block)
            count = (index + 1) * block
            query = keep_half(q_ref[rows, :], half) * jnp.asarray(SCALE, BF16)
            scores = dot_nt(k_ref[:count, :], query)
            scores = causal_tail(scores, -index * block, block)
            top = jnp.max(scores, axis=0, keepdims=True)
            weights = jnp.exp(scores - top)
            total = jnp.sum(weights, axis=0, keepdims=True)
            lse_ref[0, half : half + 1, rows] = top + jnp.log(total)
            weights = weights * (1.0 / total)
            ot = dot(v_t[half * HEAD : (half + 1) * HEAD, :count], weights.astype(BF16))
            ot_ref[0, half * HEAD : (half + 1) * HEAD, rows] = ot

    one_head(0)

    @pl.when(2 * pair + 1 < heads)
    def _():
        one_head(1)

    @pl.when(2 * pair + 1 >= heads)
    def _():
        ot_ref[0, HEAD:, :] = jnp.zeros((HEAD, length), F32)
        lse_ref[0, 1:2, :] = jnp.zeros((1, length), F32)

    o_ref[...] = jnp.transpose(ot_ref[0]).astype(BF16)


def attend(queries, keys, values, heads):
    length, width = queries.shape
    pairs = width // LANES
    block = min(256, length)
    column = pl.BlockSpec((length, LANES), lambda p: (0, p))
    return pl.pallas_call(
        functools.partial(attend_kernel, block, heads),
        grid=(pairs,),
        in_specs=[column] * 3,
        out_specs=[
            column,
            pl.BlockSpec((1, LANES, length), lambda p: (p, 0, 0)),
            pl.BlockSpec((1, 2, length), lambda p: (p, 0, 0)),
        ],
        out_shape=[
            jax.ShapeDtypeStruct((length, width), BF16),
            jax.ShapeDtypeStruct((pairs, LANES, length), F32),
            jax.ShapeDtypeStruct((pairs, 2, length), F32),
        ],
        name="attend",
    )(queries, keys, values)


def attend_back_kernel(
    block, heads, q_ref, k_ref, v_ref, do_ref, ot_ref, lse_ref, dq_ref, dk_ref, dv_ref, dk_sum, dv_sum
):
    length = q_ref.shape[0]
    pair = pl.program_id(0)
    k_t = jnp.transpose(k_ref[...].astype(F32)).astype(BF16)
    do_t = jnp.transpose(do_ref[...].astype(F32))
    dk_sum[...] = jnp.zeros_like(dk_sum)
    dv_sum[...] = jnp.zeros_like(dv_sum)
    dq_ref[...] = jnp.zeros_like(dq_ref)

    def one_head(half):
        span = slice(half * HEAD, (half + 1) * HEAD)
        shared = jnp.sum(do_t[span, :] * ot_ref[0, span, :], axis=0, keepdims=True)
        for index in range(length // block):
            rows = slice(index * block, (index + 1) * block)
            count = (index + 1) * block
            query = keep_half(q_ref[rows, :], half) * jnp.asarray(SCALE, BF16)
            grad = keep_half(do_ref[rows, :], half)
            scores = dot_nt(k_ref[:count, :], query)
            scores = causal_tail(scores, -index * block, block)
            probs = jnp.exp(scores - lse_ref[0, half : half + 1, rows])
            grad_probs = dot_nt(v_ref[:count, :], grad)
            grad_scores = (probs * (grad_probs - shared[:, rows])).astype(BF16)
            dv_sum[:count, :] += dot(probs.astype(BF16), grad)
            dk_sum[:count, :] += dot(grad_scores, query)
            dq_t = dot(k_t[span, :count], grad_scores) * SCALE
            pad = jnp.zeros_like(dq_t)
            both = jnp.concatenate([dq_t, pad] if half == 0 else [pad, dq_t], axis=0)
            dq_ref[rows, :] = dq_ref[rows, :] + jnp.transpose(both).astype(BF16)

    one_head(0)

    @pl.when(2 * pair + 1 < heads)
    def _():
        one_head(1)

    dk_ref[...] = dk_sum[...].astype(BF16)
    dv_ref[...] = dv_sum[...].astype(BF16)


def attend_back(queries, keys, values, grad, ot, lse, heads):
    length, width = queries.shape
    pairs = width // LANES
    block = min(256, length)
    column = pl.BlockSpec((length, LANES), lambda p: (0, p))
    return pl.pallas_call(
        functools.partial(attend_back_kernel, block, heads),
        grid=(pairs,),
        in_specs=[column] * 4
        + [
            pl.BlockSpec((1, LANES, length), lambda p: (p, 0, 0)),
            pl.BlockSpec((1, 2, length), lambda p: (p, 0, 0)),
        ],
        out_specs=[column] * 3,
        out_shape=[jax.ShapeDtypeStruct((length, width), BF16)] * 3,
        scratch_shapes=[pltpu.VMEM((length, LANES), F32)] * 2,
        name="attend_back",
    )(queries, keys, values, grad, ot, lse)


class Place:
    def __init__(self):
        self.parts = lax.axis_size("fsdp")
        self.n_ctx = lax.axis_size("ctx")
        self.part = lax.axis_index("fsdp")
        self.ctx = lax.axis_index("ctx")
        self.beside = self.part + 1 - 2 * (self.part % 2)
        self.far = (self.part + 2) % self.parts
        self.diagonal = (self.beside + 2) % self.parts

    def at(self, position):
        n = self.n_ctx
        position = (position + 2 * n) % n
        upper = position // (n // 2)
        return (1 - upper) * 2 * position + upper * (2 * (n - 1 - position) + 1)

    @property
    def position(self):
        odd = self.ctx % 2
        return (1 - odd) * (self.ctx // 2) + odd * (self.n_ctx - 1 - self.ctx // 2)


def like(shape, dtype):
    return jax.ShapeDtypeStruct(shape, dtype)


def remote(source, target, send, recv, **where):
    return pltpu.make_async_remote_copy(
        src_ref=source,
        dst_ref=target,
        send_sem=send,
        recv_sem=recv,
        device_id=where,
        device_id_type=pl.DeviceIdType.MESH,
    )


def cut(rows):
    step = 64 if rows % 64 == 0 else rows
    return [slice(start, start + step) for start in range(0, rows, step)]


class Gather:
    reach = ("fsdp",)

    def __init__(self, array):
        self.ins = [array]
        self.parts = lax.axis_size("fsdp")
        self.pieces = cut(array.shape[0])
        self.outs = [jax.ShapeDtypeStruct((self.parts, *array.shape), array.dtype)]
        self.scratch = [pltpu.SemaphoreType.DMA((3, len(self.pieces)))] * 2

    def phases(self, place, ins, outs, scratch):
        (source,), (out,), (send, recv) = ins, outs, scratch
        count = range(len(self.pieces))

        def copy(kind, k, index, target):
            piece = self.pieces[k]
            start = source.at[piece] if kind < 2 else out.at[index, piece]
            return remote(start, out.at[index, piece], send.at[kind, k], recv.at[kind, k], fsdp=target)

        def first():
            for k in count:
                copy(1, k, place.part, place.far).start()
            for k in count:
                copy(0, k, place.part, place.beside).start()
            out[place.part] = source[...]

        def second():
            for k in count:
                copy(1, k, place.far, place.far).wait_recv()
                copy(2, k, place.far, place.beside).start()

        def third():
            for k in count:
                copy(0, k, place.beside, place.beside).wait_recv()
                copy(2, k, place.diagonal, place.beside).wait_recv()
            for k in count:
                copy(0, k, place.part, place.beside).wait_send()
                copy(1, k, place.part, place.far).wait_send()
                copy(2, k, place.far, place.beside).wait_send()

        return [first, second, third]


class Scatter:
    reach = ("fsdp",)

    def __init__(self, array):
        parts, rows, columns = array.shape
        self.ins = [array]
        self.pieces = cut(rows)
        self.outs = [jax.ShapeDtypeStruct((rows, columns), F32)]
        self.scratch = [pltpu.VMEM((rows, columns), array.dtype)] * 3
        self.scratch += [pltpu.SemaphoreType.DMA((3, len(self.pieces)))] * 2

    def phases(self, place, ins, outs, scratch):
        (source,), (out,) = ins, outs
        for_far, for_own, from_far, send, recv = scratch
        count = range(len(self.pieces))

        def copy(kind, k):
            piece = self.pieces[k]
            start, target, where = [
                (source.at[place.diagonal, piece], for_far, place.beside),
                (source.at[place.beside, piece], for_own, place.beside),
                (for_far.at[piece], from_far, place.far),
            ][kind]
            return remote(start, target.at[piece], send.at[kind, k], recv.at[kind, k], fsdp=where)

        def first():
            for k in count:
                copy(0, k).start()
            for k in count:
                copy(1, k).start()

        def second():
            for k in count:
                piece = self.pieces[k]
                copy(0, k).wait_recv()
                total = for_far[piece].astype(F32) + source[place.far, piece].astype(F32)
                for_far[piece] = total.astype(for_far.dtype)
                copy(2, k).start()

        def third():
            for k in count:
                piece = self.pieces[k]
                copy(1, k).wait_recv()
                out[piece] = for_own[piece].astype(F32) + source[place.part, piece].astype(F32)

        def fourth():
            for k in count:
                piece = self.pieces[k]
                copy(2, k).wait_recv()
                out[piece] += from_far[piece].astype(F32)
            for k in count:
                for kind in range(3):
                    copy(kind, k).wait_send()

        return [first, second, third, fourth]


class ToHeads:
    reach = ("ctx",)

    def __init__(self, arrays):
        seqs, _, half, columns = arrays[0].shape
        self.n = lax.axis_size("ctx")
        self.groups = self.n // seqs
        self.piece = columns // self.groups
        self.ins = list(arrays)
        self.outs = [jax.ShapeDtypeStruct((2 * self.n, half, self.piece), a.dtype) for a in arrays]
        self.scratch = [pltpu.SemaphoreType.DMA((len(arrays), 2, self.n))] * 2

    def whole(self, ref, other, half):
        if self.groups == 1:
            return ref.at[other, half]
        column = pl.multiple_of((other % self.groups) * self.piece, LANES)
        return ref.at[other // self.groups, half, :, pl.ds(column, self.piece)]

    def block(self, ref, other, half):
        return ref.at[other if half == 0 else 2 * self.n - 1 - other]

    def source(self, ref, other, half):
        return self.whole(ref, other, half)

    def target(self, ref, other, half):
        return self.block(ref, other, half)

    def phases(self, place, ins, outs, scratch):
        send, recv = scratch
        n, me = self.n, place.ctx
        every = [(i, half) for i in range(len(ins)) for half in range(2)]

        def begin(i):
            def start(step, _):
                other = (me + step) % n
                for half in range(2):
                    remote(
                        self.source(ins[i], other, half),
                        self.target(outs[i], me, half),
                        send.at[i, half, step],
                        recv.at[i, half, step],
                        ctx=other,
                    ).start()
                return 0

            lax.fori_loop(1, n, start, 0)
            for half in range(2):
                self.target(outs[i], me, half)[...] = self.source(ins[i], me, half)[...]

        def first():
            def start(step, _):
                other = (me + step) % n
                for i, half in every:
                    remote(
                        self.source(ins[i], other, half),
                        self.target(outs[i], me, half),
                        send.at[i, half, step],
                        recv.at[i, half, step],
                        ctx=other,
                    ).start()
                return 0

            lax.fori_loop(1, n, start, 0)
            for i, half in every:
                self.target(outs[i], me, half)[...] = self.source(ins[i], me, half)[...]

        self.begin = begin

        def second():
            def end(step, _):
                other = (me + n - step) % n
                for i, half in every:
                    copy = remote(
                        self.source(ins[i], other, half),
                        self.target(outs[i], other, half),
                        send.at[i, half, step],
                        recv.at[i, half, step],
                        ctx=other,
                    )
                    copy.wait_recv()
                    copy.wait_send()
                return 0

            lax.fori_loop(1, n, end, 0)

        return [first, second]


class FromHeads(ToHeads):
    def __init__(self, arrays, seqs):
        blocks, half, piece = arrays[0].shape
        self.n = blocks // 2
        self.groups = self.n // seqs
        self.piece = piece
        self.ins = list(arrays)
        shape = (seqs, 2, half, piece * self.groups)
        self.outs = [jax.ShapeDtypeStruct(shape, a.dtype) for a in arrays]
        self.scratch = [pltpu.SemaphoreType.DMA((len(arrays), 2, self.n))] * 2

    def source(self, ref, other, half):
        return self.block(ref, other, half)

    def target(self, ref, other, half):
        return self.whole(ref, other, half)


class Swap:
    reach = ("fsdp",)

    def __init__(self, arrays, live, wide):
        self.parts = lax.axis_size("fsdp")
        self.live, self.wide = live, wide
        self.ins = list(arrays)
        rows = arrays[0].shape[0]
        shape = (len(arrays), self.parts, rows, wide)
        self.outs = [jax.ShapeDtypeStruct(shape[1:], arrays[0].dtype)] * len(arrays)
        self.scratch = [pltpu.VMEM(shape, arrays[0].dtype)]
        self.scratch += [pltpu.SemaphoreType.DMA((len(arrays), self.parts))] * 2

    def phases(self, place, ins, outs, scratch):
        stage, send, recv = scratch
        parts, live = self.parts, self.live
        every = [(i, step) for step in (2, 3, 1) for i in range(len(ins))]

        def copy(i, step, index):
            other = (place.part + step) % parts
            return remote(
                stage.at[i, other], outs[i].at[index], send.at[i, step], recv.at[i, step], fsdp=other
            )

        def first():
            for i, ref in enumerate(ins):
                for part in range(parts):
                    start = part * live
                    stop = min(start + live, ref.shape[1])
                    stage[i, part, :, : stop - start] = ref[:, start:stop]
                    if stop - start < self.wide:
                        shape = (ref.shape[0], self.wide - stop + start)
                        stage[i, part, :, stop - start :] = jnp.zeros(shape, ref.dtype)
            for i, step in every:
                copy(i, step, place.part).start()
            for i in range(len(ins)):
                outs[i][place.part] = stage[i, place.part]

        def second():
            for i, step in every:
                copy(i, step, (place.part + parts - step) % parts).wait_recv()
                copy(i, step, place.part).wait_send()

        return [first, second]


class Window:
    reach = ("fsdp",)

    def __init__(self, array, live, wide):
        self.parts = lax.axis_size("fsdp")
        self.quarter, columns = array.shape
        self.live, self.wide = live, wide
        self.near = (live - self.quarter) * self.parts
        self.ins = [array]
        self.outs = [jax.ShapeDtypeStruct((wide, columns), array.dtype)]
        self.scratch = [pltpu.VMEM((self.quarter + self.near, columns), array.dtype)]
        self.scratch += [pltpu.SemaphoreType.DMA] * 2

    def phases(self, place, ins, outs, scratch):
        (source,), (out,), (both, send, recv) = ins, outs, scratch
        left = (place.part + self.parts - 1) % self.parts
        copy = remote(
            source.at[: self.near], both.at[self.quarter :], send, recv, fsdp=left
        )

        def first():
            copy.start()
            both[: self.quarter] = source[...]

        def second():
            copy.wait()
            start = pl.multiple_of(place.part * (self.live - self.quarter), 16)
            rows = both[pl.ds(start, self.live), :]
            index = lax.broadcasted_iota(jnp.int32, rows.shape, 0) + place.part * self.live
            inside = index < self.quarter * self.parts
            out[: self.live] = jnp.where(inside, rows, jnp.zeros_like(rows))
            if self.wide > self.live:
                out[self.live :] = jnp.zeros((self.wide - self.live, rows.shape[1]), rows.dtype)

        return [first, second]


class Total:
    reach = ("ctx",)

    def __init__(self, array):
        self.n = lax.axis_size("ctx")
        self.ins = [array]
        self.outs = [jax.ShapeDtypeStruct(array.shape, F32)]
        self.scratch = [pltpu.VMEM((self.n, *array.shape), array.dtype)]
        self.scratch += [pltpu.SemaphoreType.DMA((self.n,))] * 2

    def phases(self, place, ins, outs, scratch):
        (source,), (out,), (held, send, recv) = ins, outs, scratch
        n, me = self.n, place.ctx

        def copy(step, index):
            return remote(source, held.at[index], send.at[step], recv.at[step], ctx=(me + step) % n)

        def first():
            lax.fori_loop(1, n, lambda step, _: (copy(step, me).start(), 0)[1], 0)
            held[me] = source[...]

        def last():
            def end(step, _):
                copy(step, (me + n - step) % n).wait_recv()
                copy(step, me).wait_send()
                return 0

            lax.fori_loop(1, n, end, 0)
            total = held[0].astype(F32)
            for i in range(1, n):
                total = total + held[i].astype(F32)
            out[...] = total

        return [first, last]


class Ring:
    reach = ("ring", "fsdp")

    def __init__(self, products):
        self.n = n = lax.axis_size("ctx")
        self.parts = lax.axis_size("fsdp")
        self.per = n // self.parts
        self.products, self.streams, lefts = [], [], []
        self.ins, self.outs, slots, local, turned = [], [], [], [], []
        for left, right, widths, crossing in products:
            rows, columns = left.shape[1] // n, right.shape[1]
            known = [k for k, other in enumerate(lefts) if other is left]
            if not known:
                lefts.append(left)
                turned.append(pltpu.VMEM((n, rows, left.shape[0]), left.dtype))
            index = len(self.products)
            self.products.append((known[0] if known else len(lefts) - 1, crossing))
            self.ins.append(right)
            self.outs.append(like((n, rows, columns), BF16))
            slots.append(pltpu.VMEM((n - 1, rows, columns), BF16))
            local.append(pltpu.VMEM((2, rows, columns), BF16))
            start = 0
            for direction, count in zip((1, -1), widths):
                if count:
                    self.streams.append((index, slice(start, start + count), direction))
                start += count
        self.streams.sort(key=lambda stream: not self.products[stream[0]][1])
        self.counts = (len(lefts), len(products))
        self.ins = lefts + self.ins
        self.spaces = [pl.ANY] * len(self.outs)
        self.scratch = turned + slots + local
        self.scratch += [pltpu.SemaphoreType.DMA((len(self.streams), 2, n))] * 2

    def phases(self, place, ins, outs, scratch):
        n_left, n_product = self.counts
        lefts, rights = ins[:n_left], ins[n_left:]
        turned, scratch = scratch[:n_left], scratch[n_left:]
        slots, scratch = scratch[:n_product], scratch[n_product:]
        local, (send, recv) = scratch[:n_product], scratch[n_product:]
        n, parts, per, here = self.n, self.parts, self.per, place.position
        shift = place.ctx // per
        owner = (place.part + shift) % parts

        def make(step):
            for stream, (index, columns, direction) in enumerate(self.streams):
                slab = place.at(here - direction * (step + 1))
                if crosses(stream):
                    slab = (slab + per * place.part) % n
                left = turned[self.products[index][0]]
                own = dot(left[slab], rights[index][:, columns])
                local[index][step % 2, :, columns] = own.astype(BF16)

        def way(stream):
            return self.streams[stream][2]

        def crosses(stream):
            return self.products[self.streams[stream][0]][1]

        def reducing(stream, step):
            index, columns, _ = self.streams[stream]
            source = local[index].at[0] if step == 0 else slots[index].at[step - 1]
            return remote(
                source.at[:, columns],
                slots[index].at[step, :, columns],
                send.at[stream, 0, step],
                recv.at[stream, 0, step],
                ctx=place.at(here + way(stream)),
            )

        def last(stream):
            index, columns, _ = self.streams[stream]
            return slots[index].at[n - 2, :, columns]

        def mine(stream):
            index, columns, _ = self.streams[stream]
            return outs[index].at[place.ctx, :, columns]

        def crossing(stream):
            return remote(
                last(stream),
                mine(stream),
                send.at[stream, 0, n - 1],
                recv.at[stream, 0, n - 1],
                fsdp=owner,
            )

        def keeping(stream):
            return pltpu.make_async_copy(last(stream), mine(stream), send.at[stream, 0, n - 1])

        def gathering(stream, step, back=0):
            index, columns, _ = self.streams[stream]
            slab = place.at(here - way(stream) * (step + back))
            block = outs[index].at[slab, :, columns]
            source = block
            if step == 0 and back == 0 and not crosses(stream):
                source = last(stream)
            return remote(
                source,
                block,
                send.at[stream, 1, step],
                recv.at[stream, 1, step],
                ctx=place.at(here + way(stream)),
            )

        every = range(len(self.streams))

        def begin():
            for left, target in zip(lefts, turned):
                rows = target.shape[1]
                for k in range(n):
                    target[k] = jnp.transpose(left[:, k * rows : (k + 1) * rows])
            make(0)
            for stream in every:
                reducing(stream, 0).start()
            make(1)

        def add(stream, step):
            index, columns, _ = self.streams[stream]
            reducing(stream, step).wait_recv()
            total = slots[index][step, :, columns].astype(F32)
            total = total + local[index][(step + 1) % 2, :, columns].astype(F32)
            slots[index][step, :, columns] = total.astype(BF16)

        def reduce(step):
            for stream in every:
                add(stream, step - 1)
                reducing(stream, step).start()
            if step == 1:
                for stream in every:
                    reducing(stream, 0).wait_send()
            make(step + 1)

        def turn():
            for stream in every:
                add(stream, n - 2)
                if not crosses(stream):
                    gathering(stream, 0).start()
                    keeping(stream).start()
                    continue

                @pl.when(shift == 0)
                def _():
                    keeping(stream).start()

                @pl.when(shift != 0)
                def _():
                    crossing(stream).start()

        def launch(stream):
            @pl.when(shift == 0)
            def _():
                keeping(stream).wait()

            @pl.when(shift != 0)
            def _():
                crossing(stream).wait()

            gathering(stream, 0).start()

        def forward(turn):
            for stream in [s for s in every if not crosses(s)] + [s for s in every if crosses(s)]:
                step = turn - 1 if crosses(stream) else turn
                if step == 0:
                    launch(stream)
                elif step < n - 1:
                    gathering(stream, step - 1, 1).wait_recv()
                    gathering(stream, step).start()

        def end():
            for stream in every:
                gathering(stream, n - 2, 1).wait_recv()
            for stream in every:
                if not crosses(stream):
                    keeping(stream).wait()
                for step in range(n - 1):
                    if step:
                        reducing(stream, step).wait_send()
                    gathering(stream, step).wait_send()

        steps = [begin]
        steps += [functools.partial(reduce, step) for step in range(1, n - 1)]
        steps += [turn]
        steps += [functools.partial(forward, step) for step in range(1, n)]
        return steps + [end]


def exchange_kernel(transfers, places, *refs):
    refs = list(refs)
    inputs = refs[: max(places) + 1]
    refs = [inputs[index] for index in places] + refs[len(inputs) :]

    def take(lists):
        taken = []
        for items in lists:
            taken.append(refs[: len(items)])
            del refs[: len(items)]
        return taken

    ins = take([t.ins for t in transfers])
    outs = take([t.outs for t in transfers])
    scratch = take([t.scratch for t in transfers])
    place = Place()
    reach = {name for t in transfers for name in t.reach}
    peers = []
    if "fsdp" in reach:
        peers += [dict(fsdp=(place.part + k) % place.parts) for k in range(1, place.parts)]
    if "ctx" in reach:
        peers += [dict(ctx=(place.ctx + k) % place.n_ctx) for k in range(1, place.n_ctx)]
    if "ring" in reach:
        peers += [dict(ctx=place.at(place.position + k)) for k in (1, -1)]
    barrier = pltpu.get_barrier_semaphore()
    for peer in peers:
        pl.semaphore_signal(barrier, inc=1, device_id=peer, device_id_type=pl.DeviceIdType.MESH)
    pl.semaphore_wait(barrier, len(peers))
    lists = [t.phases(place, *each) for t, *each in zip(transfers, ins, outs, scratch)]
    for index in range(max(map(len, lists))):
        for phases in lists:
            if index < len(phases):
                phases[index]()


def exchange(number, name, *transfers):
    memory = pl.BlockSpec(memory_space=pltpu.VMEM)
    ins, places = [], []
    for array in [a for t in transfers for a in t.ins]:
        known = [k for k, other in enumerate(ins) if other is array]
        places.append(known[0] if known else len(ins))
        if not known:
            ins.append(array)
    outs = [a for t in transfers for a in t.outs]
    spaces = []
    for t in transfers:
        spaces += getattr(t, "spaces", [pltpu.VMEM] * len(t.outs))
    results = pl.pallas_call(
        functools.partial(exchange_kernel, transfers, places),
        out_shape=outs,
        in_specs=[memory] * len(ins),
        out_specs=[pl.BlockSpec(memory_space=space) for space in spaces],
        scratch_shapes=[s for t in transfers for s in t.scratch],
        compiler_params=pltpu.CompilerParams(collective_id=number, has_side_effects=True),
        name=name,
    )(*ins)
    results = list(results)
    split = []
    for t in transfers:
        split.append(results[: len(t.outs)])
        del results[: len(t.outs)]
    return split


def share(transfer, place, refs, ins, outs):
    count = len(transfer.scratch)
    taken = refs[:count]
    del refs[:count]
    return transfer.phases(place, ins, outs, taken)


def quarter_rows(place_index, own):
    return pl.ds(pl.multiple_of(place_index * own, own), own)


def scattered(place, partial, part, scatter_phases):
    first, second, third, fourth = scatter_phases

    def fill(index):
        part[index] = partial(index).astype(part.dtype)

    def begin():
        fill(place.diagonal)
        fill(place.beside)
        first()

    def middle():
        fill(place.far)
        second()

    def later():
        fill(place.part)
        third()

    return [begin, middle, later, fourth]


class Middle:
    reach = ("fsdp", "ctx")

    def __init__(self, blocks, seqs, out_w, x_full, vectors):
        own, width = x_full.shape
        parts = lax.axis_size("fsdp")
        self.own, self.parts = own, parts
        self.heads = FromHeads([blocks], seqs)
        self.scatter = Scatter(like((parts, own, width), BF16))
        self.gather = Gather(like((own, width), BF16))
        self.ins = [blocks, out_w, x_full, vectors]
        self.outs = [
            self.heads.outs[0],
            like((own, width), F32),
            like((own, width), F32),
            like((own, 1), F32),
            self.gather.outs[0],
        ]
        self.scratch = [
            pltpu.VMEM((parts, own, width), BF16),
            pltpu.VMEM((own, width), F32),
            pltpu.VMEM((own, width), BF16),
        ]
        for transfer in (self.heads, self.scatter, self.gather):
            self.scratch += transfer.scratch

    def phases(self, place, ins, outs, scratch):
        blocks, out_w, x_full, vectors = ins
        attended, resid, hat, inv, normed_all = outs
        part, branch, normed, *rest = scratch
        heads = share(self.heads, place, rest, [blocks], [attended])
        scatter = share(self.scatter, place, rest, [part], [branch])
        gather = share(self.gather, place, rest, [normed], [normed_all])
        seqs, _, half, cols = attended.shape
        group = seqs // self.parts

        def partial(index):
            rows = attended[pl.ds(index * group, group)].reshape(self.own, cols)
            return dot(rows, out_w[...])

        def norm():
            total = x_full[...] + branch[...] + vectors[0:1]
            resid[...] = total
            hat[...], inv[...] = normalize(total)
            normed[...] = (hat[...] * vectors[1:2] + vectors[2:3]).astype(BF16)

        return heads + scattered(place, partial, part, scatter) + [norm] + gather


class Product:
    reach = ("fsdp",)

    def __init__(self, left, right, own):
        parts, width = lax.axis_size("fsdp"), right.shape[1]
        self.own = own
        self.scatter = Scatter(like((parts, own, width), BF16))
        self.ins = [left, right]
        self.outs = [like((own, width), F32)]
        self.scratch = [pltpu.VMEM((parts, own, width), BF16), *self.scatter.scratch]

    def phases(self, place, ins, outs, scratch):
        left, right = ins
        part, *rest = scratch
        scatter = share(self.scatter, place, rest, [part], outs)

        def partial(index):
            return dot(left[quarter_rows(index, self.own), :], right[...])

        return scattered(place, partial, part, scatter)


class SecondBack:
    reach = ("fsdp",)

    def __init__(self, grad_pre, fc, hat, inv, gain, grad_y, out_w):
        own, width = hat.shape
        parts = lax.axis_size("fsdp")
        self.own, self.parts = own, parts
        self.scatter = Scatter(like((parts, own, width), BF16))
        self.gather = Gather(like((own, width), BF16))
        self.ins = [grad_pre, fc, hat, inv, gain, grad_y, out_w]
        self.outs = [
            like((own, width), F32),
            self.gather.outs[0],
            like((parts * own, out_w.shape[0]), BF16),
            like((4, width), F32),
        ]
        self.scratch = [
            pltpu.VMEM((parts, own, width), BF16),
            pltpu.VMEM((own, width), F32),
            pltpu.VMEM((own, width), BF16),
        ]
        for transfer in (self.scatter, self.gather):
            self.scratch += transfer.scratch

    def phases(self, place, ins, outs, scratch):
        grad_pre, fc, hat, inv, gain, grad_y, out_w = ins
        resid, branch_all, attended, sums = outs
        part, norm_grad, branch, *rest = scratch
        scatter = share(self.scatter, place, rest, [part], [norm_grad])
        gather = share(self.gather, place, rest, [branch], [branch_all])
        own = self.own

        def partial(index):
            return dot_nt(grad_pre[quarter_rows(index, own), :], fc[...])

        def norm():
            given = grad_y[...].astype(F32)
            total = given + norm_back(norm_grad[...], gain[...], hat[...], inv[...])
            resid[...] = total
            branch[...] = total.astype(BF16)
            sums[0:1] = jnp.sum(norm_grad[...] * hat[...], axis=0, keepdims=True)
            sums[1:2] = jnp.sum(norm_grad[...], axis=0, keepdims=True)
            sums[2:3] = jnp.sum(branch[...].astype(F32), axis=0, keepdims=True)
            sums[3:4] = jnp.sum(given, axis=0, keepdims=True)

        def project():
            for index in range(self.parts):
                rows = dot_nt(branch_all[index], out_w[...])
                attended[index * own : (index + 1) * own] = rows.astype(BF16)

        return scattered(place, partial, part, scatter) + [norm] + gather + [project]


class FirstBack:
    reach = ("fsdp", "ctx")

    def __init__(self, grads, weights, hat, inv, gain, resid, rest, bias_fc):
        own, width = hat.shape
        parts = lax.axis_size("fsdp")
        self.own, self.parts, self.count = own, parts, len(grads)
        quarter = width // parts
        lines = rest.shape[0] + 2
        self.scatter = Scatter(like((parts, own, width), BF16))
        self.small = Scatter(like((parts, lines, quarter), F32))
        self.total = Total(like((lines + bias_fc.shape[0], quarter), F32))
        self.ins = [*grads, *weights, hat, inv, gain, resid, rest, bias_fc]
        self.outs = [like((own, width), F32), self.total.outs[0]]
        self.scratch = [
            pltpu.VMEM((parts, own, width), BF16),
            pltpu.VMEM((own, width), F32),
            pltpu.VMEM((lines, width), F32),
            pltpu.VMEM((parts, lines, quarter), F32),
            pltpu.VMEM((lines, quarter), F32),
            pltpu.VMEM((lines + bias_fc.shape[0], quarter), F32),
        ]
        for transfer in (self.scatter, self.small, self.total):
            self.scratch += transfer.scratch

    def phases(self, place, ins, outs, scratch):
        grads, weights = ins[: self.count], ins[self.count : 2 * self.count]
        hat, inv, gain, resid, others, bias_fc = ins[2 * self.count :]
        input_grad, totals = outs
        part, norm_grad, lines, small, small_sum, packed, *rest = scratch
        scatter = share(self.scatter, place, rest, [part], [norm_grad])
        small_scatter = share(self.small, place, rest, [small], [small_sum])
        total = share(self.total, place, rest, [packed], [totals])
        quarter = small.shape[2]
        count = lines.shape[0]

        def partial(index):
            rows = quarter_rows(index, self.own)
            return sum(dot_nt(grad[rows, :], weight[...]) for grad, weight in zip(grads, weights))

        def norm():
            input_grad[...] = resid[...] + norm_back(norm_grad[...], gain[...], hat[...], inv[...])
            lines[0:1] = jnp.sum(norm_grad[...] * hat[...], axis=0, keepdims=True)
            lines[1:2] = jnp.sum(norm_grad[...], axis=0, keepdims=True)
            lines[2:] = others[...]
            for index in range(self.parts):
                small[index] = lines[:, index * quarter : (index + 1) * quarter]

        def pack():
            packed[:count] = small_sum[...]
            packed[count:] = bias_fc[...]
            total[0]()

        phases = scattered(place, partial, part, scatter) + [norm] + small_scatter
        return phases + [pack, total[1]]


class Later:
    def __init__(self, transfer, *steps):
        self.transfer, self.steps = transfer, steps
        self.reach = transfer.reach
        self.ins, self.outs, self.scratch = transfer.ins, transfer.outs, transfer.scratch

    def phases(self, place, ins, outs, scratch):
        phases = [lambda: None] * (self.steps[-1] + 1)
        for step, phase in zip(self.steps, self.transfer.phases(place, ins, outs, scratch)):
            phases[step] = phase
        return phases


class Spread:
    reach = ("fsdp", "ring")

    def __init__(self, arrays, live, wide):
        self.n = lax.axis_size("ctx")
        self.parts = lax.axis_size("fsdp")
        self.live, self.wide = live, wide
        self.across = wide // LANES
        self.down = self.n // self.across
        self.rows = arrays[0].shape[0] // self.down
        self.ins = list(arrays)
        shape = (self.parts, self.down, self.rows, wide)
        self.outs = [like(shape, a.dtype) for a in arrays]
        self.scratch = [pltpu.VMEM(shape, a.dtype) for a in arrays]
        self.scratch += [pltpu.SemaphoreType.DMA((len(arrays), self.parts + self.n))] * 2

    @staticmethod
    def fits(rows, wide):
        across = wide // LANES
        n = lax.axis_size("ctx")
        return n % across == 0 and rows % (n // across) == 0 and rows // (n // across) % 8 == 0

    def phases(self, place, ins, outs, scratch):
        stages, (send, recv) = scratch[:-2], scratch[-2:]
        n, parts, here = self.n, self.parts, place.position
        every = range(len(ins))

        def of(ctx):
            column = pl.multiple_of(ctx % self.across * LANES, LANES)
            return (ctx // self.across, slice(None), pl.ds(column, LANES))

        def piece(i, step, index):
            other = (place.part + step) % parts
            mine = of(place.ctx)
            return remote(
                stages[i].at[(other, *mine)],
                outs[i].at[(index, *mine)],
                send.at[i, step],
                recv.at[i, step],
                fsdp=other,
            )

        def passing(i, step, back=0):
            direction = 1 - 2 * (i % 2)
            block = outs[i].at[(slice(None), *of(place.at(here - direction * (step + back))))]
            return remote(
                block,
                block,
                send.at[i, parts + step],
                recv.at[i, parts + step],
                ctx=place.at(here + direction),
            )

        def first():
            for i in every:
                for part in range(parts):
                    start = part * self.live
                    stop = min(start + self.live, ins[i].shape[1])
                    for half in range(self.down):
                        rows = slice(half * self.rows, (half + 1) * self.rows)
                        block = ins[i][rows, start:stop]
                        stages[i][part, half, :, : stop - start] = block
                        if stop - start < self.wide:
                            zeros = jnp.zeros((self.rows, self.wide - stop + start), block.dtype)
                            stages[i][part, half, :, stop - start :] = zeros
                for step in (2, 3, 1):
                    piece(i, step, place.part).start()
                mine = of(place.ctx)
                outs[i][(place.part, *mine)] = stages[i][(place.part, *mine)]

        def turn():
            for i in every:
                for step in (1, 2, 3):
                    piece(i, step, (place.part + parts - step) % parts).wait_recv()
                passing(i, 0).start()

        def forward(step):
            for i in every:
                passing(i, step - 1, 1).wait_recv()
                passing(i, step).start()

        def end():
            for i in every:
                passing(i, n - 2, 1).wait_recv()
            for i in every:
                for step in (1, 2, 3):
                    piece(i, step, place.part).wait_send()
                for step in range(n - 1):
                    passing(i, step).wait_send()

        return [first, turn] + [functools.partial(forward, s) for s in range(1, n - 1)] + [end]


class First:
    reach = ("fsdp", "ctx", "ring")

    def __init__(self, inputs, vectors, weights, live, cols, seqs):
        own, width = inputs.shape
        self.parts = parts = lax.axis_size("fsdp")
        self.n = lax.axis_size("ctx")
        self.own, self.live, self.count = own, live, len(vectors)
        quarter = width // parts
        self.spread = Spread(weights[1:], live, cols) if Spread.fits(quarter, cols) else None
        self.swap = Swap(weights[:1] if self.spread else weights, live, cols)
        self.small = Gather(like((len(vectors), quarter), BF16))
        self.gather = Gather(like((own, width), BF16))
        token = like((seqs, 2, own // (seqs // parts) // 2, cols), BF16)
        self.heads = ToHeads([token] * 3)
        self.ins = [inputs, *vectors, *weights]
        self.outs = [
            *[like((width, cols), BF16)] * 3,
            like((own, width), F32),
            like((own, 1), F32),
            self.gather.outs[0],
            like((len(vectors), width), F32),
            *self.heads.outs,
        ]
        self.scratch = [
            pltpu.VMEM((len(vectors), quarter), BF16),
            pltpu.VMEM((parts, len(vectors), quarter), BF16),
            pltpu.VMEM((own, width), BF16),
            pltpu.VMEM((2, cols), F32),
        ]
        self.scratch += [pltpu.VMEM(token.shape, BF16)] * 3
        self.moved = [*self.swap.outs, *(self.spread.outs if self.spread else [])]
        self.scratch += [pltpu.VMEM(out.shape, BF16) for out in self.moved]
        for transfer in (self.swap, self.small, self.gather, self.heads):
            self.scratch += transfer.scratch
        if self.spread:
            self.scratch += self.spread.scratch

    def phases(self, place, ins, outs, scratch):
        inputs, vectors, weights = ins[0], ins[1 : 1 + self.count], ins[1 + self.count :]
        qkv, (hat, inv, normed_all, full), heads_out = outs[:3], outs[3:7], outs[7:]
        small_own, small_all, normed, bias, *rest = scratch
        tokens, rest = rest[:3], rest[3:]
        moved, rest = rest[:3], rest[3:]
        swapped = moved[: len(self.swap.outs)]
        swap = share(self.swap, place, rest, weights[: len(swapped)], swapped)
        small = share(self.small, place, rest, [small_own], [small_all])
        gather = share(self.gather, place, rest, [normed], [normed_all])
        heads = share(self.heads, place, rest, tokens, heads_out)
        begin_heads = self.heads.begin
        spread = []
        if self.spread:
            spread = share(self.spread, place, rest, weights[1:], moved[1:])
        parts, live, own = self.parts, self.live, self.own
        quarter = small_own.shape[1]
        group = tokens[0].shape[0] // parts

        def begin():
            for index, vector in enumerate(vectors):
                small_own[index : index + 1] = vector[...].reshape(1, quarter)
            small[0]()
            if spread:
                spread[0]()
            swap[0]()
            hat[...], inv[...] = normalize(inputs[...].astype(F32))

        def norm():
            small[1]()
            small[2]()
            for part in range(parts):
                full[:, part * quarter : (part + 1) * quarter] = small_all[part].astype(F32)
            normed[...] = (hat[...] * full[0:1] + full[1:2]).astype(BF16)
            gather[0]()
            bias[...] = jnp.zeros_like(bias)
            for part in range(parts):

                @pl.when(place.part == part)
                def _():
                    stop = min(live, full.shape[1] - part * live)
                    bias[:, :stop] = full[2:4, part * live : part * live + stop]

        def arrive():
            gather[1]()
            gather[2]()
            swap[1]()

        def unpack(i):
            source, target = moved[i], qkv[i]
            if len(source.shape) == 3:
                rows = source.shape[1]
                for part in range(parts):
                    target[part * rows : (part + 1) * rows] = source[part]
                return
            _, down, rows, _ = source.shape
            for part in range(parts):
                for half in range(down):
                    start = (part * down + half) * rows
                    target[start : start + rows] = source[part, half]

        def project(i):
            unpack(i)
            for part in range(parts):
                rows = dot(normed_all[part], qkv[i][...])
                if i != 1:
                    rows = rows + bias[i // 2 : i // 2 + 1]
                shape = (group, *tokens[i].shape[1:])
                tokens[i][part * group : (part + 1) * group] = rows.astype(BF16).reshape(shape)
            begin_heads(i)

        phases = [begin, norm] + spread[1:] + [arrive]
        self.ready = len(phases)
        return phases + [functools.partial(project, i) for i in range(3)] + [heads[1]]


def results_kernel(widths, parts, order_ref, *refs):
    for index, (live, total) in enumerate(widths):
        out = refs[len(widths) * parts + index]
        for part in range(parts):
            stop = min((part + 1) * live, total)
            block = refs[index * parts + part][0, :, : stop - part * live]
            out[:, part * live : stop] = block.astype(F32)


def by_rows(arrays, widths, per, part, parts):
    slabs, rows, _ = arrays[0].shape
    order = (part - jnp.arange(parts, dtype=jnp.int32) + parts) % parts
    if rows % 8:
        outs = []
        for array, (live, total) in zip(arrays, widths):
            array = jnp.take(array.reshape(parts, per, rows, -1), order, axis=0)[..., :live]
            array = jnp.transpose(array, (1, 2, 0, 3)).reshape(per * rows, parts * live)
            outs.append(array[:, :total].astype(F32))
        return outs
    step = 40 if rows % 40 == 0 else rows
    inner = rows // step

    def source(column, array):
        return pl.BlockSpec(
            (1, step, array.shape[2]),
            lambda i, order: (order[column] * per + i // inner, i % inner, 0),
        )

    return pl.pallas_call(
        functools.partial(results_kernel, widths, parts),
        out_shape=[jax.ShapeDtypeStruct((per * rows, total), F32) for _, total in widths],
        grid_spec=pltpu.PrefetchScalarGridSpec(
            num_scalar_prefetch=1,
            grid=(per * inner,),
            in_specs=[source(column, array) for array in arrays for column in range(parts)],
            out_specs=[pl.BlockSpec((step, total), lambda i, order: (i, 0)) for _, total in widths],
        ),
        name="by_rows",
    )(order, *[array for array in arrays for _ in range(parts)])


def on_device(
    inputs,
    cotangent,
    w_query,
    w_key,
    w_value,
    w_out,
    w_fc,
    w_proj,
    ln1_gain,
    ln1_bias,
    query_bias,
    value_bias,
    out_bias,
    ln2_gain,
    ln2_bias,
    fc_bias,
    proj_bias,
):
    parts = lax.axis_size("fsdp")
    n_ctx = lax.axis_size("ctx")
    me_part = lax.axis_index("fsdp")
    seqs, rows, width = inputs.shape
    hidden = w_fc.shape[1]
    quarter = width // parts
    hidden_part = hidden // parts
    own = seqs * rows
    all_seqs = seqs * parts
    tokens = all_seqs * rows
    length = rows * n_ctx
    half_rows = rows // 2
    groups = n_ctx // all_seqs
    heads_part = -(-HEADS // parts)
    live = heads_part * HEAD
    slots = -(-heads_part // (2 * groups)) * 2 * groups
    cols = slots * HEAD
    piece = cols // groups
    heads_here = heads_part if groups == 1 else slots // groups
    near = (live - quarter) * parts
    per = n_ctx // parts
    slab = width // n_ctx

    def by_sequences(array):
        return array.reshape(all_seqs, 2, half_rows, cols)

    def uneven(columns, more=1):
        low = (columns // 2 + more * (LANES - 1)) // LANES * LANES
        return (low, columns - low)

    x_full = inputs.astype(F32).reshape(own, width)
    vectors = [ln1_gain, ln1_bias, query_bias, value_bias, out_bias, ln2_gain, ln2_bias, proj_bias]
    first = First(
        inputs.reshape(own, width),
        vectors,
        [w_query, w_key, w_value],
        live,
        cols,
        all_seqs,
    )
    steps = 3 + (n_ctx if first.spread else 0)
    (*qkv, hat_one, inv_one, normed_one, full, q_heads, k_heads, v_heads), (fc,), (out_w,) = exchange(
        0,
        "first",
        first,
        Later(Swap([w_fc], hidden_part, hidden_part), steps, steps + 3),
        Later(Window(w_out, live, cols), steps, steps + 3),
    )
    gain_one, gain_two, bias_proj = full[0], full[5], full[7]
    bias_fc = fc_bias.astype(F32)
    normed_one = normed_one.reshape(tokens, width)
    fc = fc.reshape(width, hidden_part)
    proj = w_proj
    heads = [q_heads, k_heads, v_heads]

    q_seq, k_seq, v_seq = [a.reshape(length, piece) for a in heads]
    o_seq, ot, lse = attend(q_seq, k_seq, v_seq, heads_here)

    def blocks(array):
        return array.reshape(2 * n_ctx, half_rows, piece)

    (attended, resid, hat_two, inv_two, normed_two), (grad_y,) = exchange(
        2,
        "middle",
        Middle(blocks(o_seq), all_seqs, out_w, x_full, full[4:7]),
        Gather(cotangent.reshape(own, width)),
    )
    attended = attended.reshape(tokens, cols)
    normed_two = normed_two.reshape(tokens, width)
    grad_y = grad_y.reshape(tokens, width)

    pre_act = dot(normed_two, fc) + bias_fc
    value, slope = gelu_both(pre_act)
    activated = value.astype(BF16)

    grad_pre = (dot_nt(grad_y, proj) * slope).astype(BF16)
    grad_bias_fc = jnp.sum(grad_pre.astype(F32), axis=0)
    (proj_grad, fc_grad), (grad_resid, grad_branch, grad_attended, sums_two) = exchange(
        3,
        "wide_grads",
        Ring(
            [
                (activated, grad_y, uneven(width), False),
                (normed_two, grad_pre, uneven(hidden_part, 0), True),
            ]
        ),
        SecondBack(
            grad_pre, fc, hat_two, inv_two, gain_two[None], cotangent.reshape(own, width), out_w
        ),
    )
    grad_branch = grad_branch.reshape(tokens, width)

    ((grad_heads,),) = exchange(4, "to_heads_back", ToHeads([by_sequences(grad_attended)]))
    dq_seq, dk_seq, dv_seq = attend_back(
        q_seq, k_seq, v_seq, grad_heads.reshape(length, piece), ot, lse, heads_here
    )
    grad_qkv, (mlp,) = exchange(
        5,
        "from_heads_back",
        Later(FromHeads([blocks(a) for a in (dq_seq, dk_seq, dv_seq)], all_seqs), 0, 4),
        Product(activated, proj, own),
    )
    outputs = (resid + mlp + bias_proj).astype(BF16).reshape(seqs, rows, width)
    grad_qkv = [a.reshape(tokens, cols) for a in grad_qkv]
    grad_bias_query = jnp.sum(grad_qkv[0].astype(F32), axis=0)
    grad_bias_value = jnp.sum(grad_qkv[2].astype(F32), axis=0)

    def window(vector):
        whole = jnp.zeros((parts * live,), F32)
        return lax.dynamic_update_slice_in_dim(whole, vector[:live], me_part * live, 0)[:width]

    small_grads = jnp.concatenate(
        [window(grad_bias_query)[None], window(grad_bias_value)[None], sums_two]
    )

    (out_grad, q_grad, k_grad, v_grad), (input_grad, small_grads) = exchange(
        6,
        "narrow_grads",
        Ring(
            [
                (attended, grad_branch, uneven(width), False),
                (normed_one, grad_qkv[0], (cols, 0), True),
                (normed_one, grad_qkv[1], (0, cols), True),
                (normed_one, grad_qkv[2], uneven(cols), True),
            ]
        ),
        FirstBack(
            grad_qkv,
            qkv,
            hat_one,
            inv_one,
            gain_one[None],
            grad_resid,
            small_grads,
            grad_bias_fc.reshape(-1, quarter),
        ),
    )
    input_grad = input_grad.reshape(seqs, rows, width)
    fc_out, q_out, k_out, v_out = by_rows(
        [fc_grad, q_grad, k_grad, v_grad],
        [(hidden_part, hidden)] + [(live, width)] * 3,
        per,
        me_part,
        parts,
    )
    out_rows = out_grad.reshape(cols, width)[:live]
    from_left = lax.ppermute(out_rows[live - near :], "fsdp", [(i, i + 1) for i in range(parts - 1)])
    out_rows = lax.dynamic_slice_in_dim(
        jnp.concatenate([from_left, out_rows]), near - me_part * (live - quarter), quarter, 0
    ).astype(F32)
    return (
        outputs,
        input_grad,
        q_out,
        k_out,
        v_out,
        out_rows,
        fc_out,
        proj_grad.reshape(hidden_part, width).astype(F32),
        small_grads[0],
        small_grads[1],
        small_grads[2],
        small_grads[3],
        small_grads[6],
        small_grads[4],
        small_grads[5],
        small_grads[8:].reshape(-1),
        small_grads[7],
    )


def solution(mesh):
    tokens = P("fsdp", "ctx", None)
    matrix = P("fsdp", None)
    vector = P("fsdp")
    return jax.shard_map(
        on_device,
        mesh=mesh,
        in_specs=(tokens, tokens) + (matrix,) * 6 + (vector,) * 9,
        out_specs=(tokens, tokens) + (matrix,) * 6 + (vector,) * 9,
        check_vma=False,
    )
```

```python
import functools

import jax
import jax.numpy as jnp
from jax import lax
from jax.experimental import pallas as pl
from jax.experimental.pallas import tpu as pltpu
from jax.sharding import PartitionSpec as P

HEADS = 25
HEAD = 64
EPS = 1e-05
SCALE = 0.125
NEGATIVE = -1000000000.0
ROOT = 0.7978845608028654
CUBIC = 0.044715
LANES = 128
F32 = jnp.float32
BF16 = jnp.bfloat16


def normalize(values):
    centre = jnp.mean(values, axis=-1, keepdims=True)
    centred = values - centre
    spread = jnp.mean(centred * centred, axis=-1, keepdims=True)
    inv_std = lax.rsqrt(spread + EPS)
    return (centred * inv_std, inv_std)


def norm_back(grad_norm, gain, normal, inv_std):
    scaled = grad_norm * gain
    return inv_std * (
        scaled
        - jnp.mean(scaled, axis=-1, keepdims=True)
        - normal * jnp.mean(scaled * normal, axis=-1, keepdims=True)
    )


def gelu_both(values):
    tangent = jnp.tanh(ROOT * (values + CUBIC * values * values * values))
    value = 0.5 * values * (1.0 + tangent)
    slope = 0.5 * (1.0 + tangent) + 0.5 * values * (1.0 - tangent * tangent) * ROOT * (
        1.0 + 3.0 * CUBIC * values * values
    )
    return value, slope


def dot(left, right):
    return jnp.dot(left, right, preferred_element_type=F32)


def dot_nt(left, right):
    return lax.dot_general(left, right, (((1,), (1,)), ((), ())), preferred_element_type=F32)


def dot_tn(left, right):
    return lax.dot_general(left, right, (((0,), (0,)), ((), ())), preferred_element_type=F32)


def lane_half(shape, half):
    lane = lax.broadcasted_iota(jnp.int32, shape, 1)
    return (lane < HEAD) if half == 0 else (lane >= HEAD)


def keep_half(array, half):
    return jnp.where(lane_half(array.shape, half), array, jnp.zeros_like(array))


def causal_tail(scores, first_row, block):
    keys = lax.broadcasted_iota(jnp.int32, scores.shape, 0) + first_row
    queries = lax.broadcasted_iota(jnp.int32, scores.shape, 1)
    return jnp.where(keys <= queries, scores, NEGATIVE)


def attend_kernel(block, heads, q_ref, k_ref, v_ref, o_ref, ot_ref, lse_ref):
    length = q_ref.shape[0]
    pair = pl.program_id(0)
    v_t = jnp.transpose(v_ref[...].astype(F32)).astype(BF16)

    def one_head(half):
        for index in range(length // block):
            rows = slice(index * block, (index + 1) * block)
            count = (index + 1) * block
            query = keep_half(q_ref[rows, :], half) * jnp.asarray(SCALE, BF16)
            scores = dot_nt(k_ref[:count, :], query)
            scores = causal_tail(scores, -index * block, block)
            top = jnp.max(scores, axis=0, keepdims=True)
            weights = jnp.exp(scores - top)
            total = jnp.sum(weights, axis=0, keepdims=True)
            lse_ref[0, half : half + 1, rows] = top + jnp.log(total)
            weights = weights * (1.0 / total)
            ot = dot(v_t[half * HEAD : (half + 1) * HEAD, :count], weights.astype(BF16))
            ot_ref[0, half * HEAD : (half + 1) * HEAD, rows] = ot

    one_head(0)

    @pl.when(2 * pair + 1 < heads)
    def _():
        one_head(1)

    @pl.when(2 * pair + 1 >= heads)
    def _():
        ot_ref[0, HEAD:, :] = jnp.zeros((HEAD, length), F32)
        lse_ref[0, 1:2, :] = jnp.zeros((1, length), F32)

    o_ref[...] = jnp.transpose(ot_ref[0]).astype(BF16)


def attend(queries, keys, values, heads):
    length, width = queries.shape
    pairs = width // LANES
    block = min(256, length)
    column = pl.BlockSpec((length, LANES), lambda p: (0, p))
    return pl.pallas_call(
        functools.partial(attend_kernel, block, heads),
        grid=(pairs,),
        in_specs=[column] * 3,
        out_specs=[
            column,
            pl.BlockSpec((1, LANES, length), lambda p: (p, 0, 0)),
            pl.BlockSpec((1, 2, length), lambda p: (p, 0, 0)),
        ],
        out_shape=[
            jax.ShapeDtypeStruct((length, width), BF16),
            jax.ShapeDtypeStruct((pairs, LANES, length), F32),
            jax.ShapeDtypeStruct((pairs, 2, length), F32),
        ],
        name="attend",
    )(queries, keys, values)


def attend_back_kernel(
    block, heads, q_ref, k_ref, v_ref, do_ref, ot_ref, lse_ref, dq_ref, dk_ref, dv_ref, dk_sum, dv_sum
):
    length = q_ref.shape[0]
    pair = pl.program_id(0)
    k_t = jnp.transpose(k_ref[...].astype(F32)).astype(BF16)
    do_t = jnp.transpose(do_ref[...].astype(F32))
    dk_sum[...] = jnp.zeros_like(dk_sum)
    dv_sum[...] = jnp.zeros_like(dv_sum)
    dq_ref[...] = jnp.zeros_like(dq_ref)

    def one_head(half):
        span = slice(half * HEAD, (half + 1) * HEAD)
        shared = jnp.sum(do_t[span, :] * ot_ref[0, span, :], axis=0, keepdims=True)
        for index in range(length // block):
            rows = slice(index * block, (index + 1) * block)
            count = (index + 1) * block
            query = keep_half(q_ref[rows, :], half) * jnp.asarray(SCALE, BF16)
            grad = keep_half(do_ref[rows, :], half)
            scores = dot_nt(k_ref[:count, :], query)
            scores = causal_tail(scores, -index * block, block)
            probs = jnp.exp(scores - lse_ref[0, half : half + 1, rows])
            grad_probs = dot_nt(v_ref[:count, :], grad)
            grad_scores = (probs * (grad_probs - shared[:, rows])).astype(BF16)
            dv_sum[:count, :] += dot(probs.astype(BF16), grad)
            dk_sum[:count, :] += dot(grad_scores, query)
            dq_t = dot(k_t[span, :count], grad_scores) * SCALE
            pad = jnp.zeros_like(dq_t)
            both = jnp.concatenate([dq_t, pad] if half == 0 else [pad, dq_t], axis=0)
            dq_ref[rows, :] = dq_ref[rows, :] + jnp.transpose(both).astype(BF16)

    one_head(0)

    @pl.when(2 * pair + 1 < heads)
    def _():
        one_head(1)

    dk_ref[...] = dk_sum[...].astype(BF16)
    dv_ref[...] = dv_sum[...].astype(BF16)


def attend_back(queries, keys, values, grad, ot, lse, heads):
    length, width = queries.shape
    pairs = width // LANES
    block = min(256, length)
    column = pl.BlockSpec((length, LANES), lambda p: (0, p))
    return pl.pallas_call(
        functools.partial(attend_back_kernel, block, heads),
        grid=(pairs,),
        in_specs=[column] * 4
        + [
            pl.BlockSpec((1, LANES, length), lambda p: (p, 0, 0)),
            pl.BlockSpec((1, 2, length), lambda p: (p, 0, 0)),
        ],
        out_specs=[column] * 3,
        out_shape=[jax.ShapeDtypeStruct((length, width), BF16)] * 3,
        scratch_shapes=[pltpu.VMEM((length, LANES), F32)] * 2,
        name="attend_back",
    )(queries, keys, values, grad, ot, lse)


class Place:
    def __init__(self):
        self.parts = lax.axis_size("fsdp")
        self.n_ctx = lax.axis_size("ctx")
        self.part = lax.axis_index("fsdp")
        self.ctx = lax.axis_index("ctx")
        self.beside = self.part + 1 - 2 * (self.part % 2)
        self.far = (self.part + 2) % self.parts
        self.diagonal = (self.beside + 2) % self.parts

    def at(self, position):
        n = self.n_ctx
        position = (position + 2 * n) % n
        upper = position // (n // 2)
        return (1 - upper) * 2 * position + upper * (2 * (n - 1 - position) + 1)

    @property
    def position(self):
        odd = self.ctx % 2
        return (1 - odd) * (self.ctx // 2) + odd * (self.n_ctx - 1 - self.ctx // 2)


def like(shape, dtype):
    return jax.ShapeDtypeStruct(shape, dtype)


def remote(source, target, send, recv, **where):
    return pltpu.make_async_remote_copy(
        src_ref=source,
        dst_ref=target,
        send_sem=send,
        recv_sem=recv,
        device_id=where,
        device_id_type=pl.DeviceIdType.MESH,
    )


def cut(rows):
    step = 64 if rows % 64 == 0 else rows
    return [slice(start, start + step) for start in range(0, rows, step)]


class Gather:
    reach = ("fsdp",)

    def __init__(self, array):
        self.ins = [array]
        self.parts = lax.axis_size("fsdp")
        self.pieces = cut(array.shape[0])
        self.outs = [jax.ShapeDtypeStruct((self.parts, *array.shape), array.dtype)]
        self.scratch = [pltpu.SemaphoreType.DMA((3, len(self.pieces)))] * 2

    def phases(self, place, ins, outs, scratch):
        (source,), (out,), (send, recv) = ins, outs, scratch
        count = range(len(self.pieces))

        def copy(kind, k, index, target):
            piece = self.pieces[k]
            start = source.at[piece] if kind < 2 else out.at[index, piece]
            return remote(start, out.at[index, piece], send.at[kind, k], recv.at[kind, k], fsdp=target)

        def first():
            for k in count:
                copy(1, k, place.part, place.far).start()
            for k in count:
                copy(0, k, place.part, place.beside).start()
            out[place.part] = source[...]

        def second():
            for k in count:
                copy(1, k, place.far, place.far).wait_recv()
                copy(2, k, place.far, place.beside).start()

        def third():
            for k in count:
                copy(0, k, place.beside, place.beside).wait_recv()
                copy(2, k, place.diagonal, place.beside).wait_recv()
            for k in count:
                copy(0, k, place.part, place.beside).wait_send()
                copy(1, k, place.part, place.far).wait_send()
                copy(2, k, place.far, place.beside).wait_send()

        return [first, second, third]


class Scatter:
    reach = ("fsdp",)

    def __init__(self, array):
        parts, rows, columns = array.shape
        self.ins = [array]
        self.pieces = cut(rows)
        self.outs = [jax.ShapeDtypeStruct((rows, columns), F32)]
        self.scratch = [pltpu.VMEM((rows, columns), array.dtype)] * 3
        self.scratch += [pltpu.SemaphoreType.DMA((3, len(self.pieces)))] * 2

    def phases(self, place, ins, outs, scratch):
        (source,), (out,) = ins, outs
        for_far, for_own, from_far, send, recv = scratch
        count = range(len(self.pieces))

        def copy(kind, k):
            piece = self.pieces[k]
            start, target, where = [
                (source.at[place.diagonal, piece], for_far, place.beside),
                (source.at[place.beside, piece], for_own, place.beside),
                (for_far.at[piece], from_far, place.far),
            ][kind]
            return remote(start, target.at[piece], send.at[kind, k], recv.at[kind, k], fsdp=where)

        def first():
            for k in count:
                copy(0, k).start()
            for k in count:
                copy(1, k).start()

        def second():
            for k in count:
                piece = self.pieces[k]
                copy(0, k).wait_recv()
                total = for_far[piece].astype(F32) + source[place.far, piece].astype(F32)
                for_far[piece] = total.astype(for_far.dtype)
                copy(2, k).start()

        def third():
            for k in count:
                piece = self.pieces[k]
                copy(1, k).wait_recv()
                out[piece] = for_own[piece].astype(F32) + source[place.part, piece].astype(F32)

        def fourth():
            for k in count:
                piece = self.pieces[k]
                copy(2, k).wait_recv()
                out[piece] += from_far[piece].astype(F32)
            for k in count:
                for kind in range(3):
                    copy(kind, k).wait_send()

        return [first, second, third, fourth]


class ToHeads:
    reach = ("ctx",)

    def __init__(self, arrays):
        seqs, _, half, columns = arrays[0].shape
        self.n = lax.axis_size("ctx")
        self.groups = self.n // seqs
        self.piece = columns // self.groups
        self.ins = list(arrays)
        self.outs = [jax.ShapeDtypeStruct((2 * self.n, half, self.piece), a.dtype) for a in arrays]
        self.scratch = [pltpu.SemaphoreType.DMA((len(arrays), 2, self.n))] * 2

    def whole(self, ref, other, half):
        if self.groups == 1:
            return ref.at[other, half]
        column = pl.multiple_of((other % self.groups) * self.piece, LANES)
        return ref.at[other // self.groups, half, :, pl.ds(column, self.piece)]

    def block(self, ref, other, half):
        return ref.at[other if half == 0 else 2 * self.n - 1 - other]

    def source(self, ref, other, half):
        return self.whole(ref, other, half)

    def target(self, ref, other, half):
        return self.block(ref, other, half)

    def phases(self, place, ins, outs, scratch):
        send, recv = scratch
        n, me = self.n, place.ctx
        every = [(i, half) for i in range(len(ins)) for half in range(2)]

        def begin(i):
            def start(step, _):
                other = (me + step) % n
                for half in range(2):
                    remote(
                        self.source(ins[i], other, half),
                        self.target(outs[i], me, half),
                        send.at[i, half, step],
                        recv.at[i, half, step],
                        ctx=other,
                    ).start()
                return 0

            lax.fori_loop(1, n, start, 0)
            for half in range(2):
                self.target(outs[i], me, half)[...] = self.source(ins[i], me, half)[...]

        def first():
            def start(step, _):
                other = (me + step) % n
                for i, half in every:
                    remote(
                        self.source(ins[i], other, half),
                        self.target(outs[i], me, half),
                        send.at[i, half, step],
                        recv.at[i, half, step],
                        ctx=other,
                    ).start()
                return 0

            lax.fori_loop(1, n, start, 0)
            for i, half in every:
                self.target(outs[i], me, half)[...] = self.source(ins[i], me, half)[...]

        self.begin = begin

        def second():
            def end(step, _):
                other = (me + n - step) % n
                for i, half in every:
                    copy = remote(
                        self.source(ins[i], other, half),
                        self.target(outs[i], other, half),
                        send.at[i, half, step],
                        recv.at[i, half, step],
                        ctx=other,
                    )
                    copy.wait_recv()
                    copy.wait_send()
                return 0

            lax.fori_loop(1, n, end, 0)

        return [first, second]


class FromHeads(ToHeads):
    def __init__(self, arrays, seqs):
        blocks, half, piece = arrays[0].shape
        self.n = blocks // 2
        self.groups = self.n // seqs
        self.piece = piece
        self.ins = list(arrays)
        shape = (seqs, 2, half, piece * self.groups)
        self.outs = [jax.ShapeDtypeStruct(shape, a.dtype) for a in arrays]
        self.scratch = [pltpu.SemaphoreType.DMA((len(arrays), 2, self.n))] * 2

    def source(self, ref, other, half):
        return self.block(ref, other, half)

    def target(self, ref, other, half):
        return self.whole(ref, other, half)


class Swap:
    reach = ("fsdp",)

    def __init__(self, arrays, live, wide):
        self.parts = lax.axis_size("fsdp")
        self.live, self.wide = live, wide
        self.ins = list(arrays)
        rows = arrays[0].shape[0]
        shape = (len(arrays), self.parts, rows, wide)
        self.outs = [jax.ShapeDtypeStruct(shape[1:], arrays[0].dtype)] * len(arrays)
        self.scratch = [pltpu.VMEM(shape, arrays[0].dtype)]
        self.scratch += [pltpu.SemaphoreType.DMA((len(arrays), self.parts))] * 2

    def phases(self, place, ins, outs, scratch):
        stage, send, recv = scratch
        parts, live = self.parts, self.live
        every = [(i, step) for step in (2, 3, 1) for i in range(len(ins))]

        def copy(i, step, index):
            other = (place.part + step) % parts
            return remote(
                stage.at[i, other], outs[i].at[index], send.at[i, step], recv.at[i, step], fsdp=other
            )

        def first():
            for i, ref in enumerate(ins):
                for part in range(parts):
                    start = part * live
                    stop = min(start + live, ref.shape[1])
                    stage[i, part, :, : stop - start] = ref[:, start:stop]
                    if stop - start < self.wide:
                        shape = (ref.shape[0], self.wide - stop + start)
                        stage[i, part, :, stop - start :] = jnp.zeros(shape, ref.dtype)
            for i, step in every:
                copy(i, step, place.part).start()
            for i in range(len(ins)):
                outs[i][place.part] = stage[i, place.part]

        def second():
            for i, step in every:
                copy(i, step, (place.part + parts - step) % parts).wait_recv()
                copy(i, step, place.part).wait_send()

        return [first, second]


class Window:
    reach = ("fsdp",)

    def __init__(self, array, live, wide):
        self.parts = lax.axis_size("fsdp")
        self.quarter, columns = array.shape
        self.live, self.wide = live, wide
        self.near = (live - self.quarter) * self.parts
        self.ins = [array]
        self.outs = [jax.ShapeDtypeStruct((wide, columns), array.dtype)]
        self.scratch = [pltpu.VMEM((self.quarter + self.near, columns), array.dtype)]
        self.scratch += [pltpu.SemaphoreType.DMA] * 2

    def phases(self, place, ins, outs, scratch):
        (source,), (out,), (both, send, recv) = ins, outs, scratch
        left = (place.part + self.parts - 1) % self.parts
        copy = remote(
            source.at[: self.near], both.at[self.quarter :], send, recv, fsdp=left
        )

        def first():
            copy.start()
            both[: self.quarter] = source[...]

        def second():
            copy.wait()
            start = pl.multiple_of(place.part * (self.live - self.quarter), 16)
            rows = both[pl.ds(start, self.live), :]
            index = lax.broadcasted_iota(jnp.int32, rows.shape, 0) + place.part * self.live
            inside = index < self.quarter * self.parts
            out[: self.live] = jnp.where(inside, rows, jnp.zeros_like(rows))
            if self.wide > self.live:
                out[self.live :] = jnp.zeros((self.wide - self.live, rows.shape[1]), rows.dtype)

        return [first, second]


class Total:
    reach = ("ctx",)

    def __init__(self, array):
        self.n = lax.axis_size("ctx")
        self.ins = [array]
        self.outs = [jax.ShapeDtypeStruct(array.shape, F32)]
        self.scratch = [pltpu.VMEM((self.n, *array.shape), array.dtype)]
        self.scratch += [pltpu.SemaphoreType.DMA((self.n,))] * 2

    def phases(self, place, ins, outs, scratch):
        (source,), (out,), (held, send, recv) = ins, outs, scratch
        n, me = self.n, place.ctx

        def copy(step, index):
            return remote(source, held.at[index], send.at[step], recv.at[step], ctx=(me + step) % n)

        def first():
            lax.fori_loop(1, n, lambda step, _: (copy(step, me).start(), 0)[1], 0)
            held[me] = source[...]

        def last():
            def end(step, _):
                copy(step, (me + n - step) % n).wait_recv()
                copy(step, me).wait_send()
                return 0

            lax.fori_loop(1, n, end, 0)
            total = held[0].astype(F32)
            for i in range(1, n):
                total = total + held[i].astype(F32)
            out[...] = total

        return [first, last]


class Ring:
    reach = ("ring", "fsdp")

    def __init__(self, products):
        self.n = n = lax.axis_size("ctx")
        self.parts = lax.axis_size("fsdp")
        self.per = n // self.parts
        self.products, self.streams, lefts = [], [], []
        self.ins, self.outs, slots, local, turned = [], [], [], [], []
        for left, right, heights, crossing in products:
            rows, columns = left.shape[1] // n, right.shape[1]
            known = [k for k, other in enumerate(lefts) if other is left]
            if not known:
                lefts.append(left)
                turned.append(pltpu.VMEM((n, rows, left.shape[0]), left.dtype))
            index = len(self.products)
            self.products.append((known[0] if known else len(lefts) - 1, crossing))
            self.ins.append(right)
            self.outs.append(like((n, rows, columns), BF16))
            slots.append(pltpu.VMEM((n - 1, rows, columns), BF16))
            local.append(pltpu.VMEM((2, rows, columns), BF16))
            start = 0
            for direction, count in zip((1, -1), heights):
                if count:
                    self.streams.append((index, slice(start, start + count), direction))
                start += count
        self.streams.sort(key=lambda stream: not self.products[stream[0]][1])
        self.counts = (len(lefts), len(products))
        self.ins = lefts + self.ins
        self.spaces = [pl.ANY] * len(self.outs)
        self.scratch = turned + slots + local
        self.scratch += [pltpu.SemaphoreType.DMA((len(self.streams), 2, n))] * 2

    def phases(self, place, ins, outs, scratch):
        n_left, n_product = self.counts
        lefts, rights = ins[:n_left], ins[n_left:]
        turned, scratch = scratch[:n_left], scratch[n_left:]
        slots, scratch = scratch[:n_product], scratch[n_product:]
        local, (send, recv) = scratch[:n_product], scratch[n_product:]
        n, parts, per, here = self.n, self.parts, self.per, place.position
        shift = place.ctx // per
        owner = (place.part + shift) % parts

        def make(step):
            for stream, (index, part, direction) in enumerate(self.streams):
                slab = place.at(here - direction * (step + 1))
                if crosses(stream):
                    slab = (slab + per * place.part) % n
                left = turned[self.products[index][0]]
                own = dot(left[slab, part], rights[index][...])
                local[index][step % 2, part] = own.astype(BF16)

        def way(stream):
            return self.streams[stream][2]

        def crosses(stream):
            return self.products[self.streams[stream][0]][1]

        def reducing(stream, step):
            index, part, _ = self.streams[stream]
            source = local[index].at[0] if step == 0 else slots[index].at[step - 1]
            return remote(
                source.at[part],
                slots[index].at[step, part],
                send.at[stream, 0, step],
                recv.at[stream, 0, step],
                ctx=place.at(here + way(stream)),
            )

        def last(stream):
            index, part, _ = self.streams[stream]
            return slots[index].at[n - 2, part]

        def mine(stream):
            index, part, _ = self.streams[stream]
            return outs[index].at[place.ctx, part]

        def crossing(stream):
            return remote(
                last(stream),
                mine(stream),
                send.at[stream, 0, n - 1],
                recv.at[stream, 0, n - 1],
                fsdp=owner,
            )

        def keeping(stream):
            return pltpu.make_async_copy(last(stream), mine(stream), send.at[stream, 0, n - 1])

        def gathering(stream, step, back=0):
            index, part, _ = self.streams[stream]
            slab = place.at(here - way(stream) * (step + back))
            block = outs[index].at[slab, part]
            source = block
            if step == 0 and back == 0 and not crosses(stream):
                source = last(stream)
            return remote(
                source,
                block,
                send.at[stream, 1, step],
                recv.at[stream, 1, step],
                ctx=place.at(here + way(stream)),
            )

        every = range(len(self.streams))

        def begin():
            for left, target in zip(lefts, turned):
                rows = target.shape[1]
                for k in range(n):
                    target[k] = jnp.transpose(left[:, k * rows : (k + 1) * rows])
            make(0)
            for stream in every:
                reducing(stream, 0).start()
            make(1)

        def add(stream, step):
            index, part, _ = self.streams[stream]
            reducing(stream, step).wait_recv()
            total = slots[index][step, part].astype(F32)
            total = total + local[index][(step + 1) % 2, part].astype(F32)
            slots[index][step, part] = total.astype(BF16)

        def reduce(step):
            for stream in every:
                add(stream, step - 1)
                reducing(stream, step).start()
            if step == 1:
                for stream in every:
                    reducing(stream, 0).wait_send()
            make(step + 1)

        def turn():
            for stream in every:
                add(stream, n - 2)
                if not crosses(stream):
                    gathering(stream, 0).start()
                    keeping(stream).start()
                    continue

                @pl.when(shift == 0)
                def _():
                    keeping(stream).start()

                @pl.when(shift != 0)
                def _():
                    crossing(stream).start()

        def launch(stream):
            @pl.when(shift == 0)
            def _():
                keeping(stream).wait()

            @pl.when(shift != 0)
            def _():
                crossing(stream).wait()

            gathering(stream, 0).start()

        def forward(turn):
            for stream in [s for s in every if not crosses(s)] + [s for s in every if crosses(s)]:
                step = turn - 1 if crosses(stream) else turn
                if step == 0:
                    launch(stream)
                elif step < n - 1:
                    gathering(stream, step - 1, 1).wait_recv()
                    gathering(stream, step).start()

        def end():
            for stream in every:
                gathering(stream, n - 2, 1).wait_recv()
            for stream in every:
                if not crosses(stream):
                    keeping(stream).wait()
                for step in range(n - 1):
                    if step:
                        reducing(stream, step).wait_send()
                    gathering(stream, step).wait_send()

        steps = [begin]
        steps += [functools.partial(reduce, step) for step in range(1, n - 1)]
        steps += [turn]
        steps += [functools.partial(forward, step) for step in range(1, n)]
        return steps + [end]


def exchange_kernel(transfers, places, *refs):
    refs = list(refs)
    inputs = refs[: max(places) + 1]
    refs = [inputs[index] for index in places] + refs[len(inputs) :]

    def take(lists):
        taken = []
        for items in lists:
            taken.append(refs[: len(items)])
            del refs[: len(items)]
        return taken

    ins = take([t.ins for t in transfers])
    outs = take([t.outs for t in transfers])
    scratch = take([t.scratch for t in transfers])
    place = Place()
    reach = {name for t in transfers for name in t.reach}
    peers = []
    if "fsdp" in reach:
        peers += [dict(fsdp=(place.part + k) % place.parts) for k in range(1, place.parts)]
    if "ctx" in reach:
        peers += [dict(ctx=(place.ctx + k) % place.n_ctx) for k in range(1, place.n_ctx)]
    if "ring" in reach:
        peers += [dict(ctx=place.at(place.position + k)) for k in (1, -1)]
    barrier = pltpu.get_barrier_semaphore()
    for peer in peers:
        pl.semaphore_signal(barrier, inc=1, device_id=peer, device_id_type=pl.DeviceIdType.MESH)
    pl.semaphore_wait(barrier, len(peers))
    lists = [t.phases(place, *each) for t, *each in zip(transfers, ins, outs, scratch)]
    for index in range(max(map(len, lists))):
        for phases in lists:
            if index < len(phases):
                phases[index]()


def exchange(number, name, *transfers):
    memory = pl.BlockSpec(memory_space=pltpu.VMEM)
    ins, places = [], []
    for array in [a for t in transfers for a in t.ins]:
        known = [k for k, other in enumerate(ins) if other is array]
        places.append(known[0] if known else len(ins))
        if not known:
            ins.append(array)
    outs = [a for t in transfers for a in t.outs]
    spaces = []
    for t in transfers:
        spaces += getattr(t, "spaces", [pltpu.VMEM] * len(t.outs))
    results = pl.pallas_call(
        functools.partial(exchange_kernel, transfers, places),
        out_shape=outs,
        in_specs=[memory] * len(ins),
        out_specs=[pl.BlockSpec(memory_space=space) for space in spaces],
        scratch_shapes=[s for t in transfers for s in t.scratch],
        compiler_params=pltpu.CompilerParams(collective_id=number, has_side_effects=True),
        name=name,
    )(*ins)
    results = list(results)
    split = []
    for t in transfers:
        split.append(results[: len(t.outs)])
        del results[: len(t.outs)]
    return split


def share(transfer, place, refs, ins, outs):
    count = len(transfer.scratch)
    taken = refs[:count]
    del refs[:count]
    return transfer.phases(place, ins, outs, taken)


def quarter_rows(place_index, own):
    return pl.ds(pl.multiple_of(place_index * own, own), own)


def scattered(place, partial, part, scatter_phases):
    first, second, third, fourth = scatter_phases

    def fill(index):
        part[index] = partial(index).astype(part.dtype)

    def begin():
        fill(place.diagonal)
        fill(place.beside)
        first()

    def middle():
        fill(place.far)
        second()

    def later():
        fill(place.part)
        third()

    return [begin, middle, later, fourth]


class Middle:
    reach = ("fsdp", "ctx")

    def __init__(self, blocks, seqs, out_w, x_full, vectors):
        own, width = x_full.shape
        parts = lax.axis_size("fsdp")
        self.own, self.parts = own, parts
        self.heads = FromHeads([blocks], seqs)
        self.scatter = Scatter(like((parts, own, width), BF16))
        self.gather = Gather(like((own, width), BF16))
        self.ins = [blocks, out_w, x_full, vectors]
        self.outs = [
            self.heads.outs[0],
            like((own, width), F32),
            like((own, width), F32),
            like((own, 1), F32),
            self.gather.outs[0],
        ]
        self.scratch = [
            pltpu.VMEM((parts, own, width), BF16),
            pltpu.VMEM((own, width), F32),
            pltpu.VMEM((own, width), BF16),
        ]
        for transfer in (self.heads, self.scatter, self.gather):
            self.scratch += transfer.scratch

    def phases(self, place, ins, outs, scratch):
        blocks, out_w, x_full, vectors = ins
        attended, resid, hat, inv, normed_all = outs
        part, branch, normed, *rest = scratch
        heads = share(self.heads, place, rest, [blocks], [attended])
        scatter = share(self.scatter, place, rest, [part], [branch])
        gather = share(self.gather, place, rest, [normed], [normed_all])
        seqs, _, half, cols = attended.shape
        group = seqs // self.parts

        def partial(index):
            rows = attended[pl.ds(index * group, group)].reshape(self.own, cols)
            return dot(rows, out_w[...])

        def norm():
            total = x_full[...] + branch[...] + vectors[0:1]
            resid[...] = total
            hat[...], inv[...] = normalize(total)
            normed[...] = (hat[...] * vectors[1:2] + vectors[2:3]).astype(BF16)

        return heads + scattered(place, partial, part, scatter) + [norm] + gather


class Product:
    reach = ("fsdp",)

    def __init__(self, left, right, own):
        parts, width = lax.axis_size("fsdp"), right.shape[1]
        self.own = own
        self.scatter = Scatter(like((parts, own, width), BF16))
        self.ins = [left, right]
        self.outs = [like((own, width), F32)]
        self.scratch = [pltpu.VMEM((parts, own, width), BF16), *self.scatter.scratch]

    def phases(self, place, ins, outs, scratch):
        left, right = ins
        part, *rest = scratch
        scatter = share(self.scatter, place, rest, [part], outs)

        def partial(index):
            return dot(left[quarter_rows(index, self.own), :], right[...])

        return scattered(place, partial, part, scatter)


class SecondBack:
    reach = ("fsdp",)

    def __init__(self, grad_pre, fc, hat, inv, gain, grad_y, out_w):
        own, width = hat.shape
        parts = lax.axis_size("fsdp")
        self.own, self.parts = own, parts
        self.scatter = Scatter(like((parts, own, width), BF16))
        self.gather = Gather(like((own, width), BF16))
        self.ins = [grad_pre, fc, hat, inv, gain, grad_y, out_w]
        self.outs = [
            like((own, width), F32),
            self.gather.outs[0],
            like((parts * own, out_w.shape[0]), BF16),
            like((4, width), F32),
        ]
        self.scratch = [
            pltpu.VMEM((parts, own, width), BF16),
            pltpu.VMEM((own, width), F32),
            pltpu.VMEM((own, width), BF16),
        ]
        for transfer in (self.scatter, self.gather):
            self.scratch += transfer.scratch

    def phases(self, place, ins, outs, scratch):
        grad_pre, fc, hat, inv, gain, grad_y, out_w = ins
        resid, branch_all, attended, sums = outs
        part, norm_grad, branch, *rest = scratch
        scatter = share(self.scatter, place, rest, [part], [norm_grad])
        gather = share(self.gather, place, rest, [branch], [branch_all])
        own = self.own

        def partial(index):
            return dot_nt(grad_pre[quarter_rows(index, own), :], fc[...])

        def norm():
            given = grad_y[...].astype(F32)
            total = given + norm_back(norm_grad[...], gain[...], hat[...], inv[...])
            resid[...] = total
            branch[...] = total.astype(BF16)
            sums[0:1] = jnp.sum(norm_grad[...] * hat[...], axis=0, keepdims=True)
            sums[1:2] = jnp.sum(norm_grad[...], axis=0, keepdims=True)
            sums[2:3] = jnp.sum(branch[...].astype(F32), axis=0, keepdims=True)
            sums[3:4] = jnp.sum(given, axis=0, keepdims=True)

        def project():
            for index in range(self.parts):
                rows = dot_nt(branch_all[index], out_w[...])
                attended[index * own : (index + 1) * own] = rows.astype(BF16)

        return scattered(place, partial, part, scatter) + [norm] + gather + [project]


class FirstBack:
    reach = ("fsdp", "ctx")

    def __init__(self, grads, weights, hat, inv, gain, resid, rest, bias_fc):
        own, width = hat.shape
        parts = lax.axis_size("fsdp")
        self.own, self.parts, self.count = own, parts, len(grads)
        quarter = width // parts
        lines = rest.shape[0] + 2
        self.scatter = Scatter(like((parts, own, width), BF16))
        self.small = Scatter(like((parts, lines, quarter), F32))
        self.total = Total(like((lines + bias_fc.shape[0], quarter), F32))
        self.ins = [*grads, *weights, hat, inv, gain, resid, rest, bias_fc]
        self.outs = [like((own, width), F32), self.total.outs[0]]
        self.scratch = [
            pltpu.VMEM((parts, own, width), BF16),
            pltpu.VMEM((own, width), F32),
            pltpu.VMEM((lines, width), F32),
            pltpu.VMEM((parts, lines, quarter), F32),
            pltpu.VMEM((lines, quarter), F32),
            pltpu.VMEM((lines + bias_fc.shape[0], quarter), F32),
        ]
        for transfer in (self.scatter, self.small, self.total):
            self.scratch += transfer.scratch

    def phases(self, place, ins, outs, scratch):
        grads, weights = ins[: self.count], ins[self.count : 2 * self.count]
        hat, inv, gain, resid, others, bias_fc = ins[2 * self.count :]
        input_grad, totals = outs
        part, norm_grad, lines, small, small_sum, packed, *rest = scratch
        scatter = share(self.scatter, place, rest, [part], [norm_grad])
        small_scatter = share(self.small, place, rest, [small], [small_sum])
        total = share(self.total, place, rest, [packed], [totals])
        quarter = small.shape[2]
        count = lines.shape[0]

        def partial(index):
            rows = quarter_rows(index, self.own)
            return sum(dot_nt(grad[rows, :], weight[...]) for grad, weight in zip(grads, weights))

        def norm():
            input_grad[...] = resid[...] + norm_back(norm_grad[...], gain[...], hat[...], inv[...])
            lines[0:1] = jnp.sum(norm_grad[...] * hat[...], axis=0, keepdims=True)
            lines[1:2] = jnp.sum(norm_grad[...], axis=0, keepdims=True)
            lines[2:] = others[...]
            for index in range(self.parts):
                small[index] = lines[:, index * quarter : (index + 1) * quarter]

        def pack():
            packed[:count] = small_sum[...]
            packed[count:] = bias_fc[...]
            total[0]()

        phases = scattered(place, partial, part, scatter) + [norm] + small_scatter
        return phases + [pack, total[1]]


class Later:
    def __init__(self, transfer, *steps):
        self.transfer, self.steps = transfer, steps
        self.reach = transfer.reach
        self.ins, self.outs, self.scratch = transfer.ins, transfer.outs, transfer.scratch

    def phases(self, place, ins, outs, scratch):
        phases = [lambda: None] * (self.steps[-1] + 1)
        for step, phase in zip(self.steps, self.transfer.phases(place, ins, outs, scratch)):
            phases[step] = phase
        return phases


class Spread:
    reach = ("fsdp", "ring")

    def __init__(self, arrays, live, wide):
        self.n = lax.axis_size("ctx")
        self.parts = lax.axis_size("fsdp")
        self.live, self.wide = live, wide
        self.across = wide // LANES
        self.down = self.n // self.across
        self.rows = arrays[0].shape[0] // self.down
        self.ins = list(arrays)
        shape = (self.parts, self.down, self.rows, wide)
        self.outs = [like(shape, a.dtype) for a in arrays]
        self.scratch = [pltpu.VMEM(shape, a.dtype) for a in arrays]
        self.scratch += [pltpu.SemaphoreType.DMA((len(arrays), self.parts + self.n))] * 2

    @staticmethod
    def fits(rows, wide):
        across = wide // LANES
        n = lax.axis_size("ctx")
        return n % across == 0 and rows % (n // across) == 0 and rows // (n // across) % 8 == 0

    def phases(self, place, ins, outs, scratch):
        stages, (send, recv) = scratch[:-2], scratch[-2:]
        n, parts, here = self.n, self.parts, place.position
        every = range(len(ins))

        def of(ctx):
            column = pl.multiple_of(ctx % self.across * LANES, LANES)
            return (ctx // self.across, slice(None), pl.ds(column, LANES))

        def piece(i, step, index):
            other = (place.part + step) % parts
            mine = of(place.ctx)
            return remote(
                stages[i].at[(other, *mine)],
                outs[i].at[(index, *mine)],
                send.at[i, step],
                recv.at[i, step],
                fsdp=other,
            )

        def passing(i, step, back=0):
            direction = 1 - 2 * (i % 2)
            block = outs[i].at[(slice(None), *of(place.at(here - direction * (step + back))))]
            return remote(
                block,
                block,
                send.at[i, parts + step],
                recv.at[i, parts + step],
                ctx=place.at(here + direction),
            )

        def first():
            for i in every:
                for part in range(parts):
                    start = part * self.live
                    stop = min(start + self.live, ins[i].shape[1])
                    for half in range(self.down):
                        rows = slice(half * self.rows, (half + 1) * self.rows)
                        block = ins[i][rows, start:stop]
                        stages[i][part, half, :, : stop - start] = block
                        if stop - start < self.wide:
                            zeros = jnp.zeros((self.rows, self.wide - stop + start), block.dtype)
                            stages[i][part, half, :, stop - start :] = zeros
                for step in (2, 3, 1):
                    piece(i, step, place.part).start()
                mine = of(place.ctx)
                outs[i][(place.part, *mine)] = stages[i][(place.part, *mine)]

        def turn():
            for i in every:
                for step in (1, 2, 3):
                    piece(i, step, (place.part + parts - step) % parts).wait_recv()
                passing(i, 0).start()

        def forward(step):
            for i in every:
                passing(i, step - 1, 1).wait_recv()
                passing(i, step).start()

        def end():
            for i in every:
                passing(i, n - 2, 1).wait_recv()
            for i in every:
                for step in (1, 2, 3):
                    piece(i, step, place.part).wait_send()
                for step in range(n - 1):
                    passing(i, step).wait_send()

        return [first, turn] + [functools.partial(forward, s) for s in range(1, n - 1)] + [end]


class First:
    reach = ("fsdp", "ctx", "ring")

    def __init__(self, inputs, vectors, weights, live, cols, seqs):
        own, width = inputs.shape
        self.parts = parts = lax.axis_size("fsdp")
        self.n = lax.axis_size("ctx")
        self.own, self.live, self.count = own, live, len(vectors)
        quarter = width // parts
        self.spread = Spread(weights[1:], live, cols) if Spread.fits(quarter, cols) else None
        self.swap = Swap(weights[:1] if self.spread else weights, live, cols)
        self.small = Gather(like((len(vectors), quarter), BF16))
        self.gather = Gather(like((own, width), BF16))
        token = like((seqs, 2, own // (seqs // parts) // 2, cols), BF16)
        self.heads = ToHeads([token] * 3)
        self.ins = [inputs, *vectors, *weights]
        self.outs = [
            *[like((width, cols), BF16)] * 3,
            like((own, width), F32),
            like((own, 1), F32),
            self.gather.outs[0],
            like((len(vectors), width), F32),
            *self.heads.outs,
        ]
        self.scratch = [
            pltpu.VMEM((len(vectors), quarter), BF16),
            pltpu.VMEM((parts, len(vectors), quarter), BF16),
            pltpu.VMEM((own, width), BF16),
            pltpu.VMEM((2, cols), F32),
        ]
        self.scratch += [pltpu.VMEM(token.shape, BF16)] * 3
        self.moved = [*self.swap.outs, *(self.spread.outs if self.spread else [])]
        self.scratch += [pltpu.VMEM(out.shape, BF16) for out in self.moved]
        for transfer in (self.swap, self.small, self.gather, self.heads):
            self.scratch += transfer.scratch
        if self.spread:
            self.scratch += self.spread.scratch

    def phases(self, place, ins, outs, scratch):
        inputs, vectors, weights = ins[0], ins[1 : 1 + self.count], ins[1 + self.count :]
        qkv, (hat, inv, normed_all, full), heads_out = outs[:3], outs[3:7], outs[7:]
        small_own, small_all, normed, bias, *rest = scratch
        tokens, rest = rest[:3], rest[3:]
        moved, rest = rest[:3], rest[3:]
        swapped = moved[: len(self.swap.outs)]
        swap = share(self.swap, place, rest, weights[: len(swapped)], swapped)
        small = share(self.small, place, rest, [small_own], [small_all])
        gather = share(self.gather, place, rest, [normed], [normed_all])
        heads = share(self.heads, place, rest, tokens, heads_out)
        begin_heads = self.heads.begin
        spread = []
        if self.spread:
            spread = share(self.spread, place, rest, weights[1:], moved[1:])
        parts, live, own = self.parts, self.live, self.own
        quarter = small_own.shape[1]
        group = tokens[0].shape[0] // parts

        def begin():
            for index, vector in enumerate(vectors):
                small_own[index : index + 1] = vector[...].reshape(1, quarter)
            small[0]()
            if spread:
                spread[0]()
            swap[0]()
            hat[...], inv[...] = normalize(inputs[...].astype(F32))

        def norm():
            small[1]()
            small[2]()
            for part in range(parts):
                full[:, part * quarter : (part + 1) * quarter] = small_all[part].astype(F32)
            normed[...] = (hat[...] * full[0:1] + full[1:2]).astype(BF16)
            gather[0]()
            bias[...] = jnp.zeros_like(bias)
            for part in range(parts):

                @pl.when(place.part == part)
                def _():
                    stop = min(live, full.shape[1] - part * live)
                    bias[:, :stop] = full[2:4, part * live : part * live + stop]

        def arrive():
            gather[1]()
            gather[2]()
            swap[1]()

        def unpack(i):
            source, target = moved[i], qkv[i]
            if len(source.shape) == 3:
                rows = source.shape[1]
                for part in range(parts):
                    target[part * rows : (part + 1) * rows] = source[part]
                return
            _, down, rows, _ = source.shape
            for part in range(parts):
                for half in range(down):
                    start = (part * down + half) * rows
                    target[start : start + rows] = source[part, half]

        def project(i):
            unpack(i)
            for part in range(parts):
                rows = dot(normed_all[part], qkv[i][...])
                if i != 1:
                    rows = rows + bias[i // 2 : i // 2 + 1]
                shape = (group, *tokens[i].shape[1:])
                tokens[i][part * group : (part + 1) * group] = rows.astype(BF16).reshape(shape)
            begin_heads(i)

        phases = [begin, norm] + spread[1:] + [arrive]
        self.ready = len(phases)
        return phases + [functools.partial(project, i) for i in range(3)] + [heads[1]]


def results_kernel(widths, parts, order_ref, *refs):
    for index, (live, total) in enumerate(widths):
        out = refs[len(widths) * parts + index]
        for part in range(parts):
            stop = min((part + 1) * live, total)
            block = refs[index * parts + part][0, :, : stop - part * live]
            out[:, part * live : stop] = block.astype(F32)


def by_rows(arrays, widths, per, part, parts):
    slabs, rows, _ = arrays[0].shape
    order = (part - jnp.arange(parts, dtype=jnp.int32) + parts) % parts
    if rows % 8:
        outs = []
        for array, (live, total) in zip(arrays, widths):
            array = jnp.take(array.reshape(parts, per, rows, -1), order, axis=0)[..., :live]
            array = jnp.transpose(array, (1, 2, 0, 3)).reshape(per * rows, parts * live)
            outs.append(array[:, :total].astype(F32))
        return outs
    step = 40 if rows % 40 == 0 else rows
    inner = rows // step

    def source(column, array):
        return pl.BlockSpec(
            (1, step, array.shape[2]),
            lambda i, order: (order[column] * per + i // inner, i % inner, 0),
        )

    return pl.pallas_call(
        functools.partial(results_kernel, widths, parts),
        out_shape=[jax.ShapeDtypeStruct((per * rows, total), F32) for _, total in widths],
        grid_spec=pltpu.PrefetchScalarGridSpec(
            num_scalar_prefetch=1,
            grid=(per * inner,),
            in_specs=[source(column, array) for array in arrays for column in range(parts)],
            out_specs=[pl.BlockSpec((step, total), lambda i, order: (i, 0)) for _, total in widths],
        ),
        name="by_rows",
    )(order, *[array for array in arrays for _ in range(parts)])


def on_device(
    inputs,
    cotangent,
    w_query,
    w_key,
    w_value,
    w_out,
    w_fc,
    w_proj,
    ln1_gain,
    ln1_bias,
    query_bias,
    value_bias,
    out_bias,
    ln2_gain,
    ln2_bias,
    fc_bias,
    proj_bias,
):
    parts = lax.axis_size("fsdp")
    n_ctx = lax.axis_size("ctx")
    me_part = lax.axis_index("fsdp")
    seqs, rows, width = inputs.shape
    hidden = w_fc.shape[1]
    quarter = width // parts
    hidden_part = hidden // parts
    own = seqs * rows
    all_seqs = seqs * parts
    tokens = all_seqs * rows
    length = rows * n_ctx
    half_rows = rows // 2
    groups = n_ctx // all_seqs
    heads_part = -(-HEADS // parts)
    live = heads_part * HEAD
    slots = -(-heads_part // (2 * groups)) * 2 * groups
    cols = slots * HEAD
    piece = cols // groups
    heads_here = heads_part if groups == 1 else slots // groups
    near = (live - quarter) * parts
    per = n_ctx // parts
    slab = width // n_ctx

    def by_sequences(array):
        return array.reshape(all_seqs, 2, half_rows, cols)

    def split(rows, more):
        low = (rows // 2 + 7 * more) // 8 * 8
        return (low, rows - low)

    x_full = inputs.astype(F32).reshape(own, width)
    vectors = [ln1_gain, ln1_bias, query_bias, value_bias, out_bias, ln2_gain, ln2_bias, proj_bias]
    first = First(
        inputs.reshape(own, width),
        vectors,
        [w_query, w_key, w_value],
        live,
        cols,
        all_seqs,
    )
    steps = 3 + (n_ctx if first.spread else 0)
    (*qkv, hat_one, inv_one, normed_one, full, q_heads, k_heads, v_heads), (fc,), (out_w,) = exchange(
        0,
        "first",
        first,
        Later(Swap([w_fc], hidden_part, hidden_part), steps, steps + 3),
        Later(Window(w_out, live, cols), steps, steps + 3),
    )
    gain_one, gain_two, bias_proj = full[0], full[5], full[7]
    bias_fc = fc_bias.astype(F32)
    normed_one = normed_one.reshape(tokens, width)
    fc = fc.reshape(width, hidden_part)
    proj = w_proj
    heads = [q_heads, k_heads, v_heads]

    q_seq, k_seq, v_seq = [a.reshape(length, piece) for a in heads]
    o_seq, ot, lse = attend(q_seq, k_seq, v_seq, heads_here)

    def blocks(array):
        return array.reshape(2 * n_ctx, half_rows, piece)

    (attended, resid, hat_two, inv_two, normed_two), (grad_y,) = exchange(
        2,
        "middle",
        Middle(blocks(o_seq), all_seqs, out_w, x_full, full[4:7]),
        Gather(cotangent.reshape(own, width)),
    )
    attended = attended.reshape(tokens, cols)
    normed_two = normed_two.reshape(tokens, width)
    grad_y = grad_y.reshape(tokens, width)

    pre_act = dot(normed_two, fc) + bias_fc
    value, slope = gelu_both(pre_act)
    activated = value.astype(BF16)

    grad_pre = (dot_nt(grad_y, proj) * slope).astype(BF16)
    grad_bias_fc = jnp.sum(grad_pre.astype(F32), axis=0)
    (proj_grad, fc_grad), (grad_resid, grad_branch, grad_attended, sums_two) = exchange(
        3,
        "wide_grads",
        Ring(
            [
                (activated, grad_y, split(slab, 1), False),
                (normed_two, grad_pre, split(slab, 0), True),
            ]
        ),
        SecondBack(
            grad_pre, fc, hat_two, inv_two, gain_two[None], cotangent.reshape(own, width), out_w
        ),
    )
    grad_branch = grad_branch.reshape(tokens, width)

    ((grad_heads,),) = exchange(4, "to_heads_back", ToHeads([by_sequences(grad_attended)]))
    dq_seq, dk_seq, dv_seq = attend_back(
        q_seq, k_seq, v_seq, grad_heads.reshape(length, piece), ot, lse, heads_here
    )
    grad_qkv, (mlp,) = exchange(
        5,
        "from_heads_back",
        Later(FromHeads([blocks(a) for a in (dq_seq, dk_seq, dv_seq)], all_seqs), 0, 4),
        Product(activated, proj, own),
    )
    outputs = (resid + mlp + bias_proj).astype(BF16).reshape(seqs, rows, width)
    grad_qkv = [a.reshape(tokens, cols) for a in grad_qkv]
    grad_bias_query = jnp.sum(grad_qkv[0].astype(F32), axis=0)
    grad_bias_value = jnp.sum(grad_qkv[2].astype(F32), axis=0)

    def window(vector):
        whole = jnp.zeros((parts * live,), F32)
        return lax.dynamic_update_slice_in_dim(whole, vector[:live], me_part * live, 0)[:width]

    small_grads = jnp.concatenate(
        [window(grad_bias_query)[None], window(grad_bias_value)[None], sums_two]
    )

    (out_grad, q_grad, k_grad, v_grad), (input_grad, small_grads) = exchange(
        6,
        "narrow_grads",
        Ring(
            [
                (attended, grad_branch, split(cols // n_ctx, 0), False),
                (normed_one, grad_qkv[0], (slab, 0), True),
                (normed_one, grad_qkv[1], (0, slab), True),
                (normed_one, grad_qkv[2], split(slab, 1), True),
            ]
        ),
        FirstBack(
            grad_qkv,
            qkv,
            hat_one,
            inv_one,
            gain_one[None],
            grad_resid,
            small_grads,
            grad_bias_fc.reshape(-1, quarter),
        ),
    )
    input_grad = input_grad.reshape(seqs, rows, width)
    fc_out, q_out, k_out, v_out = by_rows(
        [fc_grad, q_grad, k_grad, v_grad],
        [(hidden_part, hidden)] + [(live, width)] * 3,
        per,
        me_part,
        parts,
    )
    out_rows = out_grad.reshape(cols, width)[:live]
    from_left = lax.ppermute(out_rows[live - near :], "fsdp", [(i, i + 1) for i in range(parts - 1)])
    out_rows = lax.dynamic_slice_in_dim(
        jnp.concatenate([from_left, out_rows]), near - me_part * (live - quarter), quarter, 0
    ).astype(F32)
    return (
        outputs,
        input_grad,
        q_out,
        k_out,
        v_out,
        out_rows,
        fc_out,
        proj_grad.reshape(hidden_part, width).astype(F32),
        small_grads[0],
        small_grads[1],
        small_grads[2],
        small_grads[3],
        small_grads[6],
        small_grads[4],
        small_grads[5],
        small_grads[8:].reshape(-1),
        small_grads[7],
    )


def solution(mesh):
    tokens = P("fsdp", "ctx", None)
    matrix = P("fsdp", None)
    vector = P("fsdp")
    return jax.shard_map(
        on_device,
        mesh=mesh,
        in_specs=(tokens, tokens) + (matrix,) * 6 + (vector,) * 9,
        out_specs=(tokens, tokens) + (matrix,) * 6 + (vector,) * 9,
        check_vma=False,
    )
```

```python
import functools

import jax
import jax.numpy as jnp
from jax import lax
from jax.experimental import pallas as pl
from jax.experimental.pallas import tpu as pltpu
from jax.sharding import PartitionSpec as P

HEADS = 25
HEAD = 64
EPS = 1e-05
SCALE = 0.125
NEGATIVE = -1000000000.0
ROOT = 0.7978845608028654
CUBIC = 0.044715
LANES = 128
F32 = jnp.float32
BF16 = jnp.bfloat16


def normalize(values):
    centre = jnp.mean(values, axis=-1, keepdims=True)
    centred = values - centre
    spread = jnp.mean(centred * centred, axis=-1, keepdims=True)
    inv_std = lax.rsqrt(spread + EPS)
    return (centred * inv_std, inv_std)


def norm_back(grad_norm, gain, normal, inv_std):
    scaled = grad_norm * gain
    return inv_std * (
        scaled
        - jnp.mean(scaled, axis=-1, keepdims=True)
        - normal * jnp.mean(scaled * normal, axis=-1, keepdims=True)
    )


def gelu_both(values):
    tangent = jnp.tanh(ROOT * (values + CUBIC * values * values * values))
    value = 0.5 * values * (1.0 + tangent)
    slope = 0.5 * (1.0 + tangent) + 0.5 * values * (1.0 - tangent * tangent) * ROOT * (
        1.0 + 3.0 * CUBIC * values * values
    )
    return value, slope


def dot(left, right):
    return jnp.dot(left, right, preferred_element_type=F32)


def dot_nt(left, right):
    return lax.dot_general(left, right, (((1,), (1,)), ((), ())), preferred_element_type=F32)


def dot_tn(left, right):
    return lax.dot_general(left, right, (((0,), (0,)), ((), ())), preferred_element_type=F32)


def lane_half(shape, half):
    lane = lax.broadcasted_iota(jnp.int32, shape, 1)
    return (lane < HEAD) if half == 0 else (lane >= HEAD)


def keep_half(array, half):
    return jnp.where(lane_half(array.shape, half), array, jnp.zeros_like(array))


def causal_tail(scores, first_row, block):
    keys = lax.broadcasted_iota(jnp.int32, scores.shape, 0) + first_row
    queries = lax.broadcasted_iota(jnp.int32, scores.shape, 1)
    return jnp.where(keys <= queries, scores, NEGATIVE)


def attend_pair(block, heads, pair, q_ref, k_ref, v_ref, o_ref, ot_ref, lse_ref):
    length = q_ref.shape[0]
    v_t = jnp.transpose(v_ref[...].astype(F32)).astype(BF16)

    def one_head(half):
        for index in range(length // block):
            rows = slice(index * block, (index + 1) * block)
            count = (index + 1) * block
            query = keep_half(q_ref[rows, :], half) * jnp.asarray(SCALE, BF16)
            scores = dot_nt(k_ref[:count, :], query)
            scores = causal_tail(scores, -index * block, block)
            top = jnp.max(scores, axis=0, keepdims=True)
            weights = jnp.exp(scores - top)
            total = jnp.sum(weights, axis=0, keepdims=True)
            lse_ref[0, half : half + 1, rows] = top + jnp.log(total)
            weights = weights * (1.0 / total)
            ot = dot(v_t[half * HEAD : (half + 1) * HEAD, :count], weights.astype(BF16))
            ot_ref[0, half * HEAD : (half + 1) * HEAD, rows] = ot

    one_head(0)

    @pl.when(2 * pair + 1 < heads)
    def _():
        one_head(1)

    @pl.when(2 * pair + 1 >= heads)
    def _():
        ot_ref[0, HEAD:, :] = jnp.zeros((HEAD, length), F32)
        lse_ref[0, 1:2, :] = jnp.zeros((1, length), F32)

    o_ref[...] = jnp.transpose(ot_ref[0]).astype(BF16)


def attend_back_pair(
    block, heads, pair, q_ref, k_ref, v_ref, do_ref, ot_ref, lse_ref, dq_ref, dk_ref, dv_ref, dk_sum, dv_sum
):
    length = q_ref.shape[0]
    k_t = jnp.transpose(k_ref[...].astype(F32)).astype(BF16)
    do_t = jnp.transpose(do_ref[...].astype(F32))
    dk_sum[...] = jnp.zeros_like(dk_sum)
    dv_sum[...] = jnp.zeros_like(dv_sum)
    dq_ref[...] = jnp.zeros_like(dq_ref)

    def one_head(half):
        span = slice(half * HEAD, (half + 1) * HEAD)
        shared = jnp.sum(do_t[span, :] * ot_ref[0, span, :], axis=0, keepdims=True)
        for index in range(length // block):
            rows = slice(index * block, (index + 1) * block)
            count = (index + 1) * block
            query = keep_half(q_ref[rows, :], half) * jnp.asarray(SCALE, BF16)
            grad = keep_half(do_ref[rows, :], half)
            scores = dot_nt(k_ref[:count, :], query)
            scores = causal_tail(scores, -index * block, block)
            probs = jnp.exp(scores - lse_ref[0, half : half + 1, rows])
            grad_probs = dot_nt(v_ref[:count, :], grad)
            grad_scores = (probs * (grad_probs - shared[:, rows])).astype(BF16)
            dv_sum[:count, :] += dot(probs.astype(BF16), grad)
            dk_sum[:count, :] += dot(grad_scores, query)
            dq_t = dot(k_t[span, :count], grad_scores) * SCALE
            pad = jnp.zeros_like(dq_t)
            both = jnp.concatenate([dq_t, pad] if half == 0 else [pad, dq_t], axis=0)
            dq_ref[rows, :] = dq_ref[rows, :] + jnp.transpose(both).astype(BF16)

    one_head(0)

    @pl.when(2 * pair + 1 < heads)
    def _():
        one_head(1)

    dk_ref[...] = dk_sum[...].astype(BF16)
    dv_ref[...] = dv_sum[...].astype(BF16)


class Place:
    def __init__(self):
        self.parts = lax.axis_size("fsdp")
        self.n_ctx = lax.axis_size("ctx")
        self.part = lax.axis_index("fsdp")
        self.ctx = lax.axis_index("ctx")
        self.beside = self.part + 1 - 2 * (self.part % 2)
        self.far = (self.part + 2) % self.parts
        self.diagonal = (self.beside + 2) % self.parts

    def at(self, position):
        n = self.n_ctx
        position = (position + 2 * n) % n
        upper = position // (n // 2)
        return (1 - upper) * 2 * position + upper * (2 * (n - 1 - position) + 1)

    @property
    def position(self):
        odd = self.ctx % 2
        return (1 - odd) * (self.ctx // 2) + odd * (self.n_ctx - 1 - self.ctx // 2)


def like(shape, dtype):
    return jax.ShapeDtypeStruct(shape, dtype)


def remote(source, target, send, recv, **where):
    return pltpu.make_async_remote_copy(
        src_ref=source,
        dst_ref=target,
        send_sem=send,
        recv_sem=recv,
        device_id=where,
        device_id_type=pl.DeviceIdType.MESH,
    )


def cut(rows):
    step = 64 if rows % 64 == 0 else rows
    return [slice(start, start + step) for start in range(0, rows, step)]


class Gather:
    reach = ("fsdp",)

    def __init__(self, array):
        self.ins = [array]
        self.parts = lax.axis_size("fsdp")
        self.pieces = cut(array.shape[0])
        self.outs = [jax.ShapeDtypeStruct((self.parts, *array.shape), array.dtype)]
        self.scratch = [pltpu.SemaphoreType.DMA((3, len(self.pieces)))] * 2

    def phases(self, place, ins, outs, scratch):
        (source,), (out,), (send, recv) = ins, outs, scratch
        count = range(len(self.pieces))

        def copy(kind, k, index, target):
            piece = self.pieces[k]
            start = source.at[piece] if kind < 2 else out.at[index, piece]
            return remote(start, out.at[index, piece], send.at[kind, k], recv.at[kind, k], fsdp=target)

        def first():
            for k in count:
                copy(1, k, place.part, place.far).start()
            for k in count:
                copy(0, k, place.part, place.beside).start()
            out[place.part] = source[...]

        def second():
            for k in count:
                copy(1, k, place.far, place.far).wait_recv()
                copy(2, k, place.far, place.beside).start()

        def third():
            for k in count:
                copy(0, k, place.beside, place.beside).wait_recv()
                copy(2, k, place.diagonal, place.beside).wait_recv()
            for k in count:
                copy(0, k, place.part, place.beside).wait_send()
                copy(1, k, place.part, place.far).wait_send()
                copy(2, k, place.far, place.beside).wait_send()

        return [first, second, third]


class Scatter:
    reach = ("fsdp",)

    def __init__(self, array):
        parts, rows, columns = array.shape
        self.ins = [array]
        self.pieces = cut(rows)
        self.outs = [jax.ShapeDtypeStruct((rows, columns), F32)]
        self.scratch = [pltpu.VMEM((rows, columns), array.dtype)] * 3
        self.scratch += [pltpu.SemaphoreType.DMA((3, len(self.pieces)))] * 2

    def phases(self, place, ins, outs, scratch):
        (source,), (out,) = ins, outs
        for_far, for_own, from_far, send, recv = scratch
        count = range(len(self.pieces))

        def copy(kind, k):
            piece = self.pieces[k]
            start, target, where = [
                (source.at[place.diagonal, piece], for_far, place.beside),
                (source.at[place.beside, piece], for_own, place.beside),
                (for_far.at[piece], from_far, place.far),
            ][kind]
            return remote(start, target.at[piece], send.at[kind, k], recv.at[kind, k], fsdp=where)

        def first():
            for k in count:
                copy(0, k).start()
            for k in count:
                copy(1, k).start()

        def second():
            for k in count:
                piece = self.pieces[k]
                copy(0, k).wait_recv()
                total = for_far[piece].astype(F32) + source[place.far, piece].astype(F32)
                for_far[piece] = total.astype(for_far.dtype)
                copy(2, k).start()

        def third():
            for k in count:
                piece = self.pieces[k]
                copy(1, k).wait_recv()
                out[piece] = for_own[piece].astype(F32) + source[place.part, piece].astype(F32)

        def fourth():
            for k in count:
                piece = self.pieces[k]
                copy(2, k).wait_recv()
                out[piece] += from_far[piece].astype(F32)
            for k in count:
                for kind in range(3):
                    copy(kind, k).wait_send()

        return [first, second, third, fourth]


class ToHeads:
    reach = ("ctx",)

    def __init__(self, arrays):
        seqs, _, half, columns = arrays[0].shape
        self.n = lax.axis_size("ctx")
        self.groups = self.n // seqs
        self.piece = columns // self.groups
        self.ins = list(arrays)
        self.outs = [jax.ShapeDtypeStruct((2 * self.n, half, self.piece), a.dtype) for a in arrays]
        self.scratch = [pltpu.SemaphoreType.DMA((len(arrays), 2, self.n))] * 2

    def whole(self, ref, other, half):
        if self.groups == 1:
            return ref.at[other, half]
        column = pl.multiple_of((other % self.groups) * self.piece, LANES)
        return ref.at[other // self.groups, half, :, pl.ds(column, self.piece)]

    def block(self, ref, other, half):
        return ref.at[other if half == 0 else 2 * self.n - 1 - other]

    def source(self, ref, other, half):
        return self.whole(ref, other, half)

    def target(self, ref, other, half):
        return self.block(ref, other, half)

    def phases(self, place, ins, outs, scratch):
        send, recv = scratch
        n, me = self.n, place.ctx
        every = [(i, half) for i in range(len(ins)) for half in range(2)]

        def begin(i):
            def start(step, _):
                other = (me + step) % n
                for half in range(2):
                    remote(
                        self.source(ins[i], other, half),
                        self.target(outs[i], me, half),
                        send.at[i, half, step],
                        recv.at[i, half, step],
                        ctx=other,
                    ).start()
                return 0

            lax.fori_loop(1, n, start, 0)
            for half in range(2):
                self.target(outs[i], me, half)[...] = self.source(ins[i], me, half)[...]

        def first():
            def start(step, _):
                other = (me + step) % n
                for i, half in every:
                    remote(
                        self.source(ins[i], other, half),
                        self.target(outs[i], me, half),
                        send.at[i, half, step],
                        recv.at[i, half, step],
                        ctx=other,
                    ).start()
                return 0

            lax.fori_loop(1, n, start, 0)
            for i, half in every:
                self.target(outs[i], me, half)[...] = self.source(ins[i], me, half)[...]

        self.begin = begin

        def second():
            def end(step, _):
                other = (me + n - step) % n
                for i, half in every:
                    copy = remote(
                        self.source(ins[i], other, half),
                        self.target(outs[i], other, half),
                        send.at[i, half, step],
                        recv.at[i, half, step],
                        ctx=other,
                    )
                    copy.wait_recv()
                    copy.wait_send()
                return 0

            lax.fori_loop(1, n, end, 0)

        return [first, second]


class Swap:
    reach = ("fsdp",)

    def __init__(self, arrays, live, wide):
        self.parts = lax.axis_size("fsdp")
        self.live, self.wide = live, wide
        self.ins = list(arrays)
        rows = arrays[0].shape[0]
        shape = (len(arrays), self.parts, rows, wide)
        self.outs = [jax.ShapeDtypeStruct(shape[1:], arrays[0].dtype)] * len(arrays)
        self.scratch = [pltpu.VMEM(shape, arrays[0].dtype)]
        self.scratch += [pltpu.SemaphoreType.DMA((len(arrays), self.parts))] * 2

    def phases(self, place, ins, outs, scratch):
        stage, send, recv = scratch
        parts, live = self.parts, self.live
        every = [(i, step) for step in (2, 3, 1) for i in range(len(ins))]

        def copy(i, step, index):
            other = (place.part + step) % parts
            return remote(
                stage.at[i, other], outs[i].at[index], send.at[i, step], recv.at[i, step], fsdp=other
            )

        def first():
            for i, ref in enumerate(ins):
                for part in range(parts):
                    start = part * live
                    stop = min(start + live, ref.shape[1])
                    stage[i, part, :, : stop - start] = ref[:, start:stop]
                    if stop - start < self.wide:
                        shape = (ref.shape[0], self.wide - stop + start)
                        stage[i, part, :, stop - start :] = jnp.zeros(shape, ref.dtype)
            for i, step in every:
                copy(i, step, place.part).start()
            for i in range(len(ins)):
                outs[i][place.part] = stage[i, place.part]

        def second():
            for i, step in every:
                copy(i, step, (place.part + parts - step) % parts).wait_recv()
                copy(i, step, place.part).wait_send()

        return [first, second]


class Window:
    reach = ("fsdp",)

    def __init__(self, array, live, wide):
        self.parts = lax.axis_size("fsdp")
        self.quarter, columns = array.shape
        self.live, self.wide = live, wide
        self.near = (live - self.quarter) * self.parts
        self.ins = [array]
        self.outs = [jax.ShapeDtypeStruct((wide, columns), array.dtype)]
        self.scratch = [pltpu.VMEM((self.quarter + self.near, columns), array.dtype)]
        self.scratch += [pltpu.SemaphoreType.DMA] * 2

    def phases(self, place, ins, outs, scratch):
        (source,), (out,), (both, send, recv) = ins, outs, scratch
        left = (place.part + self.parts - 1) % self.parts
        copy = remote(
            source.at[: self.near], both.at[self.quarter :], send, recv, fsdp=left
        )

        def first():
            copy.start()
            both[: self.quarter] = source[...]

        def second():
            copy.wait()
            start = pl.multiple_of(place.part * (self.live - self.quarter), 16)
            rows = both[pl.ds(start, self.live), :]
            index = lax.broadcasted_iota(jnp.int32, rows.shape, 0) + place.part * self.live
            inside = index < self.quarter * self.parts
            out[: self.live] = jnp.where(inside, rows, jnp.zeros_like(rows))
            if self.wide > self.live:
                out[self.live :] = jnp.zeros((self.wide - self.live, rows.shape[1]), rows.dtype)

        return [first, second]


class Total:
    reach = ("ctx",)

    def __init__(self, array):
        self.n = lax.axis_size("ctx")
        self.ins = [array]
        self.outs = [jax.ShapeDtypeStruct(array.shape, F32)]
        self.scratch = [pltpu.VMEM((self.n, *array.shape), array.dtype)]
        self.scratch += [pltpu.SemaphoreType.DMA((self.n,))] * 2

    def phases(self, place, ins, outs, scratch):
        (source,), (out,), (held, send, recv) = ins, outs, scratch
        n, me = self.n, place.ctx

        def copy(step, index):
            return remote(source, held.at[index], send.at[step], recv.at[step], ctx=(me + step) % n)

        def first():
            lax.fori_loop(1, n, lambda step, _: (copy(step, me).start(), 0)[1], 0)
            held[me] = source[...]

        def last():
            def end(step, _):
                copy(step, (me + n - step) % n).wait_recv()
                copy(step, me).wait_send()
                return 0

            lax.fori_loop(1, n, end, 0)
            total = held[0].astype(F32)
            for i in range(1, n):
                total = total + held[i].astype(F32)
            out[...] = total

        return [first, last]


class Ring:
    reach = ("ring", "fsdp")

    def __init__(self, products):
        self.n = n = lax.axis_size("ctx")
        self.parts = lax.axis_size("fsdp")
        self.per = n // self.parts
        self.products, self.streams, lefts = [], [], []
        self.ins, self.outs, slots, local, turned = [], [], [], [], []
        for left, right, heights, crossing in products:
            rows, columns = left.shape[1] // n, right.shape[1]
            known = [k for k, other in enumerate(lefts) if other is left]
            if not known:
                lefts.append(left)
                turned.append(pltpu.VMEM((n, rows, left.shape[0]), left.dtype))
            index = len(self.products)
            self.products.append((known[0] if known else len(lefts) - 1, crossing))
            self.ins.append(right)
            self.outs.append(like((n, rows, columns), BF16))
            slots.append(pltpu.VMEM((n - 1, rows, columns), BF16))
            local.append(pltpu.VMEM((2, rows, columns), BF16))
            start = 0
            for direction, count in zip((1, -1), heights):
                if count:
                    self.streams.append((index, slice(start, start + count), direction))
                start += count
        self.streams.sort(key=lambda stream: not self.products[stream[0]][1])
        self.counts = (len(lefts), len(products))
        self.ins = lefts + self.ins
        self.spaces = [pl.ANY] * len(self.outs)
        self.scratch = turned + slots + local
        self.scratch += [pltpu.SemaphoreType.DMA((len(self.streams), 2, n))] * 2

    def phases(self, place, ins, outs, scratch):
        n_left, n_product = self.counts
        lefts, rights = ins[:n_left], ins[n_left:]
        turned, scratch = scratch[:n_left], scratch[n_left:]
        slots, scratch = scratch[:n_product], scratch[n_product:]
        local, (send, recv) = scratch[:n_product], scratch[n_product:]
        n, parts, per, here = self.n, self.parts, self.per, place.position
        shift = place.ctx // per
        owner = (place.part + shift) % parts

        def make(step):
            for stream, (index, part, direction) in enumerate(self.streams):
                slab = place.at(here - direction * (step + 1))
                if crosses(stream):
                    slab = (slab + per * place.part) % n
                left = turned[self.products[index][0]]
                own = dot(left[slab, part], rights[index][...])
                local[index][step % 2, part] = own.astype(BF16)

        def way(stream):
            return self.streams[stream][2]

        def crosses(stream):
            return self.products[self.streams[stream][0]][1]

        def reducing(stream, step):
            index, part, _ = self.streams[stream]
            source = local[index].at[0] if step == 0 else slots[index].at[step - 1]
            return remote(
                source.at[part],
                slots[index].at[step, part],
                send.at[stream, 0, step],
                recv.at[stream, 0, step],
                ctx=place.at(here + way(stream)),
            )

        def last(stream):
            index, part, _ = self.streams[stream]
            return slots[index].at[n - 2, part]

        def mine(stream):
            index, part, _ = self.streams[stream]
            return outs[index].at[place.ctx, part]

        def crossing(stream):
            return remote(
                last(stream),
                mine(stream),
                send.at[stream, 0, n - 1],
                recv.at[stream, 0, n - 1],
                fsdp=owner,
            )

        def keeping(stream):
            return pltpu.make_async_copy(last(stream), mine(stream), send.at[stream, 0, n - 1])

        def gathering(stream, step, back=0):
            index, part, _ = self.streams[stream]
            slab = place.at(here - way(stream) * (step + back))
            block = outs[index].at[slab, part]
            source = block
            if step == 0 and back == 0 and not crosses(stream):
                source = last(stream)
            return remote(
                source,
                block,
                send.at[stream, 1, step],
                recv.at[stream, 1, step],
                ctx=place.at(here + way(stream)),
            )

        every = range(len(self.streams))

        def begin():
            for left, target in zip(lefts, turned):
                rows = target.shape[1]
                for k in range(n):
                    target[k] = jnp.transpose(left[:, k * rows : (k + 1) * rows])
            make(0)
            for stream in every:
                reducing(stream, 0).start()
            make(1)

        def add(stream, step):
            index, part, _ = self.streams[stream]
            reducing(stream, step).wait_recv()
            total = slots[index][step, part].astype(F32)
            total = total + local[index][(step + 1) % 2, part].astype(F32)
            slots[index][step, part] = total.astype(BF16)

        def reduce(step):
            for stream in every:
                add(stream, step - 1)
                reducing(stream, step).start()
            if step == 1:
                for stream in every:
                    reducing(stream, 0).wait_send()
            make(step + 1)

        def turn():
            for stream in every:
                add(stream, n - 2)
                if not crosses(stream):
                    gathering(stream, 0).start()
                    keeping(stream).start()
                    continue

                @pl.when(shift == 0)
                def _():
                    keeping(stream).start()

                @pl.when(shift != 0)
                def _():
                    crossing(stream).start()

        def launch(stream):
            @pl.when(shift == 0)
            def _():
                keeping(stream).wait()

            @pl.when(shift != 0)
            def _():
                crossing(stream).wait()

            gathering(stream, 0).start()

        def forward(turn):
            for stream in [s for s in every if not crosses(s)] + [s for s in every if crosses(s)]:
                step = turn - 1 if crosses(stream) else turn
                if step == 0:
                    launch(stream)
                elif step < n - 1:
                    gathering(stream, step - 1, 1).wait_recv()
                    gathering(stream, step).start()

        def end():
            for stream in every:
                gathering(stream, n - 2, 1).wait_recv()
            for stream in every:
                if not crosses(stream):
                    keeping(stream).wait()
                for step in range(n - 1):
                    if step:
                        reducing(stream, step).wait_send()
                    gathering(stream, step).wait_send()

        steps = [begin]
        steps += [functools.partial(reduce, step) for step in range(1, n - 1)]
        steps += [turn]
        steps += [functools.partial(forward, step) for step in range(1, n)]
        return steps + [end]


def exchange_kernel(transfers, places, *refs):
    refs = list(refs)
    inputs = refs[: max(places) + 1]
    refs = [inputs[index] for index in places] + refs[len(inputs) :]

    def take(lists):
        taken = []
        for items in lists:
            taken.append(refs[: len(items)])
            del refs[: len(items)]
        return taken

    ins = take([t.ins for t in transfers])
    outs = take([t.outs for t in transfers])
    scratch = take([t.scratch for t in transfers])
    place = Place()
    reach = {name for t in transfers for name in t.reach}
    peers = []
    if "fsdp" in reach:
        peers += [dict(fsdp=(place.part + k) % place.parts) for k in range(1, place.parts)]
    if "ctx" in reach:
        peers += [dict(ctx=(place.ctx + k) % place.n_ctx) for k in range(1, place.n_ctx)]
    if "ring" in reach:
        peers += [dict(ctx=place.at(place.position + k)) for k in (1, -1)]
    barrier = pltpu.get_barrier_semaphore()
    for peer in peers:
        pl.semaphore_signal(barrier, inc=1, device_id=peer, device_id_type=pl.DeviceIdType.MESH)
    pl.semaphore_wait(barrier, len(peers))
    lists = [t.phases(place, *each) for t, *each in zip(transfers, ins, outs, scratch)]
    for index in range(max(map(len, lists))):
        for phases in lists:
            if index < len(phases):
                phases[index]()


def exchange(number, name, *transfers):
    memory = pl.BlockSpec(memory_space=pltpu.VMEM)
    ins, places = [], []
    for array in [a for t in transfers for a in t.ins]:
        known = [k for k, other in enumerate(ins) if other is array]
        places.append(known[0] if known else len(ins))
        if not known:
            ins.append(array)
    outs = [a for t in transfers for a in t.outs]
    spaces = []
    for t in transfers:
        spaces += getattr(t, "spaces", [pltpu.VMEM] * len(t.outs))
    results = pl.pallas_call(
        functools.partial(exchange_kernel, transfers, places),
        out_shape=outs,
        in_specs=[memory] * len(ins),
        out_specs=[pl.BlockSpec(memory_space=space) for space in spaces],
        scratch_shapes=[s for t in transfers for s in t.scratch],
        compiler_params=pltpu.CompilerParams(collective_id=number, has_side_effects=True),
        name=name,
    )(*ins)
    results = list(results)
    split = []
    for t in transfers:
        split.append(results[: len(t.outs)])
        del results[: len(t.outs)]
    return split


def share(transfer, place, refs, ins, outs):
    count = len(transfer.scratch)
    taken = refs[:count]
    del refs[:count]
    return transfer.phases(place, ins, outs, taken)


def quarter_rows(place_index, own):
    return pl.ds(pl.multiple_of(place_index * own, own), own)


def scattered(place, partial, part, scatter_phases):
    first, second, third, fourth = scatter_phases

    def fill(index):
        part[index] = partial(index).astype(part.dtype)

    def begin():
        fill(place.diagonal)
        fill(place.beside)
        first()

    def middle():
        fill(place.far)
        second()

    def later():
        fill(place.part)
        third()

    return [begin, middle, later, fourth]


class Sender:
    def __init__(self, count, seqs, half, piece):
        self.n = n = lax.axis_size("ctx")
        self.half, self.piece, self.pairs = half, piece, piece // LANES
        self.groups = n // seqs
        self.count = count
        self.outs = [like((seqs, 2, half, piece * self.groups), BF16)] * count
        self.scratch = [pltpu.VMEM((2 * n * half, piece), BF16)] * count
        self.scratch += [pltpu.SemaphoreType.DMA((count, 2, self.pairs, n))] * 2

    def bind(self, place, outs, scratch):
        held, (send, recv) = scratch[: self.count], scratch[self.count :]
        n, me, half = self.n, place.ctx, self.half
        every = [(i, side) for i in range(self.count) for side in range(2)]

        def block(ref, pair, other, side):
            index = other if side == 0 else 2 * n - 1 - other
            rows = pl.ds(pl.multiple_of(index * half, half), half)
            return ref.at[rows, pl.ds(pl.multiple_of(pair * LANES, LANES), LANES)]

        def place_of(ref, pair, other, side):
            column = pl.multiple_of(other % self.groups * self.piece + pair * LANES, LANES)
            return ref.at[other // self.groups, side, :, pl.ds(column, LANES)]

        def copy(i, side, pair, step, index):
            other = (me + step) % n
            return remote(
                block(held[i], pair, other, side),
                place_of(outs[i], pair, index, side),
                send.at[i, side, pair, step],
                recv.at[i, side, pair, step],
                ctx=other,
            )

        def begin(pair):
            def start(step, _):
                for i, side in every:
                    copy(i, side, pair, step, me).start()
                return 0

            lax.fori_loop(1, n, start, 0)
            for i, side in every:
                place_of(outs[i], pair, me, side)[...] = block(held[i], pair, me, side)[...]

        def end():
            def pair_end(pair, _):
                def step_end(step, _):
                    for i, side in every:
                        copy(i, side, pair, step, (me + n - step) % n).wait_recv()
                        copy(i, side, pair, step, me).wait_send()
                    return 0

                lax.fori_loop(1, n, step_end, 0)
                return 0

            lax.fori_loop(0, self.pairs, pair_end, 0)

        return held, begin, end


def lanes(ref, pair):
    return ref.at[:, pl.ds(pl.multiple_of(pair * LANES, LANES), LANES)]


class Attend:
    reach = ("ctx",)

    def __init__(self, queries, keys, values, heads, seqs, half):
        length, piece = queries.shape
        self.block, self.heads = min(256, length), heads
        self.sender = Sender(1, seqs, half, piece)
        pairs = self.sender.pairs
        self.ins = [queries, keys, values]
        self.outs = [
            *self.sender.outs,
            like((pairs, LANES, length), F32),
            like((pairs, 2, length), F32),
        ]
        self.scratch = self.sender.scratch

    def phases(self, place, ins, outs, scratch):
        out, ot, lse = outs
        held, begin, end = self.sender.bind(place, [out], scratch)

        def run():
            def one(pair, _):
                columns = [lanes(ref, pair) for ref in (*ins, held[0])]
                own = pl.ds(pair, 1)
                attend_pair(self.block, self.heads, pair, *columns, ot.at[own], lse.at[own])
                begin(pair)
                return 0

            lax.fori_loop(0, self.sender.pairs, one, 0)

        return [run, end]


class AttendBack:
    reach = ("ctx",)

    def __init__(self, queries, keys, values, grad, ot, lse, heads, seqs, half):
        length, piece = queries.shape
        self.block, self.heads = min(256, length), heads
        self.sender = Sender(3, seqs, half, piece)
        self.ins = [queries, keys, values, grad, ot, lse]
        self.outs = self.sender.outs
        self.scratch = [pltpu.VMEM((length, LANES), F32)] * 2 + self.sender.scratch

    def phases(self, place, ins, outs, scratch):
        *given, ot, lse = ins
        sums, scratch = scratch[:2], scratch[2:]
        held, begin, end = self.sender.bind(place, outs, scratch)

        def run():
            def one(pair, _):
                own = pl.ds(pair, 1)
                attend_back_pair(
                    self.block,
                    self.heads,
                    pair,
                    *[lanes(ref, pair) for ref in given],
                    ot.at[own],
                    lse.at[own],
                    *[lanes(ref, pair) for ref in held],
                    *sums,
                )
                begin(pair)
                return 0

            lax.fori_loop(0, self.sender.pairs, one, 0)

        return [run, end]


class Middle:
    reach = ("fsdp", "ctx")

    def __init__(self, heads, out_w, x_full, vectors):
        own, width = x_full.shape
        parts = lax.axis_size("fsdp")
        self.own, self.parts = own, parts
        self.heads = heads
        self.scatter = Scatter(like((parts, own, width), BF16))
        self.gather = Gather(like((own, width), BF16))
        self.ins = [*heads.ins, out_w, x_full, vectors]
        self.outs = [
            *heads.outs,
            like((own, width), F32),
            like((own, width), F32),
            like((own, 1), F32),
            self.gather.outs[0],
        ]
        self.scratch = [
            pltpu.VMEM((parts, own, width), BF16),
            pltpu.VMEM((own, width), F32),
            pltpu.VMEM((own, width), BF16),
        ]
        for transfer in (self.heads, self.scatter, self.gather):
            self.scratch += transfer.scratch

    def phases(self, place, ins, outs, scratch):
        *given, out_w, x_full, vectors = ins
        attended, ot, lse, resid, hat, inv, normed_all = outs
        part, branch, normed, *rest = scratch
        heads = share(self.heads, place, rest, given, [attended, ot, lse])
        scatter = share(self.scatter, place, rest, [part], [branch])
        gather = share(self.gather, place, rest, [normed], [normed_all])
        seqs, _, half, cols = attended.shape
        group = seqs // self.parts

        def partial(index):
            rows = attended[pl.ds(index * group, group)].reshape(self.own, cols)
            return dot(rows, out_w[...])

        def norm():
            total = x_full[...] + branch[...] + vectors[0:1]
            resid[...] = total
            hat[...], inv[...] = normalize(total)
            normed[...] = (hat[...] * vectors[1:2] + vectors[2:3]).astype(BF16)

        return heads + scattered(place, partial, part, scatter) + [norm] + gather


class Product:
    reach = ("fsdp",)

    def __init__(self, left, right, own):
        parts, width = lax.axis_size("fsdp"), right.shape[1]
        self.own = own
        self.scatter = Scatter(like((parts, own, width), BF16))
        self.ins = [left, right]
        self.outs = [like((own, width), F32)]
        self.scratch = [pltpu.VMEM((parts, own, width), BF16), *self.scatter.scratch]

    def phases(self, place, ins, outs, scratch):
        left, right = ins
        part, *rest = scratch
        scatter = share(self.scatter, place, rest, [part], outs)

        def partial(index):
            return dot(left[quarter_rows(index, self.own), :], right[...])

        return scattered(place, partial, part, scatter)


class SecondBack:
    reach = ("fsdp",)

    def __init__(self, grad_pre, fc, hat, inv, gain, grad_y, out_w):
        own, width = hat.shape
        parts = lax.axis_size("fsdp")
        self.own, self.parts = own, parts
        self.scatter = Scatter(like((parts, own, width), BF16))
        self.gather = Gather(like((own, width), BF16))
        self.ins = [grad_pre, fc, hat, inv, gain, grad_y, out_w]
        self.outs = [
            like((own, width), F32),
            self.gather.outs[0],
            like((parts * own, out_w.shape[0]), BF16),
            like((4, width), F32),
        ]
        self.scratch = [
            pltpu.VMEM((parts, own, width), BF16),
            pltpu.VMEM((own, width), F32),
            pltpu.VMEM((own, width), BF16),
        ]
        for transfer in (self.scatter, self.gather):
            self.scratch += transfer.scratch

    def phases(self, place, ins, outs, scratch):
        grad_pre, fc, hat, inv, gain, grad_y, out_w = ins
        resid, branch_all, attended, sums = outs
        part, norm_grad, branch, *rest = scratch
        scatter = share(self.scatter, place, rest, [part], [norm_grad])
        gather = share(self.gather, place, rest, [branch], [branch_all])
        own = self.own

        def partial(index):
            return dot_nt(grad_pre[quarter_rows(index, own), :], fc[...])

        def norm():
            given = grad_y[...].astype(F32)
            total = given + norm_back(norm_grad[...], gain[...], hat[...], inv[...])
            resid[...] = total
            branch[...] = total.astype(BF16)
            sums[0:1] = jnp.sum(norm_grad[...] * hat[...], axis=0, keepdims=True)
            sums[1:2] = jnp.sum(norm_grad[...], axis=0, keepdims=True)
            sums[2:3] = jnp.sum(branch[...].astype(F32), axis=0, keepdims=True)
            sums[3:4] = jnp.sum(given, axis=0, keepdims=True)

        def project():
            for index in range(self.parts):
                rows = dot_nt(branch_all[index], out_w[...])
                attended[index * own : (index + 1) * own] = rows.astype(BF16)

        return scattered(place, partial, part, scatter) + [norm] + gather + [project]


class FirstBack:
    reach = ("fsdp", "ctx")

    def __init__(self, grads, weights, hat, inv, gain, resid, rest, bias_fc):
        own, width = hat.shape
        parts = lax.axis_size("fsdp")
        self.own, self.parts, self.count = own, parts, len(grads)
        quarter = width // parts
        lines = rest.shape[0] + 2
        self.scatter = Scatter(like((parts, own, width), BF16))
        self.small = Scatter(like((parts, lines, quarter), F32))
        self.total = Total(like((lines + bias_fc.shape[0], quarter), F32))
        self.ins = [*grads, *weights, hat, inv, gain, resid, rest, bias_fc]
        self.outs = [like((own, width), F32), self.total.outs[0]]
        self.scratch = [
            pltpu.VMEM((parts, own, width), BF16),
            pltpu.VMEM((own, width), F32),
            pltpu.VMEM((lines, width), F32),
            pltpu.VMEM((parts, lines, quarter), F32),
            pltpu.VMEM((lines, quarter), F32),
            pltpu.VMEM((lines + bias_fc.shape[0], quarter), F32),
        ]
        for transfer in (self.scatter, self.small, self.total):
            self.scratch += transfer.scratch

    def phases(self, place, ins, outs, scratch):
        grads, weights = ins[: self.count], ins[self.count : 2 * self.count]
        hat, inv, gain, resid, others, bias_fc = ins[2 * self.count :]
        input_grad, totals = outs
        part, norm_grad, lines, small, small_sum, packed, *rest = scratch
        scatter = share(self.scatter, place, rest, [part], [norm_grad])
        small_scatter = share(self.small, place, rest, [small], [small_sum])
        total = share(self.total, place, rest, [packed], [totals])
        quarter = small.shape[2]
        count = lines.shape[0]

        def partial(index):
            rows = quarter_rows(index, self.own)
            return sum(dot_nt(grad[rows, :], weight[...]) for grad, weight in zip(grads, weights))

        def norm():
            input_grad[...] = resid[...] + norm_back(norm_grad[...], gain[...], hat[...], inv[...])
            lines[0:1] = jnp.sum(norm_grad[...] * hat[...], axis=0, keepdims=True)
            lines[1:2] = jnp.sum(norm_grad[...], axis=0, keepdims=True)
            lines[2:] = others[...]
            for index in range(self.parts):
                small[index] = lines[:, index * quarter : (index + 1) * quarter]

        def pack():
            packed[:count] = small_sum[...]
            packed[count:] = bias_fc[...]
            total[0]()

        phases = scattered(place, partial, part, scatter) + [norm] + small_scatter
        return phases + [pack, total[1]]


class Later:
    def __init__(self, transfer, *steps):
        self.transfer, self.steps = transfer, steps
        self.reach = transfer.reach
        self.ins, self.outs, self.scratch = transfer.ins, transfer.outs, transfer.scratch

    def phases(self, place, ins, outs, scratch):
        phases = [lambda: None] * (self.steps[-1] + 1)
        for step, phase in zip(self.steps, self.transfer.phases(place, ins, outs, scratch)):
            phases[step] = phase
        return phases


class Spread:
    reach = ("fsdp", "ring")

    def __init__(self, arrays, live, wide):
        self.n = lax.axis_size("ctx")
        self.parts = lax.axis_size("fsdp")
        self.live, self.wide = live, wide
        self.across = wide // LANES
        self.down = self.n // self.across
        self.rows = arrays[0].shape[0] // self.down
        self.ins = list(arrays)
        shape = (self.parts, self.down, self.rows, wide)
        self.outs = [like(shape, a.dtype) for a in arrays]
        self.scratch = [pltpu.VMEM(shape, a.dtype) for a in arrays]
        self.scratch += [pltpu.SemaphoreType.DMA((len(arrays), self.parts + self.n))] * 2

    @staticmethod
    def fits(rows, wide):
        across = wide // LANES
        n = lax.axis_size("ctx")
        return n % across == 0 and rows % (n // across) == 0 and rows // (n // across) % 8 == 0

    def phases(self, place, ins, outs, scratch):
        stages, (send, recv) = scratch[:-2], scratch[-2:]
        n, parts, here = self.n, self.parts, place.position
        every = range(len(ins))

        def of(ctx):
            column = pl.multiple_of(ctx % self.across * LANES, LANES)
            return (ctx // self.across, slice(None), pl.ds(column, LANES))

        def piece(i, step, index):
            other = (place.part + step) % parts
            mine = of(place.ctx)
            return remote(
                stages[i].at[(other, *mine)],
                outs[i].at[(index, *mine)],
                send.at[i, step],
                recv.at[i, step],
                fsdp=other,
            )

        def passing(i, step, back=0):
            direction = 1 - 2 * (i % 2)
            block = outs[i].at[(slice(None), *of(place.at(here - direction * (step + back))))]
            return remote(
                block,
                block,
                send.at[i, parts + step],
                recv.at[i, parts + step],
                ctx=place.at(here + direction),
            )

        def first():
            for i in every:
                for part in range(parts):
                    start = part * self.live
                    stop = min(start + self.live, ins[i].shape[1])
                    for half in range(self.down):
                        rows = slice(half * self.rows, (half + 1) * self.rows)
                        block = ins[i][rows, start:stop]
                        stages[i][part, half, :, : stop - start] = block
                        if stop - start < self.wide:
                            zeros = jnp.zeros((self.rows, self.wide - stop + start), block.dtype)
                            stages[i][part, half, :, stop - start :] = zeros
                for step in (2, 3, 1):
                    piece(i, step, place.part).start()
                mine = of(place.ctx)
                outs[i][(place.part, *mine)] = stages[i][(place.part, *mine)]

        def turn():
            for i in every:
                for step in (1, 2, 3):
                    piece(i, step, (place.part + parts - step) % parts).wait_recv()
                passing(i, 0).start()

        def forward(step):
            for i in every:
                passing(i, step - 1, 1).wait_recv()
                passing(i, step).start()

        def end():
            for i in every:
                passing(i, n - 2, 1).wait_recv()
            for i in every:
                for step in (1, 2, 3):
                    piece(i, step, place.part).wait_send()
                for step in range(n - 1):
                    passing(i, step).wait_send()

        return [first, turn] + [functools.partial(forward, s) for s in range(1, n - 1)] + [end]


class First:
    reach = ("fsdp", "ctx", "ring")

    def __init__(self, inputs, vectors, weights, live, cols, seqs):
        own, width = inputs.shape
        self.parts = parts = lax.axis_size("fsdp")
        self.n = lax.axis_size("ctx")
        self.own, self.live, self.count = own, live, len(vectors)
        quarter = width // parts
        self.spread = Spread(weights[1:], live, cols) if Spread.fits(quarter, cols) else None
        self.swap = Swap(weights[:1] if self.spread else weights, live, cols)
        self.small = Gather(like((len(vectors), quarter), BF16))
        self.gather = Gather(like((own, width), BF16))
        token = like((seqs, 2, own // (seqs // parts) // 2, cols), BF16)
        self.heads = ToHeads([token] * 3)
        self.ins = [inputs, *vectors, *weights]
        self.outs = [
            *[like((width, cols), BF16)] * 3,
            like((own, width), F32),
            like((own, 1), F32),
            self.gather.outs[0],
            like((len(vectors), width), F32),
            *self.heads.outs,
        ]
        self.scratch = [
            pltpu.VMEM((len(vectors), quarter), BF16),
            pltpu.VMEM((parts, len(vectors), quarter), BF16),
            pltpu.VMEM((own, width), BF16),
            pltpu.VMEM((2, cols), F32),
        ]
        self.scratch += [pltpu.VMEM(token.shape, BF16)] * 3
        self.moved = [*self.swap.outs, *(self.spread.outs if self.spread else [])]
        self.scratch += [pltpu.VMEM(out.shape, BF16) for out in self.moved]
        for transfer in (self.swap, self.small, self.gather, self.heads):
            self.scratch += transfer.scratch
        if self.spread:
            self.scratch += self.spread.scratch

    def phases(self, place, ins, outs, scratch):
        inputs, vectors, weights = ins[0], ins[1 : 1 + self.count], ins[1 + self.count :]
        qkv, (hat, inv, normed_all, full), heads_out = outs[:3], outs[3:7], outs[7:]
        small_own, small_all, normed, bias, *rest = scratch
        tokens, rest = rest[:3], rest[3:]
        moved, rest = rest[:3], rest[3:]
        swapped = moved[: len(self.swap.outs)]
        swap = share(self.swap, place, rest, weights[: len(swapped)], swapped)
        small = share(self.small, place, rest, [small_own], [small_all])
        gather = share(self.gather, place, rest, [normed], [normed_all])
        heads = share(self.heads, place, rest, tokens, heads_out)
        begin_heads = self.heads.begin
        spread = []
        if self.spread:
            spread = share(self.spread, place, rest, weights[1:], moved[1:])
        parts, live, own = self.parts, self.live, self.own
        quarter = small_own.shape[1]
        group = tokens[0].shape[0] // parts

        def begin():
            for index, vector in enumerate(vectors):
                small_own[index : index + 1] = vector[...].reshape(1, quarter)
            small[0]()
            if spread:
                spread[0]()
            swap[0]()
            hat[...], inv[...] = normalize(inputs[...].astype(F32))

        def norm():
            small[1]()
            small[2]()
            for part in range(parts):
                full[:, part * quarter : (part + 1) * quarter] = small_all[part].astype(F32)
            normed[...] = (hat[...] * full[0:1] + full[1:2]).astype(BF16)
            gather[0]()
            bias[...] = jnp.zeros_like(bias)
            for part in range(parts):

                @pl.when(place.part == part)
                def _():
                    stop = min(live, full.shape[1] - part * live)
                    bias[:, :stop] = full[2:4, part * live : part * live + stop]

        def arrive():
            gather[1]()
            gather[2]()
            swap[1]()

        def unpack(i):
            source, target = moved[i], qkv[i]
            if len(source.shape) == 3:
                rows = source.shape[1]
                for part in range(parts):
                    target[part * rows : (part + 1) * rows] = source[part]
                return
            _, down, rows, _ = source.shape
            for part in range(parts):
                for half in range(down):
                    start = (part * down + half) * rows
                    target[start : start + rows] = source[part, half]

        def project(i):
            unpack(i)
            for part in range(parts):
                rows = dot(normed_all[part], qkv[i][...])
                if i != 1:
                    rows = rows + bias[i // 2 : i // 2 + 1]
                shape = (group, *tokens[i].shape[1:])
                tokens[i][part * group : (part + 1) * group] = rows.astype(BF16).reshape(shape)
            begin_heads(i)

        phases = [begin, norm] + spread[1:] + [arrive]
        self.ready = len(phases)
        return phases + [functools.partial(project, i) for i in range(3)] + [heads[1]]


def results_kernel(widths, parts, order_ref, *refs):
    for index, (live, total) in enumerate(widths):
        out = refs[len(widths) * parts + index]
        for part in range(parts):
            stop = min((part + 1) * live, total)
            block = refs[index * parts + part][0, :, : stop - part * live]
            out[:, part * live : stop] = block.astype(F32)


def by_rows(arrays, widths, per, part, parts):
    slabs, rows, _ = arrays[0].shape
    order = (part - jnp.arange(parts, dtype=jnp.int32) + parts) % parts
    if rows % 8:
        outs = []
        for array, (live, total) in zip(arrays, widths):
            array = jnp.take(array.reshape(parts, per, rows, -1), order, axis=0)[..., :live]
            array = jnp.transpose(array, (1, 2, 0, 3)).reshape(per * rows, parts * live)
            outs.append(array[:, :total].astype(F32))
        return outs
    step = 40 if rows % 40 == 0 else rows
    inner = rows // step

    def source(column, array):
        return pl.BlockSpec(
            (1, step, array.shape[2]),
            lambda i, order: (order[column] * per + i // inner, i % inner, 0),
        )

    return pl.pallas_call(
        functools.partial(results_kernel, widths, parts),
        out_shape=[jax.ShapeDtypeStruct((per * rows, total), F32) for _, total in widths],
        grid_spec=pltpu.PrefetchScalarGridSpec(
            num_scalar_prefetch=1,
            grid=(per * inner,),
            in_specs=[source(column, array) for array in arrays for column in range(parts)],
            out_specs=[pl.BlockSpec((step, total), lambda i, order: (i, 0)) for _, total in widths],
        ),
        name="by_rows",
    )(order, *[array for array in arrays for _ in range(parts)])


def on_device(
    inputs,
    cotangent,
    w_query,
    w_key,
    w_value,
    w_out,
    w_fc,
    w_proj,
    ln1_gain,
    ln1_bias,
    query_bias,
    value_bias,
    out_bias,
    ln2_gain,
    ln2_bias,
    fc_bias,
    proj_bias,
):
    parts = lax.axis_size("fsdp")
    n_ctx = lax.axis_size("ctx")
    me_part = lax.axis_index("fsdp")
    seqs, rows, width = inputs.shape
    hidden = w_fc.shape[1]
    quarter = width // parts
    hidden_part = hidden // parts
    own = seqs * rows
    all_seqs = seqs * parts
    tokens = all_seqs * rows
    length = rows * n_ctx
    half_rows = rows // 2
    groups = n_ctx // all_seqs
    heads_part = -(-HEADS // parts)
    live = heads_part * HEAD
    slots = -(-heads_part // (2 * groups)) * 2 * groups
    cols = slots * HEAD
    piece = cols // groups
    heads_here = heads_part if groups == 1 else slots // groups
    near = (live - quarter) * parts
    per = n_ctx // parts
    slab = width // n_ctx

    def by_sequences(array):
        return array.reshape(all_seqs, 2, half_rows, cols)

    def split(rows, more):
        low = (rows // 2 + 7 * more) // 8 * 8
        return (low, rows - low)

    x_full = inputs.astype(F32).reshape(own, width)
    vectors = [ln1_gain, ln1_bias, query_bias, value_bias, out_bias, ln2_gain, ln2_bias, proj_bias]
    first = First(
        inputs.reshape(own, width),
        vectors,
        [w_query, w_key, w_value],
        live,
        cols,
        all_seqs,
    )
    steps = 3 + (n_ctx if first.spread else 0)
    (*qkv, hat_one, inv_one, normed_one, full, q_heads, k_heads, v_heads), (fc,), (out_w,) = exchange(
        0,
        "first",
        first,
        Later(Swap([w_fc], hidden_part, hidden_part), steps, steps + 3),
        Later(Window(w_out, live, cols), steps, steps + 3),
    )
    gain_one, gain_two, bias_proj = full[0], full[5], full[7]
    bias_fc = fc_bias.astype(F32)
    normed_one = normed_one.reshape(tokens, width)
    fc = fc.reshape(width, hidden_part)
    proj = w_proj
    heads = [q_heads, k_heads, v_heads]

    q_seq, k_seq, v_seq = [a.reshape(length, piece) for a in heads]
    (attended, ot, lse, resid, hat_two, inv_two, normed_two), (grad_y,) = exchange(
        2,
        "middle",
        Middle(
            Attend(q_seq, k_seq, v_seq, heads_here, all_seqs, half_rows), out_w, x_full, full[4:7]
        ),
        Gather(cotangent.reshape(own, width)),
    )
    attended = attended.reshape(tokens, cols)
    normed_two = normed_two.reshape(tokens, width)
    grad_y = grad_y.reshape(tokens, width)

    pre_act = dot(normed_two, fc) + bias_fc
    value, slope = gelu_both(pre_act)
    activated = value.astype(BF16)

    grad_pre = (dot_nt(grad_y, proj) * slope).astype(BF16)
    grad_bias_fc = jnp.sum(grad_pre.astype(F32), axis=0)
    (proj_grad, fc_grad), (grad_resid, grad_branch, grad_attended, sums_two) = exchange(
        3,
        "wide_grads",
        Ring(
            [
                (activated, grad_y, split(slab, 1), False),
                (normed_two, grad_pre, split(slab, 0), True),
            ]
        ),
        SecondBack(
            grad_pre, fc, hat_two, inv_two, gain_two[None], cotangent.reshape(own, width), out_w
        ),
    )
    grad_branch = grad_branch.reshape(tokens, width)

    ((grad_heads,),) = exchange(4, "to_heads_back", ToHeads([by_sequences(grad_attended)]))
    back = AttendBack(
        q_seq,
        k_seq,
        v_seq,
        grad_heads.reshape(length, piece),
        ot,
        lse,
        heads_here,
        all_seqs,
        half_rows,
    )
    grad_qkv, (mlp,) = exchange(
        5,
        "from_heads_back",
        Later(back, 0, 4),
        Product(activated, proj, own),
    )
    outputs = (resid + mlp + bias_proj).astype(BF16).reshape(seqs, rows, width)
    grad_qkv = [a.reshape(tokens, cols) for a in grad_qkv]
    grad_bias_query = jnp.sum(grad_qkv[0].astype(F32), axis=0)
    grad_bias_value = jnp.sum(grad_qkv[2].astype(F32), axis=0)

    def window(vector):
        whole = jnp.zeros((parts * live,), F32)
        return lax.dynamic_update_slice_in_dim(whole, vector[:live], me_part * live, 0)[:width]

    small_grads = jnp.concatenate(
        [window(grad_bias_query)[None], window(grad_bias_value)[None], sums_two]
    )

    (out_grad, q_grad, k_grad, v_grad), (input_grad, small_grads) = exchange(
        6,
        "narrow_grads",
        Ring(
            [
                (attended, grad_branch, split(cols // n_ctx, 0), False),
                (normed_one, grad_qkv[0], (slab, 0), True),
                (normed_one, grad_qkv[1], (0, slab), True),
                (normed_one, grad_qkv[2], split(slab, 1), True),
            ]
        ),
        FirstBack(
            grad_qkv,
            qkv,
            hat_one,
            inv_one,
            gain_one[None],
            grad_resid,
            small_grads,
            grad_bias_fc.reshape(-1, quarter),
        ),
    )
    input_grad = input_grad.reshape(seqs, rows, width)
    fc_out, q_out, k_out, v_out = by_rows(
        [fc_grad, q_grad, k_grad, v_grad],
        [(hidden_part, hidden)] + [(live, width)] * 3,
        per,
        me_part,
        parts,
    )
    out_rows = out_grad.reshape(cols, width)[:live]
    from_left = lax.ppermute(out_rows[live - near :], "fsdp", [(i, i + 1) for i in range(parts - 1)])
    out_rows = lax.dynamic_slice_in_dim(
        jnp.concatenate([from_left, out_rows]), near - me_part * (live - quarter), quarter, 0
    ).astype(F32)
    return (
        outputs,
        input_grad,
        q_out,
        k_out,
        v_out,
        out_rows,
        fc_out,
        proj_grad.reshape(hidden_part, width).astype(F32),
        small_grads[0],
        small_grads[1],
        small_grads[2],
        small_grads[3],
        small_grads[6],
        small_grads[4],
        small_grads[5],
        small_grads[8:].reshape(-1),
        small_grads[7],
    )


def solution(mesh):
    tokens = P("fsdp", "ctx", None)
    matrix = P("fsdp", None)
    vector = P("fsdp")
    return jax.shard_map(
        on_device,
        mesh=mesh,
        in_specs=(tokens, tokens) + (matrix,) * 6 + (vector,) * 9,
        out_specs=(tokens, tokens) + (matrix,) * 6 + (vector,) * 9,
        check_vma=False,
    )
```

```python
import functools

import jax
import jax.numpy as jnp
from jax import lax
from jax.experimental import pallas as pl
from jax.experimental.pallas import tpu as pltpu
from jax.sharding import PartitionSpec as P

HEADS = 25
HEAD = 64
EPS = 1e-05
SCALE = 0.125
NEGATIVE = -1000000000.0
ROOT = 0.7978845608028654
CUBIC = 0.044715
LANES = 128
F32 = jnp.float32
BF16 = jnp.bfloat16


def normalize(values):
    centre = jnp.mean(values, axis=-1, keepdims=True)
    centred = values - centre
    spread = jnp.mean(centred * centred, axis=-1, keepdims=True)
    inv_std = lax.rsqrt(spread + EPS)
    return (centred * inv_std, inv_std)


def norm_back(grad_norm, gain, normal, inv_std):
    scaled = grad_norm * gain
    return inv_std * (
        scaled
        - jnp.mean(scaled, axis=-1, keepdims=True)
        - normal * jnp.mean(scaled * normal, axis=-1, keepdims=True)
    )


def gelu_both(values):
    tangent = jnp.tanh(ROOT * (values + CUBIC * values * values * values))
    value = 0.5 * values * (1.0 + tangent)
    slope = 0.5 * (1.0 + tangent) + 0.5 * values * (1.0 - tangent * tangent) * ROOT * (
        1.0 + 3.0 * CUBIC * values * values
    )
    return value, slope


def dot(left, right):
    return jnp.dot(left, right, preferred_element_type=F32)


def dot_nt(left, right):
    return lax.dot_general(left, right, (((1,), (1,)), ((), ())), preferred_element_type=F32)


def dot_tn(left, right):
    return lax.dot_general(left, right, (((0,), (0,)), ((), ())), preferred_element_type=F32)


def lane_half(shape, half):
    lane = lax.broadcasted_iota(jnp.int32, shape, 1)
    return (lane < HEAD) if half == 0 else (lane >= HEAD)


def keep_half(array, half):
    return jnp.where(lane_half(array.shape, half), array, jnp.zeros_like(array))


def causal_tail(scores, first_row, block):
    keys = lax.broadcasted_iota(jnp.int32, scores.shape, 0) + first_row
    queries = lax.broadcasted_iota(jnp.int32, scores.shape, 1)
    return jnp.where(keys <= queries, scores, NEGATIVE)


def attend_pair(block, heads, pair, q_ref, k_ref, v_ref, o_ref, ot_ref, lse_ref):
    length = q_ref.shape[0]
    v_t = jnp.transpose(v_ref[...].astype(F32)).astype(BF16)

    def one_head(half):
        for index in range(length // block):
            rows = slice(index * block, (index + 1) * block)
            count = (index + 1) * block
            query = keep_half(q_ref[rows, :], half) * jnp.asarray(SCALE, BF16)
            scores = dot_nt(k_ref[:count, :], query)
            scores = causal_tail(scores, -index * block, block)
            top = jnp.max(scores, axis=0, keepdims=True)
            weights = jnp.exp(scores - top)
            total = jnp.sum(weights, axis=0, keepdims=True)
            lse_ref[0, half : half + 1, rows] = top + jnp.log(total)
            weights = weights * (1.0 / total)
            ot = dot(v_t[half * HEAD : (half + 1) * HEAD, :count], weights.astype(BF16))
            ot_ref[0, half * HEAD : (half + 1) * HEAD, rows] = ot

    one_head(0)

    @pl.when(2 * pair + 1 < heads)
    def _():
        one_head(1)

    @pl.when(2 * pair + 1 >= heads)
    def _():
        ot_ref[0, HEAD:, :] = jnp.zeros((HEAD, length), F32)
        lse_ref[0, 1:2, :] = jnp.zeros((1, length), F32)

    o_ref[...] = jnp.transpose(ot_ref[0]).astype(BF16)


def attend_back_pair(
    block, heads, pair, q_ref, k_ref, v_ref, do_ref, ot_ref, lse_ref, dq_ref, dk_ref, dv_ref, dk_sum, dv_sum
):
    length = q_ref.shape[0]
    k_t = jnp.transpose(k_ref[...].astype(F32)).astype(BF16)
    do_t = jnp.transpose(do_ref[...].astype(F32))
    dk_sum[...] = jnp.zeros_like(dk_sum)
    dv_sum[...] = jnp.zeros_like(dv_sum)
    dq_ref[...] = jnp.zeros_like(dq_ref)

    def one_head(half):
        span = slice(half * HEAD, (half + 1) * HEAD)
        shared = jnp.sum(do_t[span, :] * ot_ref[0, span, :], axis=0, keepdims=True)
        for index in range(length // block):
            rows = slice(index * block, (index + 1) * block)
            count = (index + 1) * block
            query = keep_half(q_ref[rows, :], half) * jnp.asarray(SCALE, BF16)
            grad = keep_half(do_ref[rows, :], half)
            scores = dot_nt(k_ref[:count, :], query)
            scores = causal_tail(scores, -index * block, block)
            probs = jnp.exp(scores - lse_ref[0, half : half + 1, rows])
            grad_probs = dot_nt(v_ref[:count, :], grad)
            grad_scores = (probs * (grad_probs - shared[:, rows])).astype(BF16)
            dv_sum[:count, :] += dot(probs.astype(BF16), grad)
            dk_sum[:count, :] += dot(grad_scores, query)
            dq_t = dot(k_t[span, :count], grad_scores) * SCALE
            pad = jnp.zeros_like(dq_t)
            both = jnp.concatenate([dq_t, pad] if half == 0 else [pad, dq_t], axis=0)
            dq_ref[rows, :] = dq_ref[rows, :] + jnp.transpose(both).astype(BF16)

    one_head(0)

    @pl.when(2 * pair + 1 < heads)
    def _():
        one_head(1)

    dk_ref[...] = dk_sum[...].astype(BF16)
    dv_ref[...] = dv_sum[...].astype(BF16)


class Place:
    def __init__(self):
        self.parts = lax.axis_size("fsdp")
        self.n_ctx = lax.axis_size("ctx")
        self.part = lax.axis_index("fsdp")
        self.ctx = lax.axis_index("ctx")
        self.beside = self.part + 1 - 2 * (self.part % 2)
        self.far = (self.part + 2) % self.parts
        self.diagonal = (self.beside + 2) % self.parts

    def at(self, position):
        n = self.n_ctx
        position = (position + 2 * n) % n
        upper = position // (n // 2)
        return (1 - upper) * 2 * position + upper * (2 * (n - 1 - position) + 1)

    @property
    def position(self):
        odd = self.ctx % 2
        return (1 - odd) * (self.ctx // 2) + odd * (self.n_ctx - 1 - self.ctx // 2)


def like(shape, dtype):
    return jax.ShapeDtypeStruct(shape, dtype)


def remote(source, target, send, recv, **where):
    return pltpu.make_async_remote_copy(
        src_ref=source,
        dst_ref=target,
        send_sem=send,
        recv_sem=recv,
        device_id=where,
        device_id_type=pl.DeviceIdType.MESH,
    )


def cut(rows):
    step = 64 if rows % 64 == 0 else rows
    return [slice(start, start + step) for start in range(0, rows, step)]


class Gather:
    reach = ("fsdp",)

    def __init__(self, array):
        self.ins = [array]
        self.parts = lax.axis_size("fsdp")
        self.pieces = cut(array.shape[0])
        self.outs = [jax.ShapeDtypeStruct((self.parts, *array.shape), array.dtype)]
        self.scratch = [pltpu.SemaphoreType.DMA((3, len(self.pieces)))] * 2

    def phases(self, place, ins, outs, scratch):
        (source,), (out,), (send, recv) = ins, outs, scratch
        count = range(len(self.pieces))

        def copy(kind, k, index, target):
            piece = self.pieces[k]
            start = source.at[piece] if kind < 2 else out.at[index, piece]
            return remote(start, out.at[index, piece], send.at[kind, k], recv.at[kind, k], fsdp=target)

        def first():
            for k in count:
                copy(1, k, place.part, place.far).start()
            for k in count:
                copy(0, k, place.part, place.beside).start()
            out[place.part] = source[...]

        def second():
            for k in count:
                copy(1, k, place.far, place.far).wait_recv()
                copy(2, k, place.far, place.beside).start()

        def third():
            for k in count:
                copy(0, k, place.beside, place.beside).wait_recv()
                copy(2, k, place.diagonal, place.beside).wait_recv()
            for k in count:
                copy(0, k, place.part, place.beside).wait_send()
                copy(1, k, place.part, place.far).wait_send()
                copy(2, k, place.far, place.beside).wait_send()

        return [first, second, third]


class Scatter:
    reach = ("fsdp",)

    def __init__(self, array):
        parts, rows, columns = array.shape
        self.ins = [array]
        self.pieces = cut(rows)
        self.outs = [jax.ShapeDtypeStruct((rows, columns), F32)]
        self.scratch = [pltpu.VMEM((rows, columns), array.dtype)] * 3
        self.scratch += [pltpu.SemaphoreType.DMA((3, len(self.pieces)))] * 2

    def phases(self, place, ins, outs, scratch):
        (source,), (out,) = ins, outs
        for_far, for_own, from_far, send, recv = scratch
        count = range(len(self.pieces))

        def copy(kind, k):
            piece = self.pieces[k]
            start, target, where = [
                (source.at[place.diagonal, piece], for_far, place.beside),
                (source.at[place.beside, piece], for_own, place.beside),
                (for_far.at[piece], from_far, place.far),
            ][kind]
            return remote(start, target.at[piece], send.at[kind, k], recv.at[kind, k], fsdp=where)

        def first():
            for k in count:
                copy(0, k).start()
            for k in count:
                copy(1, k).start()

        def second():
            for k in count:
                piece = self.pieces[k]
                copy(0, k).wait_recv()
                total = for_far[piece].astype(F32) + source[place.far, piece].astype(F32)
                for_far[piece] = total.astype(for_far.dtype)
                copy(2, k).start()

        def third():
            for k in count:
                piece = self.pieces[k]
                copy(1, k).wait_recv()
                out[piece] = for_own[piece].astype(F32) + source[place.part, piece].astype(F32)

        def fourth():
            for k in count:
                piece = self.pieces[k]
                copy(2, k).wait_recv()
                out[piece] += from_far[piece].astype(F32)
            for k in count:
                for kind in range(3):
                    copy(kind, k).wait_send()

        return [first, second, third, fourth]


class ToHeads:
    reach = ("ctx",)

    def __init__(self, arrays):
        seqs, _, half, columns = arrays[0].shape
        self.n = lax.axis_size("ctx")
        self.groups = self.n // seqs
        self.piece = columns // self.groups
        self.ins = list(arrays)
        self.outs = [jax.ShapeDtypeStruct((2 * self.n, half, self.piece), a.dtype) for a in arrays]
        self.scratch = [pltpu.SemaphoreType.DMA((len(arrays), 2, self.n))] * 2

    def whole(self, ref, other, half):
        if self.groups == 1:
            return ref.at[other, half]
        column = pl.multiple_of((other % self.groups) * self.piece, LANES)
        return ref.at[other // self.groups, half, :, pl.ds(column, self.piece)]

    def block(self, ref, other, half):
        return ref.at[other if half == 0 else 2 * self.n - 1 - other]

    def source(self, ref, other, half):
        return self.whole(ref, other, half)

    def target(self, ref, other, half):
        return self.block(ref, other, half)

    def phases(self, place, ins, outs, scratch):
        send, recv = scratch
        n, me = self.n, place.ctx
        every = [(i, half) for i in range(len(ins)) for half in range(2)]

        def begin(i):
            def start(step, _):
                other = (me + step) % n
                for half in range(2):
                    remote(
                        self.source(ins[i], other, half),
                        self.target(outs[i], me, half),
                        send.at[i, half, step],
                        recv.at[i, half, step],
                        ctx=other,
                    ).start()
                return 0

            lax.fori_loop(1, n, start, 0)
            for half in range(2):
                self.target(outs[i], me, half)[...] = self.source(ins[i], me, half)[...]

        def first():
            def start(step, _):
                other = (me + step) % n
                for i, half in every:
                    remote(
                        self.source(ins[i], other, half),
                        self.target(outs[i], me, half),
                        send.at[i, half, step],
                        recv.at[i, half, step],
                        ctx=other,
                    ).start()
                return 0

            lax.fori_loop(1, n, start, 0)
            for i, half in every:
                self.target(outs[i], me, half)[...] = self.source(ins[i], me, half)[...]

        self.begin = begin

        def second():
            def end(step, _):
                other = (me + n - step) % n
                for i, half in every:
                    copy = remote(
                        self.source(ins[i], other, half),
                        self.target(outs[i], other, half),
                        send.at[i, half, step],
                        recv.at[i, half, step],
                        ctx=other,
                    )
                    copy.wait_recv()
                    copy.wait_send()
                return 0

            lax.fori_loop(1, n, end, 0)

        return [first, second]


class Swap:
    reach = ("fsdp",)

    def __init__(self, arrays, live, wide):
        self.parts = lax.axis_size("fsdp")
        self.live, self.wide = live, wide
        self.ins = list(arrays)
        rows = arrays[0].shape[0]
        shape = (len(arrays), self.parts, rows, wide)
        self.outs = [jax.ShapeDtypeStruct(shape[1:], arrays[0].dtype)] * len(arrays)
        self.scratch = [pltpu.VMEM(shape, arrays[0].dtype)]
        self.scratch += [pltpu.SemaphoreType.DMA((len(arrays), self.parts))] * 2

    def phases(self, place, ins, outs, scratch):
        stage, send, recv = scratch
        parts, live = self.parts, self.live
        every = [(i, step) for step in (2, 3, 1) for i in range(len(ins))]

        def copy(i, step, index):
            other = (place.part + step) % parts
            return remote(
                stage.at[i, other], outs[i].at[index], send.at[i, step], recv.at[i, step], fsdp=other
            )

        def first():
            for i, ref in enumerate(ins):
                for part in range(parts):
                    start = part * live
                    stop = min(start + live, ref.shape[1])
                    stage[i, part, :, : stop - start] = ref[:, start:stop]
                    if stop - start < self.wide:
                        shape = (ref.shape[0], self.wide - stop + start)
                        stage[i, part, :, stop - start :] = jnp.zeros(shape, ref.dtype)
            for i, step in every:
                copy(i, step, place.part).start()
            for i in range(len(ins)):
                outs[i][place.part] = stage[i, place.part]

        def second():
            for i, step in every:
                copy(i, step, (place.part + parts - step) % parts).wait_recv()
                copy(i, step, place.part).wait_send()

        return [first, second]


class Window:
    reach = ("fsdp",)

    def __init__(self, array, live, wide):
        self.parts = lax.axis_size("fsdp")
        self.quarter, columns = array.shape
        self.live, self.wide = live, wide
        self.near = (live - self.quarter) * self.parts
        self.ins = [array]
        self.outs = [jax.ShapeDtypeStruct((wide, columns), array.dtype)]
        self.scratch = [pltpu.VMEM((self.quarter + self.near, columns), array.dtype)]
        self.scratch += [pltpu.SemaphoreType.DMA] * 2

    def phases(self, place, ins, outs, scratch):
        (source,), (out,), (both, send, recv) = ins, outs, scratch
        left = (place.part + self.parts - 1) % self.parts
        copy = remote(
            source.at[: self.near], both.at[self.quarter :], send, recv, fsdp=left
        )

        def first():
            copy.start()
            both[: self.quarter] = source[...]

        def second():
            copy.wait()
            start = pl.multiple_of(place.part * (self.live - self.quarter), 16)
            rows = both[pl.ds(start, self.live), :]
            index = lax.broadcasted_iota(jnp.int32, rows.shape, 0) + place.part * self.live
            inside = index < self.quarter * self.parts
            out[: self.live] = jnp.where(inside, rows, jnp.zeros_like(rows))
            if self.wide > self.live:
                out[self.live :] = jnp.zeros((self.wide - self.live, rows.shape[1]), rows.dtype)

        return [first, second]


class Total:
    reach = ("ctx",)

    def __init__(self, array):
        self.n = lax.axis_size("ctx")
        self.ins = [array]
        self.outs = [jax.ShapeDtypeStruct(array.shape, F32)]
        self.scratch = [pltpu.VMEM((self.n, *array.shape), array.dtype)]
        self.scratch += [pltpu.SemaphoreType.DMA((self.n,))] * 2

    def phases(self, place, ins, outs, scratch):
        (source,), (out,), (held, send, recv) = ins, outs, scratch
        n, me = self.n, place.ctx

        def copy(step, index):
            return remote(source, held.at[index], send.at[step], recv.at[step], ctx=(me + step) % n)

        def first():
            lax.fori_loop(1, n, lambda step, _: (copy(step, me).start(), 0)[1], 0)
            held[me] = source[...]

        def last():
            def end(step, _):
                copy(step, (me + n - step) % n).wait_recv()
                copy(step, me).wait_send()
                return 0

            lax.fori_loop(1, n, end, 0)
            total = held[0].astype(F32)
            for i in range(1, n):
                total = total + held[i].astype(F32)
            out[...] = total

        return [first, last]


class Ring:
    reach = ("ring", "fsdp")

    def __init__(self, products):
        self.n = n = lax.axis_size("ctx")
        self.parts = lax.axis_size("fsdp")
        self.per = n // self.parts
        self.products, self.streams, lefts = [], [], []
        self.ins, self.outs, slots, local, turned = [], [], [], [], []
        for left, right, heights, crossing in products:
            rows, columns = left.shape[1] // n, right.shape[1]
            known = [k for k, other in enumerate(lefts) if other is left]
            if not known:
                lefts.append(left)
                turned.append(pltpu.VMEM((n, rows, left.shape[0]), left.dtype))
            index = len(self.products)
            self.products.append((known[0] if known else len(lefts) - 1, crossing))
            self.ins.append(right)
            self.outs.append(like((n, rows, columns), BF16))
            slots.append(pltpu.VMEM((n - 1, rows, columns), BF16))
            local.append(pltpu.VMEM((2, rows, columns), BF16))
            start = 0
            for direction, count in zip((1, -1), heights):
                if count:
                    self.streams.append((index, slice(start, start + count), direction))
                start += count
        self.streams.sort(key=lambda stream: not self.products[stream[0]][1])
        self.counts = (len(lefts), len(products))
        self.ins = lefts + self.ins
        self.spaces = [pl.ANY] * len(self.outs)
        self.scratch = turned + slots + local
        self.scratch += [pltpu.SemaphoreType.DMA((len(self.streams), 2, n))] * 2

    def phases(self, place, ins, outs, scratch):
        n_left, n_product = self.counts
        lefts, rights = ins[:n_left], ins[n_left:]
        turned, scratch = scratch[:n_left], scratch[n_left:]
        slots, scratch = scratch[:n_product], scratch[n_product:]
        local, (send, recv) = scratch[:n_product], scratch[n_product:]
        n, parts, per, here = self.n, self.parts, self.per, place.position
        shift = place.ctx // per
        owner = (place.part + shift) % parts

        def make(step):
            for stream, (index, part, direction) in enumerate(self.streams):
                slab = place.at(here - direction * (step + 1))
                if crosses(stream):
                    slab = (slab + per * place.part) % n
                left = turned[self.products[index][0]]
                own = dot(left[slab, part], rights[index][...])
                local[index][step % 2, part] = own.astype(BF16)

        def way(stream):
            return self.streams[stream][2]

        def crosses(stream):
            return self.products[self.streams[stream][0]][1]

        def reducing(stream, step):
            index, part, _ = self.streams[stream]
            source = local[index].at[0] if step == 0 else slots[index].at[step - 1]
            return remote(
                source.at[part],
                slots[index].at[step, part],
                send.at[stream, 0, step],
                recv.at[stream, 0, step],
                ctx=place.at(here + way(stream)),
            )

        def last(stream):
            index, part, _ = self.streams[stream]
            return slots[index].at[n - 2, part]

        def mine(stream):
            index, part, _ = self.streams[stream]
            return outs[index].at[place.ctx, part]

        def crossing(stream):
            return remote(
                last(stream),
                mine(stream),
                send.at[stream, 0, n - 1],
                recv.at[stream, 0, n - 1],
                fsdp=owner,
            )

        def keeping(stream):
            return pltpu.make_async_copy(last(stream), mine(stream), send.at[stream, 0, n - 1])

        def gathering(stream, step, back=0):
            index, part, _ = self.streams[stream]
            slab = place.at(here - way(stream) * (step + back))
            block = outs[index].at[slab, part]
            source = block
            if step == 0 and back == 0 and not crosses(stream):
                source = last(stream)
            return remote(
                source,
                block,
                send.at[stream, 1, step],
                recv.at[stream, 1, step],
                ctx=place.at(here + way(stream)),
            )

        every = range(len(self.streams))

        def begin():
            for left, target in zip(lefts, turned):
                rows = target.shape[1]
                for k in range(n):
                    target[k] = jnp.transpose(left[:, k * rows : (k + 1) * rows])
            make(0)
            for stream in every:
                reducing(stream, 0).start()
            make(1)

        def add(stream, step):
            index, part, _ = self.streams[stream]
            reducing(stream, step).wait_recv()
            total = slots[index][step, part].astype(F32)
            total = total + local[index][(step + 1) % 2, part].astype(F32)
            slots[index][step, part] = total.astype(BF16)

        def reduce(step):
            for stream in every:
                add(stream, step - 1)
                reducing(stream, step).start()
            if step == 1:
                for stream in every:
                    reducing(stream, 0).wait_send()
            make(step + 1)

        def turn():
            for stream in every:
                add(stream, n - 2)
                if not crosses(stream):
                    gathering(stream, 0).start()
                    keeping(stream).start()
                    continue

                @pl.when(shift == 0)
                def _():
                    keeping(stream).start()

                @pl.when(shift != 0)
                def _():
                    crossing(stream).start()

        def launch(stream):
            @pl.when(shift == 0)
            def _():
                keeping(stream).wait()

            @pl.when(shift != 0)
            def _():
                crossing(stream).wait()

            gathering(stream, 0).start()

        def forward(turn):
            for stream in [s for s in every if not crosses(s)] + [s for s in every if crosses(s)]:
                step = turn - 1 if crosses(stream) else turn
                if step == 0:
                    launch(stream)
                elif step < n - 1:
                    gathering(stream, step - 1, 1).wait_recv()
                    gathering(stream, step).start()

        def end():
            for stream in every:
                gathering(stream, n - 2, 1).wait_recv()
            for stream in every:
                if not crosses(stream):
                    keeping(stream).wait()
                for step in range(n - 1):
                    if step:
                        reducing(stream, step).wait_send()
                    gathering(stream, step).wait_send()

        steps = [begin]
        steps += [functools.partial(reduce, step) for step in range(1, n - 1)]
        steps += [turn]
        steps += [functools.partial(forward, step) for step in range(1, n)]
        return steps + [end]


def exchange_kernel(transfers, places, *refs):
    refs = list(refs)
    inputs = refs[: max(places) + 1]
    refs = [inputs[index] for index in places] + refs[len(inputs) :]

    def take(lists):
        taken = []
        for items in lists:
            taken.append(refs[: len(items)])
            del refs[: len(items)]
        return taken

    ins = take([t.ins for t in transfers])
    outs = take([t.outs for t in transfers])
    scratch = take([t.scratch for t in transfers])
    place = Place()
    reach = {name for t in transfers for name in t.reach}
    peers = []
    if "fsdp" in reach:
        peers += [dict(fsdp=(place.part + k) % place.parts) for k in range(1, place.parts)]
    if "ctx" in reach:
        peers += [dict(ctx=(place.ctx + k) % place.n_ctx) for k in range(1, place.n_ctx)]
    if "ring" in reach:
        peers += [dict(ctx=place.at(place.position + k)) for k in (1, -1)]
    barrier = pltpu.get_barrier_semaphore()
    for peer in peers:
        pl.semaphore_signal(barrier, inc=1, device_id=peer, device_id_type=pl.DeviceIdType.MESH)
    pl.semaphore_wait(barrier, len(peers))
    lists = [t.phases(place, *each) for t, *each in zip(transfers, ins, outs, scratch)]
    for index in range(max(map(len, lists))):
        for phases in lists:
            if index < len(phases):
                phases[index]()


def exchange(number, name, *transfers):
    memory = pl.BlockSpec(memory_space=pltpu.VMEM)
    ins, places = [], []
    for array in [a for t in transfers for a in t.ins]:
        known = [k for k, other in enumerate(ins) if other is array]
        places.append(known[0] if known else len(ins))
        if not known:
            ins.append(array)
    outs = [a for t in transfers for a in t.outs]
    spaces = []
    for t in transfers:
        spaces += getattr(t, "spaces", [pltpu.VMEM] * len(t.outs))
    results = pl.pallas_call(
        functools.partial(exchange_kernel, transfers, places),
        out_shape=outs,
        in_specs=[memory] * len(ins),
        out_specs=[pl.BlockSpec(memory_space=space) for space in spaces],
        scratch_shapes=[s for t in transfers for s in t.scratch],
        compiler_params=pltpu.CompilerParams(collective_id=number, has_side_effects=True),
        name=name,
    )(*ins)
    results = list(results)
    split = []
    for t in transfers:
        split.append(results[: len(t.outs)])
        del results[: len(t.outs)]
    return split


def share(transfer, place, refs, ins, outs):
    count = len(transfer.scratch)
    taken = refs[:count]
    del refs[:count]
    return transfer.phases(place, ins, outs, taken)


def quarter_rows(place_index, own):
    return pl.ds(pl.multiple_of(place_index * own, own), own)


def scattered(place, partial, part, scatter_phases):
    first, second, third, fourth = scatter_phases

    def fill(index):
        part[index] = partial(index).astype(part.dtype)

    def begin():
        fill(place.diagonal)
        fill(place.beside)
        first()

    def middle():
        fill(place.far)
        second()

    def later():
        fill(place.part)
        third()

    return [begin, middle, later, fourth]


class Sender:
    def __init__(self, count, seqs, half, piece):
        self.n = n = lax.axis_size("ctx")
        self.half, self.piece, self.pairs = half, piece, piece // LANES
        self.groups = n // seqs
        self.count = count
        self.outs = [like((seqs, 2, half, piece * self.groups), BF16)] * count
        self.scratch = [pltpu.VMEM((2 * n * half, piece), BF16)] * count
        self.scratch += [pltpu.SemaphoreType.DMA((count, 2, self.pairs, n))] * 2

    def bind(self, place, outs, scratch):
        held, (send, recv) = scratch[: self.count], scratch[self.count :]
        n, me, half = self.n, place.ctx, self.half
        every = [(i, side) for i in range(self.count) for side in range(2)]

        def block(ref, pair, other, side):
            index = other if side == 0 else 2 * n - 1 - other
            rows = pl.ds(pl.multiple_of(index * half, half), half)
            return ref.at[rows, pl.ds(pl.multiple_of(pair * LANES, LANES), LANES)]

        def place_of(ref, pair, other, side):
            column = pl.multiple_of(other % self.groups * self.piece + pair * LANES, LANES)
            return ref.at[other // self.groups, side, :, pl.ds(column, LANES)]

        def copy(i, side, pair, step, index):
            other = (me + step) % n
            return remote(
                block(held[i], pair, other, side),
                place_of(outs[i], pair, index, side),
                send.at[i, side, pair, step],
                recv.at[i, side, pair, step],
                ctx=other,
            )

        def begin(pair):
            def start(step, _):
                for i, side in every:
                    copy(i, side, pair, step, me).start()
                return 0

            lax.fori_loop(1, n, start, 0)
            for i, side in every:
                place_of(outs[i], pair, me, side)[...] = block(held[i], pair, me, side)[...]

        def end():
            def pair_end(pair, _):
                def step_end(step, _):
                    for i, side in every:
                        copy(i, side, pair, step, (me + n - step) % n).wait_recv()
                        copy(i, side, pair, step, me).wait_send()
                    return 0

                lax.fori_loop(1, n, step_end, 0)
                return 0

            lax.fori_loop(0, self.pairs, pair_end, 0)

        return held, begin, end


def lanes(ref, pair):
    return ref.at[:, pl.ds(pl.multiple_of(pair * LANES, LANES), LANES)]


class Attend:
    reach = ("ctx",)

    def __init__(self, queries, keys, values, heads, seqs, half):
        length, piece = queries.shape
        self.block, self.heads = min(256, length), heads
        self.sender = Sender(1, seqs, half, piece)
        pairs = self.sender.pairs
        self.ins = [queries, keys, values]
        self.outs = [
            *self.sender.outs,
            like((pairs, LANES, length), F32),
            like((pairs, 2, length), F32),
        ]
        self.scratch = self.sender.scratch

    def phases(self, place, ins, outs, scratch):
        out, ot, lse = outs
        held, begin, end = self.sender.bind(place, [out], scratch)

        def run():
            def one(pair, _):
                columns = [lanes(ref, pair) for ref in (*ins, held[0])]
                own = pl.ds(pair, 1)
                attend_pair(self.block, self.heads, pair, *columns, ot.at[own], lse.at[own])
                begin(pair)
                return 0

            lax.fori_loop(0, self.sender.pairs, one, 0)

        return [run, end]


class AttendBack:
    reach = ("ctx",)

    def __init__(self, queries, keys, values, grad, ot, lse, heads, seqs, half):
        length, piece = queries.shape
        self.block, self.heads = min(256, length), heads
        self.sender = Sender(3, seqs, half, piece)
        self.ins = [queries, keys, values, grad, ot, lse]
        self.outs = self.sender.outs
        self.scratch = [pltpu.VMEM((length, LANES), F32)] * 2 + self.sender.scratch

    def phases(self, place, ins, outs, scratch):
        *given, ot, lse = ins
        sums, scratch = scratch[:2], scratch[2:]
        held, begin, end = self.sender.bind(place, outs, scratch)

        def run():
            def one(pair, _):
                own = pl.ds(pair, 1)
                attend_back_pair(
                    self.block,
                    self.heads,
                    pair,
                    *[lanes(ref, pair) for ref in given],
                    ot.at[own],
                    lse.at[own],
                    *[lanes(ref, pair) for ref in held],
                    *sums,
                )
                begin(pair)
                return 0

            lax.fori_loop(0, self.sender.pairs, one, 0)

        return [run, end]


class Middle:
    reach = ("fsdp", "ctx")

    def __init__(self, heads, out_w, x_full, vectors):
        own, width = x_full.shape
        parts = lax.axis_size("fsdp")
        self.own, self.parts = own, parts
        self.heads = heads
        self.scatter = Scatter(like((parts, own, width), BF16))
        self.gather = Gather(like((own, width), BF16))
        self.ins = [*heads.ins, out_w, x_full, vectors]
        self.outs = [
            *heads.outs,
            like((own, width), F32),
            like((own, width), F32),
            like((own, 1), F32),
            self.gather.outs[0],
        ]
        self.scratch = [
            pltpu.VMEM((parts, own, width), BF16),
            pltpu.VMEM((own, width), F32),
            pltpu.VMEM((own, width), BF16),
        ]
        for transfer in (self.heads, self.scatter, self.gather):
            self.scratch += transfer.scratch

    def phases(self, place, ins, outs, scratch):
        *given, out_w, x_full, vectors = ins
        attended, ot, lse, resid, hat, inv, normed_all = outs
        part, branch, normed, *rest = scratch
        heads = share(self.heads, place, rest, given, [attended, ot, lse])
        scatter = share(self.scatter, place, rest, [part], [branch])
        gather = share(self.gather, place, rest, [normed], [normed_all])
        seqs, _, half, cols = attended.shape
        group = seqs // self.parts

        def partial(index):
            rows = attended[pl.ds(index * group, group)].reshape(self.own, cols)
            return dot(rows, out_w[...])

        def norm():
            total = x_full[...] + branch[...] + vectors[0:1]
            resid[...] = total
            hat[...], inv[...] = normalize(total)
            normed[...] = (hat[...] * vectors[1:2] + vectors[2:3]).astype(BF16)

        return heads + scattered(place, partial, part, scatter) + [norm] + gather


class Product:
    reach = ("fsdp",)

    def __init__(self, left, right, own):
        parts, width = lax.axis_size("fsdp"), right.shape[1]
        self.own = own
        self.scatter = Scatter(like((parts, own, width), BF16))
        self.ins = [left, right]
        self.outs = [like((own, width), F32)]
        self.scratch = [pltpu.VMEM((parts, own, width), BF16), *self.scatter.scratch]

    def phases(self, place, ins, outs, scratch):
        left, right = ins
        part, *rest = scratch
        scatter = share(self.scatter, place, rest, [part], outs)

        def partial(index):
            return dot(left[quarter_rows(index, self.own), :], right[...])

        return scattered(place, partial, part, scatter)


class SecondBack:
    reach = ("fsdp",)

    def __init__(self, grad_pre, fc, hat, inv, gain, grad_y, out_w):
        own, width = hat.shape
        parts = lax.axis_size("fsdp")
        self.own, self.parts = own, parts
        self.scatter = Scatter(like((parts, own, width), BF16))
        self.gather = Gather(like((own, width), BF16))
        self.ins = [grad_pre, fc, hat, inv, gain, grad_y, out_w]
        self.outs = [
            like((own, width), F32),
            self.gather.outs[0],
            like((parts * own, out_w.shape[0]), BF16),
            like((4, width), F32),
        ]
        self.scratch = [
            pltpu.VMEM((parts, own, width), BF16),
            pltpu.VMEM((own, width), F32),
            pltpu.VMEM((own, width), BF16),
        ]
        for transfer in (self.scatter, self.gather):
            self.scratch += transfer.scratch

    def phases(self, place, ins, outs, scratch):
        grad_pre, fc, hat, inv, gain, grad_y, out_w = ins
        resid, branch_all, attended, sums = outs
        part, norm_grad, branch, *rest = scratch
        scatter = share(self.scatter, place, rest, [part], [norm_grad])
        gather = share(self.gather, place, rest, [branch], [branch_all])
        own = self.own

        def partial(index):
            return dot_nt(grad_pre[quarter_rows(index, own), :], fc[...])

        def norm():
            given = grad_y[...].astype(F32)
            total = given + norm_back(norm_grad[...], gain[...], hat[...], inv[...])
            resid[...] = total
            branch[...] = total.astype(BF16)
            sums[0:1] = jnp.sum(norm_grad[...] * hat[...], axis=0, keepdims=True)
            sums[1:2] = jnp.sum(norm_grad[...], axis=0, keepdims=True)
            sums[2:3] = jnp.sum(branch[...].astype(F32), axis=0, keepdims=True)
            sums[3:4] = jnp.sum(given, axis=0, keepdims=True)

        def project():
            for index in range(self.parts):
                rows = dot_nt(branch_all[index], out_w[...])
                attended[index * own : (index + 1) * own] = rows.astype(BF16)

        return scattered(place, partial, part, scatter) + [norm] + gather + [project]


class FirstBack:
    reach = ("fsdp", "ctx")

    def __init__(self, grads, weights, hat, inv, gain, resid, rest, bias_fc):
        own, width = hat.shape
        parts = lax.axis_size("fsdp")
        self.own, self.parts, self.count = own, parts, len(grads)
        quarter = width // parts
        lines = rest.shape[0] + 2
        self.scatter = Scatter(like((parts, own, width), BF16))
        self.small = Scatter(like((parts, lines, quarter), F32))
        self.total = Total(like((lines + bias_fc.shape[0], quarter), F32))
        self.ins = [*grads, *weights, hat, inv, gain, resid, rest, bias_fc]
        self.outs = [like((own, width), F32), self.total.outs[0]]
        self.scratch = [
            pltpu.VMEM((parts, own, width), BF16),
            pltpu.VMEM((own, width), F32),
            pltpu.VMEM((lines, width), F32),
            pltpu.VMEM((parts, lines, quarter), F32),
            pltpu.VMEM((lines, quarter), F32),
            pltpu.VMEM((lines + bias_fc.shape[0], quarter), F32),
        ]
        for transfer in (self.scatter, self.small, self.total):
            self.scratch += transfer.scratch

    def phases(self, place, ins, outs, scratch):
        grads, weights = ins[: self.count], ins[self.count : 2 * self.count]
        hat, inv, gain, resid, others, bias_fc = ins[2 * self.count :]
        input_grad, totals = outs
        part, norm_grad, lines, small, small_sum, packed, *rest = scratch
        scatter = share(self.scatter, place, rest, [part], [norm_grad])
        small_scatter = share(self.small, place, rest, [small], [small_sum])
        total = share(self.total, place, rest, [packed], [totals])
        quarter = small.shape[2]
        count = lines.shape[0]

        def partial(index):
            rows = quarter_rows(index, self.own)
            return sum(dot_nt(grad[rows, :], weight[...]) for grad, weight in zip(grads, weights))

        def norm():
            input_grad[...] = resid[...] + norm_back(norm_grad[...], gain[...], hat[...], inv[...])
            lines[0:1] = jnp.sum(norm_grad[...] * hat[...], axis=0, keepdims=True)
            lines[1:2] = jnp.sum(norm_grad[...], axis=0, keepdims=True)
            lines[2:] = others[...]
            for index in range(self.parts):
                small[index] = lines[:, index * quarter : (index + 1) * quarter]

        def pack():
            packed[:count] = small_sum[...]
            packed[count:] = bias_fc[...]
            total[0]()

        phases = scattered(place, partial, part, scatter) + [norm] + small_scatter
        return phases + [pack, total[1]]


class Later:
    def __init__(self, transfer, *steps):
        self.transfer, self.steps = transfer, steps
        self.reach = transfer.reach
        self.ins, self.outs, self.scratch = transfer.ins, transfer.outs, transfer.scratch

    def phases(self, place, ins, outs, scratch):
        phases = [lambda: None] * (self.steps[-1] + 1)
        for step, phase in zip(self.steps, self.transfer.phases(place, ins, outs, scratch)):
            phases[step] = phase
        return phases


class Spread:
    reach = ("fsdp", "ring")

    def __init__(self, arrays, live, wide):
        self.n = lax.axis_size("ctx")
        self.parts = lax.axis_size("fsdp")
        self.live, self.wide = live, wide
        self.across = wide // LANES
        self.down = self.n // self.across
        self.rows = arrays[0].shape[0] // self.down
        self.ins = list(arrays)
        shape = (self.parts, self.down, self.rows, wide)
        self.outs = [like(shape, a.dtype) for a in arrays]
        self.scratch = [pltpu.VMEM(shape, a.dtype) for a in arrays]
        self.scratch += [pltpu.SemaphoreType.DMA((len(arrays), self.parts + self.n))] * 2

    @staticmethod
    def fits(rows, wide):
        across = wide // LANES
        n = lax.axis_size("ctx")
        return n % across == 0 and rows % (n // across) == 0 and rows // (n // across) % 8 == 0

    def phases(self, place, ins, outs, scratch):
        stages, (send, recv) = scratch[:-2], scratch[-2:]
        n, parts, here = self.n, self.parts, place.position
        every = range(len(ins))

        def of(ctx):
            column = pl.multiple_of(ctx % self.across * LANES, LANES)
            return (ctx // self.across, slice(None), pl.ds(column, LANES))

        def piece(i, step, index):
            other = (place.part + step) % parts
            mine = of(place.ctx)
            return remote(
                stages[i].at[(other, *mine)],
                outs[i].at[(index, *mine)],
                send.at[i, step],
                recv.at[i, step],
                fsdp=other,
            )

        def passing(i, step, back=0):
            direction = 1 - 2 * (i % 2)
            block = outs[i].at[(slice(None), *of(place.at(here - direction * (step + back))))]
            return remote(
                block,
                block,
                send.at[i, parts + step],
                recv.at[i, parts + step],
                ctx=place.at(here + direction),
            )

        def first():
            for i in every:
                for part in range(parts):
                    start = part * self.live
                    stop = min(start + self.live, ins[i].shape[1])
                    for half in range(self.down):
                        rows = slice(half * self.rows, (half + 1) * self.rows)
                        block = ins[i][rows, start:stop]
                        stages[i][part, half, :, : stop - start] = block
                        if stop - start < self.wide:
                            zeros = jnp.zeros((self.rows, self.wide - stop + start), block.dtype)
                            stages[i][part, half, :, stop - start :] = zeros
                for step in (2, 3, 1):
                    piece(i, step, place.part).start()
                mine = of(place.ctx)
                outs[i][(place.part, *mine)] = stages[i][(place.part, *mine)]

        def turn():
            for i in every:
                for step in (1, 2, 3):
                    piece(i, step, (place.part + parts - step) % parts).wait_recv()
                passing(i, 0).start()

        def forward(step):
            for i in every:
                passing(i, step - 1, 1).wait_recv()
                passing(i, step).start()

        def end():
            for i in every:
                passing(i, n - 2, 1).wait_recv()
            for i in every:
                for step in (1, 2, 3):
                    piece(i, step, place.part).wait_send()
                for step in range(n - 1):
                    passing(i, step).wait_send()

        return [first, turn] + [functools.partial(forward, s) for s in range(1, n - 1)] + [end]


class First:
    reach = ("fsdp", "ctx", "ring")

    def __init__(self, inputs, vectors, weights, live, cols, seqs):
        own, width = inputs.shape
        self.parts = parts = lax.axis_size("fsdp")
        self.n = lax.axis_size("ctx")
        self.own, self.live, self.count = own, live, len(vectors)
        quarter = width // parts
        self.spread = Spread(weights[1:], live, cols) if Spread.fits(quarter, cols) else None
        self.swap = Swap(weights[:1] if self.spread else weights, live, cols)
        self.small = Gather(like((len(vectors), quarter), BF16))
        self.gather = Gather(like((own, width), BF16))
        token = like((seqs, 2, own // (seqs // parts) // 2, cols), BF16)
        self.heads = ToHeads([token] * 3)
        self.ins = [inputs, *vectors, *weights]
        self.outs = [
            *[like((width, cols), BF16)] * 3,
            like((own, width), F32),
            like((own, 1), F32),
            self.gather.outs[0],
            like((len(vectors), width), F32),
            *self.heads.outs,
        ]
        self.scratch = [
            pltpu.VMEM((len(vectors), quarter), BF16),
            pltpu.VMEM((parts, len(vectors), quarter), BF16),
            pltpu.VMEM((own, width), BF16),
            pltpu.VMEM((2, cols), F32),
        ]
        self.scratch += [pltpu.VMEM(token.shape, BF16)] * 3
        self.moved = [*self.swap.outs, *(self.spread.outs if self.spread else [])]
        self.scratch += [pltpu.VMEM(out.shape, BF16) for out in self.moved]
        for transfer in (self.swap, self.small, self.gather, self.heads):
            self.scratch += transfer.scratch
        if self.spread:
            self.scratch += self.spread.scratch

    def phases(self, place, ins, outs, scratch):
        inputs, vectors, weights = ins[0], ins[1 : 1 + self.count], ins[1 + self.count :]
        qkv, (hat, inv, normed_all, full), heads_out = outs[:3], outs[3:7], outs[7:]
        small_own, small_all, normed, bias, *rest = scratch
        tokens, rest = rest[:3], rest[3:]
        moved, rest = rest[:3], rest[3:]
        swapped = moved[: len(self.swap.outs)]
        swap = share(self.swap, place, rest, weights[: len(swapped)], swapped)
        small = share(self.small, place, rest, [small_own], [small_all])
        gather = share(self.gather, place, rest, [normed], [normed_all])
        heads = share(self.heads, place, rest, tokens, heads_out)
        begin_heads = self.heads.begin
        spread = []
        if self.spread:
            spread = share(self.spread, place, rest, weights[1:], moved[1:])
        parts, live, own = self.parts, self.live, self.own
        quarter = small_own.shape[1]
        group = tokens[0].shape[0] // parts

        def begin():
            for index, vector in enumerate(vectors):
                small_own[index : index + 1] = vector[...].reshape(1, quarter)
            small[0]()
            if spread:
                spread[0]()
            swap[0]()
            hat[...], inv[...] = normalize(inputs[...].astype(F32))

        def norm():
            small[1]()
            small[2]()
            for part in range(parts):
                full[:, part * quarter : (part + 1) * quarter] = small_all[part].astype(F32)
            normed[...] = (hat[...] * full[0:1] + full[1:2]).astype(BF16)
            gather[0]()
            bias[...] = jnp.zeros_like(bias)
            for part in range(parts):

                @pl.when(place.part == part)
                def _():
                    stop = min(live, full.shape[1] - part * live)
                    bias[:, :stop] = full[2:4, part * live : part * live + stop]

        def arrive():
            gather[1]()
            gather[2]()
            swap[1]()

        def unpack(i):
            source, target = moved[i], qkv[i]
            if len(source.shape) == 3:
                rows = source.shape[1]
                for part in range(parts):
                    target[part * rows : (part + 1) * rows] = source[part]
                return
            _, down, rows, _ = source.shape
            for part in range(parts):
                for half in range(down):
                    start = (part * down + half) * rows
                    target[start : start + rows] = source[part, half]

        def project(i):
            unpack(i)
            for part in range(parts):
                rows = dot(normed_all[part], qkv[i][...])
                if i != 1:
                    rows = rows + bias[i // 2 : i // 2 + 1]
                shape = (group, *tokens[i].shape[1:])
                tokens[i][part * group : (part + 1) * group] = rows.astype(BF16).reshape(shape)
            begin_heads(i)

        phases = [begin, norm] + spread[1:] + [arrive]
        self.ready = len(phases)
        return phases + [functools.partial(project, i) for i in range(3)] + [heads[1]]


def results_kernel(widths, parts, order_ref, *refs):
    for index, (live, total) in enumerate(widths):
        out = refs[len(widths) * parts + index]
        for part in range(parts):
            stop = min((part + 1) * live, total)
            block = refs[index * parts + part][0, :, : stop - part * live]
            out[:, part * live : stop] = block.astype(F32)


def by_rows(arrays, widths, per, part, parts):
    slabs, rows, _ = arrays[0].shape
    order = (part - jnp.arange(parts, dtype=jnp.int32) + parts) % parts
    if rows % 8:
        outs = []
        for array, (live, total) in zip(arrays, widths):
            array = jnp.take(array.reshape(parts, per, rows, -1), order, axis=0)[..., :live]
            array = jnp.transpose(array, (1, 2, 0, 3)).reshape(per * rows, parts * live)
            outs.append(array[:, :total].astype(F32))
        return outs
    step = 40 if rows % 40 == 0 else rows
    inner = rows // step

    def source(column, array):
        return pl.BlockSpec(
            (1, step, array.shape[2]),
            lambda i, order: (order[column] * per + i // inner, i % inner, 0),
        )

    return pl.pallas_call(
        functools.partial(results_kernel, widths, parts),
        out_shape=[jax.ShapeDtypeStruct((per * rows, total), F32) for _, total in widths],
        grid_spec=pltpu.PrefetchScalarGridSpec(
            num_scalar_prefetch=1,
            grid=(per * inner,),
            in_specs=[source(column, array) for array in arrays for column in range(parts)],
            out_specs=[pl.BlockSpec((step, total), lambda i, order: (i, 0)) for _, total in widths],
        ),
        name="by_rows",
    )(order, *[array for array in arrays for _ in range(parts)])


def on_device(
    inputs,
    cotangent,
    w_query,
    w_key,
    w_value,
    w_out,
    w_fc,
    w_proj,
    ln1_gain,
    ln1_bias,
    query_bias,
    value_bias,
    out_bias,
    ln2_gain,
    ln2_bias,
    fc_bias,
    proj_bias,
):
    parts = lax.axis_size("fsdp")
    n_ctx = lax.axis_size("ctx")
    me_part = lax.axis_index("fsdp")
    seqs, rows, width = inputs.shape
    hidden = w_fc.shape[1]
    quarter = width // parts
    hidden_part = hidden // parts
    own = seqs * rows
    all_seqs = seqs * parts
    tokens = all_seqs * rows
    length = rows * n_ctx
    half_rows = rows // 2
    groups = n_ctx // all_seqs
    heads_part = -(-HEADS // parts)
    live = heads_part * HEAD
    slots = -(-heads_part // (2 * groups)) * 2 * groups
    cols = slots * HEAD
    piece = cols // groups
    heads_here = heads_part if groups == 1 else slots // groups
    near = (live - quarter) * parts
    per = n_ctx // parts
    slab = width // n_ctx

    def by_sequences(array):
        return array.reshape(all_seqs, 2, half_rows, cols)

    def split(rows, more):
        low = (rows // 2 + 7 * more) // 8 * 8
        return (low, rows - low)

    x_full = inputs.astype(F32).reshape(own, width)
    vectors = [ln1_gain, ln1_bias, query_bias, value_bias, out_bias, ln2_gain, ln2_bias, proj_bias]
    first = First(
        inputs.reshape(own, width),
        vectors,
        [w_query, w_key, w_value],
        live,
        cols,
        all_seqs,
    )
    steps = 3 + (n_ctx if first.spread else 0)
    (*qkv, hat_one, inv_one, normed_one, full, q_heads, k_heads, v_heads), (fc,), (out_w,) = exchange(
        0,
        "first",
        first,
        Later(Swap([w_fc], hidden_part, hidden_part), steps + 2, steps + 3),
        Later(Window(w_out, live, cols), steps + 2, steps + 3),
    )
    gain_one, gain_two, bias_proj = full[0], full[5], full[7]
    bias_fc = fc_bias.astype(F32)
    normed_one = normed_one.reshape(tokens, width)
    fc = fc.reshape(width, hidden_part)
    proj = w_proj
    heads = [q_heads, k_heads, v_heads]

    q_seq, k_seq, v_seq = [a.reshape(length, piece) for a in heads]
    (grad_y,), (attended, ot, lse, resid, hat_two, inv_two, normed_two) = exchange(
        2,
        "middle",
        Gather(cotangent.reshape(own, width)),
        Middle(
            Attend(q_seq, k_seq, v_seq, heads_here, all_seqs, half_rows), out_w, x_full, full[4:7]
        ),
    )
    attended = attended.reshape(tokens, cols)
    normed_two = normed_two.reshape(tokens, width)
    grad_y = grad_y.reshape(tokens, width)

    pre_act = dot(normed_two, fc) + bias_fc
    value, slope = gelu_both(pre_act)
    activated = value.astype(BF16)

    grad_pre = (dot_nt(grad_y, proj) * slope).astype(BF16)
    grad_bias_fc = jnp.sum(grad_pre.astype(F32), axis=0)
    (proj_grad, fc_grad), (grad_resid, grad_branch, grad_attended, sums_two) = exchange(
        3,
        "wide_grads",
        Ring(
            [
                (activated, grad_y, split(slab, 1), False),
                (normed_two, grad_pre, split(slab, 0), True),
            ]
        ),
        SecondBack(
            grad_pre, fc, hat_two, inv_two, gain_two[None], cotangent.reshape(own, width), out_w
        ),
    )
    grad_branch = grad_branch.reshape(tokens, width)

    ((grad_heads,),) = exchange(4, "to_heads_back", ToHeads([by_sequences(grad_attended)]))
    back = AttendBack(
        q_seq,
        k_seq,
        v_seq,
        grad_heads.reshape(length, piece),
        ot,
        lse,
        heads_here,
        all_seqs,
        half_rows,
    )
    grad_qkv, (mlp,) = exchange(
        5,
        "from_heads_back",
        Later(back, 0, 4),
        Product(activated, proj, own),
    )
    outputs = (resid + mlp + bias_proj).astype(BF16).reshape(seqs, rows, width)
    grad_qkv = [a.reshape(tokens, cols) for a in grad_qkv]
    grad_bias_query = jnp.sum(grad_qkv[0].astype(F32), axis=0)
    grad_bias_value = jnp.sum(grad_qkv[2].astype(F32), axis=0)

    def window(vector):
        whole = jnp.zeros((parts * live,), F32)
        return lax.dynamic_update_slice_in_dim(whole, vector[:live], me_part * live, 0)[:width]

    small_grads = jnp.concatenate(
        [window(grad_bias_query)[None], window(grad_bias_value)[None], sums_two]
    )

    (out_grad, q_grad, k_grad, v_grad), (input_grad, small_grads) = exchange(
        6,
        "narrow_grads",
        Ring(
            [
                (attended, grad_branch, split(cols // n_ctx, 0), False),
                (normed_one, grad_qkv[0], (slab, 0), True),
                (normed_one, grad_qkv[1], (0, slab), True),
                (normed_one, grad_qkv[2], split(slab, 1), True),
            ]
        ),
        FirstBack(
            grad_qkv,
            qkv,
            hat_one,
            inv_one,
            gain_one[None],
            grad_resid,
            small_grads,
            grad_bias_fc.reshape(-1, quarter),
        ),
    )
    input_grad = input_grad.reshape(seqs, rows, width)
    fc_out, q_out, k_out, v_out = by_rows(
        [fc_grad, q_grad, k_grad, v_grad],
        [(hidden_part, hidden)] + [(live, width)] * 3,
        per,
        me_part,
        parts,
    )
    out_rows = out_grad.reshape(cols, width)[:live]
    from_left = lax.ppermute(out_rows[live - near :], "fsdp", [(i, i + 1) for i in range(parts - 1)])
    out_rows = lax.dynamic_slice_in_dim(
        jnp.concatenate([from_left, out_rows]), near - me_part * (live - quarter), quarter, 0
    ).astype(F32)
    return (
        outputs,
        input_grad,
        q_out,
        k_out,
        v_out,
        out_rows,
        fc_out,
        proj_grad.reshape(hidden_part, width).astype(F32),
        small_grads[0],
        small_grads[1],
        small_grads[2],
        small_grads[3],
        small_grads[6],
        small_grads[4],
        small_grads[5],
        small_grads[8:].reshape(-1),
        small_grads[7],
    )


def solution(mesh):
    tokens = P("fsdp", "ctx", None)
    matrix = P("fsdp", None)
    vector = P("fsdp")
    return jax.shard_map(
        on_device,
        mesh=mesh,
        in_specs=(tokens, tokens) + (matrix,) * 6 + (vector,) * 9,
        out_specs=(tokens, tokens) + (matrix,) * 6 + (vector,) * 9,
        check_vma=False,
    )
```
